32 devices in a mesh: expert: 16 (over z, y, x), context: 2 (over core).
Axes of the slice: x: 2, y: 2, z: 4, core: 2. Of those that a mesh axis runs over, the one named last changes fastest.
Arguments:
- tokens: bfloat16 [4096, 2048], P(('expert', 'context')), may hold values from -6 to 6
- routes: int32 [4096, 8], P(('expert', 'context')), may hold values from 0 to 31, all different within a row; in each aligned block of 128 rows (0 to 127, 128 to 255, ...) at most 40 rows name the same one
- documents: int32 [16, 256], P('expert'), may hold values from 0 to 3, never falling along the last dimension, each value on 1 to 128 neighbouring positions
- w_query: bfloat16 [2048, 4096], P(('expert', 'context')), may hold values from -0.125 to 0.125
- key_projection: bfloat16 [2048, 512], P(('expert', 'context')), may hold values from -0.125 to 0.125
- value_projection: bfloat16 [2048, 512], P(('expert', 'context')), may hold values from -0.125 to 0.125
- w_out: bfloat16 [4096, 2048], P(('expert', 'context')), may hold values from -0.75 to 0.75
- w_router: bfloat16 [2048, 32], P(('expert', 'context')), may hold values from -0.25 to 0.25
- gain_attn: bfloat16 [2048], P(('expert', 'context')), may hold values from 0.099609375 to 1.8984375
- gain_ffn: bfloat16 [2048], P(('expert', 'context')), may hold values from 0.099609375 to 1.8984375
- gain_query: bfloat16 [128], P(('expert', 'context')), may hold values from 0.099609375 to 1.8984375
- gain_key: bfloat16 [128], P(('expert', 'context')), may hold values from 0.099609375 to 1.8984375
- w_gate: bfloat16 [32, 2048, 768], P('expert', None, 'context'), may hold values from -0.125 to 0.125
- w_up: bfloat16 [32, 2048, 768], P('expert', None, 'context'), may hold values from -0.125 to 0.125
- w_down: bfloat16 [32, 768, 2048], P('expert', 'context'), may hold values from -0.875 to 0.875
- cotangent: bfloat16 [4096, 2048], P(('expert', 'context')), may hold values from -6 to 6
Outputs:
- block_out: bfloat16 [4096, 2048], P(('expert', 'context'))
- grad_tokens: float32 [4096, 2048], P(('expert', 'context'))
- grad_query: float32 [2048, 4096], P(('expert', 'context'))
- grad_key: float32 [2048, 512], P(('expert', 'context'))
- grad_value: float32 [2048, 512], P(('expert', 'context'))
- grad_out: float32 [4096, 2048], P(('expert', 'context'))
- grad_router: float32 [2048, 32], P(('expert', 'context'))
- grad_gain_attn: float32 [2048], P(('expert', 'context'))
- grad_gain_ffn: float32 [2048], P(('expert', 'context'))
- grad_gain_query: float32 [128], P(('expert', 'context'))
- grad_gain_key: float32 [128], P(('expert', 'context'))
- grad_gate: float32 [32, 2048, 768], P('expert', None, 'context')
- grad_up: float32 [32, 2048, 768], P('expert', None, 'context')
- grad_down: float32 [32, 768, 2048], P('expert', 'context')
The draws below stay inside these ranges and needn't reach their ends.
Inputs may be any that keep to these rules, and one draw needn't show every extreme that they name: `routes`: each row names 8 different experts; among the 128 rows of one device no expert is named more than 40 times, a bound that some block reaches. `documents`: document numbers never fall along a sequence; each document holds at most 128 positions, and one exactly that many.
All inputs are finite; a program needn't handle non-finite values.
Results may differ from the reference program's by a relative error of at most 0.025.
Values may be sent and summed in bfloat16 or wider, within the bound.
A program may use at most 320 MiB of HBM per device.

```python
import functools
import math
import jax
import jax.numpy as jnp
import numpy as np
from jax import lax

MODEL_WIDTH = 2048
QUERY_HEADS = 32
KEY_VALUE_HEADS = 4
HEAD_SIZE = 128
FF = 768
TOP = 8
DEVICE_TOKENS = 128
EXPERTS = 32
SEQUENCE_TOKENS = 256
SEQUENCE_COUNT = 16
TOKENS = 4096
CAP = 40
N_EXPERT = 16
N_CONTEXT = 2


def level_of(rng, dims, cuts, low, top_value):
    gain = 1.0
    for axis_at, parts in cuts:
        steps = jax.random.uniform(jax.random.fold_in(jax.random.fold_in(rng, 6), axis_at), (parts,), jnp.float32, low / len(cuts), top_value / len(cuts))
        gain = gain * jnp.repeat(jnp.exp(steps), dims[axis_at] // parts).reshape((-1,) + (1,) * (len(dims) - 1 - axis_at))
    return gain


def split_up(count, total, bound, lean):
    portions = [(1 << 20) // math.isqrt(grade ** lean) + 1 for grade in range(2, count + 1)]
    spare, counts = total - bound - (count - 1), [1] * (count - 1)
    while spare > 0:
        candidates = [i for i in range(count - 1) if counts[i] < bound]
        mass, budget = sum([portions[i] for i in candidates]), spare
        for i in candidates:
            extra = min(bound - counts[i], max(1, budget * portions[i] // mass), spare)
            counts[i] = counts[i] + extra
            spare = spare - extra
    return np.array([bound] + counts)


def ragged(own_key, amount, total, reach, slope):
    if amount == 2:
        one = jax.random.randint(own_key, (), max(1, total - reach), min(reach, total - 1) + 1)
        return jnp.stack([one, total - one])
    lengths = jnp.asarray(split_up(amount, total, reach, slope), jnp.int32)
    pairs = (amount - 1) // 2
    donor, taker = lengths[1:1 + 2 * pairs:2], lengths[2:2 + 2 * pairs:2]
    slack = jnp.minimum(donor - 1, reach - taker)
    moved = jax.random.randint(jax.random.fold_in(own_key, 1), (pairs,), 0, 1 << 20) % (slack + 1)
    lengths = lengths.at[1:1 + 2 * pairs:2].set(donor - moved).at[2:2 + 2 * pairs:2].set(taker + moved)
    return lengths[jax.random.permutation(jax.random.fold_in(own_key, 2), amount)]


def shared_out(key, own, number, rows, number_of, top, most, lean):
    ranking = jax.random.permutation(key, number_of)
    crowded, ordinary = portions_of(number_of, rows * top, most, lean, True), portions_of(number_of, rows * top, most, lean, False)
    places = jnp.arange(number_of)

    def named(tallies, rotation):
        used = int((tallies > 0).sum())
        fixed = max(1, used // 4)
        moved = fixed + (places - fixed + rotation * (used - fixed)) % max(1, number_of - fixed)
        return jnp.zeros((number_of,), jnp.int32).at[ranking[jnp.where(places < fixed, places, moved)]].set(jnp.asarray(tallies, jnp.int32))

    tallies = jnp.where(number % 4 == 0, named(crowded, number // 4), named(ordinary, number - number // 4 - 1))
    mixed = jax.random.permutation(jax.random.fold_in(own, 3), number_of)
    giver, sink = mixed[0:number_of // 2 * 2:2], mixed[1:number_of // 2 * 2:2]
    margin = jnp.minimum(tallies[giver] - 1, most - tallies[sink]) // 2
    margin = jnp.where((giver == ranking[0]) | (sink == ranking[0]) | (tallies[sink] == 0), 0, jnp.maximum(margin, 0))
    moved = jax.random.randint(jax.random.fold_in(own, 4), (number_of // 2,), 0, 1 << 20) % (margin + 1)
    tallies = tallies.at[giver].add(-moved).at[sink].add(moved)
    items = jnp.searchsorted(jnp.cumsum(tallies), jnp.arange(rows * top), side="right").astype(jnp.int32)
    grid = items.reshape(top, rows).T
    grid = grid[jax.random.permutation(jax.random.fold_in(own, 1), rows)]
    rotation = jax.random.randint(jax.random.fold_in(own, 2), (rows, 1), 0, top)
    return jnp.take_along_axis(grid, (jnp.arange(top)[None, :] + rotation) % top, axis=1)


def portions_of(count, total, reach, lean, full):
    portions = [(1 << 20) // math.isqrt(rank ** lean) + 1 for rank in range(1, count + 1)]
    largest = reach if full else min(reach, max(-(-total // count), total * portions[0] // sum(portions)))
    least = 1 if total - largest >= count - 1 else 0
    holding, surplus = [largest] + [least] * (count - 1), total - largest - least * (count - 1)
    while surplus > 0:
        movable = [i for i in range(1, count) if holding[i] < largest] or [i for i in range(1, count) if holding[i] < reach]
        mass, left = sum([portions[i] for i in movable]), surplus
        for i in movable:
            extra = min(reach - holding[i], max(1, left * portions[i] // mass), surplus)
            holding[i] = holding[i] + extra
            surplus = surplus - extra
    return np.array(holding)


def scatter_about(own_key, shape, width, reach, split=(), held_as=jnp.bfloat16):
    entries = jax.random.normal(own_key, shape, jnp.float32) * width
    if len(split) > 0:
        entries = level_of(own_key, shape, split, -0.22, 0.18) * entries
    return jnp.clip(entries, min=-reach, max=reach).astype(held_as)


def setup_inputs(seed: int = 0) -> dict:
    arg_keys = jax.random.split(jax.random.key(seed), 17)
    tokens = scatter_about(arg_keys[0], (TOKENS, MODEL_WIDTH), 1.0, 6.0, ((0, 32),))
    routes_keys = jax.random.split(jax.random.fold_in(arg_keys[1], 1), TOKENS // DEVICE_TOKENS)
    routes_turns = jax.random.permutation(jax.random.fold_in(arg_keys[1], 3), TOKENS // DEVICE_TOKENS)
    routes = jax.vmap(lambda own, number: shared_out(jax.random.fold_in(arg_keys[1], 2), own, number, DEVICE_TOKENS, EXPERTS, TOP, CAP, 1))(routes_keys, routes_turns).reshape((TOKENS, TOP))
    documents = jax.vmap(lambda own: jnp.searchsorted(jnp.cumsum(ragged(own, 4, SEQUENCE_TOKENS, SEQUENCE_TOKENS // 2, 0)), jnp.arange(SEQUENCE_TOKENS), side="right"))(jax.random.split(arg_keys[2], SEQUENCE_COUNT)).reshape((SEQUENCE_COUNT, SEQUENCE_TOKENS)).astype(jnp.int32)
    w_query = scatter_about(arg_keys[3], (MODEL_WIDTH, QUERY_HEADS * HEAD_SIZE), MODEL_WIDTH ** -0.5, 0.125, ((0, 32),))
    key_projection = scatter_about(arg_keys[4], (MODEL_WIDTH, KEY_VALUE_HEADS * HEAD_SIZE), MODEL_WIDTH ** -0.5, 0.125, ((0, 32),))
    value_projection = scatter_about(arg_keys[5], (MODEL_WIDTH, KEY_VALUE_HEADS * HEAD_SIZE), MODEL_WIDTH ** -0.5, 0.125, ((0, 32),))
    w_out = scatter_about(arg_keys[6], (QUERY_HEADS * HEAD_SIZE, MODEL_WIDTH), (HEAD_SIZE // 2) ** -0.5, 0.75, ((0, 32),))
    w_router = scatter_about(arg_keys[7], (MODEL_WIDTH, EXPERTS), (MODEL_WIDTH // 4) ** -0.5, 0.25, ((0, 32),))
    gain_attn = jnp.clip(1.0 + 0.18 * jax.random.normal(arg_keys[8], (MODEL_WIDTH,), jnp.float32), 0.099609375, 1.8984375).astype(jnp.bfloat16)
    gain_ffn = jnp.clip(1.0 + 0.18 * jax.random.normal(arg_keys[9], (MODEL_WIDTH,), jnp.float32), 0.099609375, 1.8984375).astype(jnp.bfloat16)
    gain_query = jnp.clip(1.0 + 0.18 * jax.random.normal(arg_keys[10], (HEAD_SIZE,), jnp.float32), 0.099609375, 1.8984375).astype(jnp.bfloat16)
    gain_key = jnp.clip(1.0 + 0.18 * jax.random.normal(arg_keys[11], (HEAD_SIZE,), jnp.float32), 0.099609375, 1.8984375).astype(jnp.bfloat16)
    w_gate = scatter_about(arg_keys[12], (EXPERTS, MODEL_WIDTH, FF), MODEL_WIDTH ** -0.5, 0.125, ((0, 16), (2, 2)))
    w_up = scatter_about(arg_keys[13], (EXPERTS, MODEL_WIDTH, FF), MODEL_WIDTH ** -0.5, 0.125, ((0, 16), (2, 2)))
    w_down = scatter_about(arg_keys[14], (EXPERTS, FF, MODEL_WIDTH), (FF // 16) ** -0.5, 0.875, ((0, 16), (1, 2)))
    cotangent = scatter_about(arg_keys[15], (TOKENS, MODEL_WIDTH), 1.0, 6.0, ((0, 32),))
    return dict(tokens=tokens, routes=routes, documents=documents, w_query=w_query, key_projection=key_projection, value_projection=value_projection, w_out=w_out, w_router=w_router, gain_attn=gain_attn, gain_ffn=gain_ffn, gain_query=gain_query, gain_key=gain_key, w_gate=w_gate, w_up=w_up, w_down=w_down, cotangent=cotangent)


@jax.custom_vjp
def narrow_precision(v):
    return lax.optimization_barrier(v.astype(jnp.bfloat16)).astype(jnp.float32)

@jax.custom_vjp
def low_back(v):
    return v

def low_keep(v):
    return (narrow_precision(v), None)

def low_pass(kept, grad):
    return (grad,)

def back_keep(v):
    return (v, None)

def back_low(kept, grad):
    return (narrow_precision(grad),)
narrow_precision.defvjp(low_keep, low_pass)
low_back.defvjp(back_keep, back_low)
epsilon = 1e-06
rope_base = 1000000.0
highest = lax.Precision.HIGHEST

def root_mean_square_gain(values_in, gain_vec):
    inverse = lax.rsqrt(lax.optimization_barrier(jnp.mean(values_in * values_in, axis=-1, keepdims=True)) + epsilon)
    return values_in * inverse * gain_vec

def rope_tables(positions):
    exponent = jnp.arange(HEAD_SIZE // 2).astype(jnp.float32) * (2.0 / HEAD_SIZE)
    frequency = jnp.exp(-math.log(rope_base) * exponent)
    angles = positions.astype(jnp.float32)[:, None] * frequency[None, :]
    return (jnp.cos(angles), jnp.sin(angles))

def apply_rotary(values_in, cosine_table, sine_table):
    half_width = values_in.shape[-1] // 2
    first_half = values_in[..., :half_width]
    second_half = values_in[..., half_width:]
    cos_wide = cosine_table[:, None, :]
    sin_wide = sine_table[:, None, :]
    return jnp.concatenate([first_half * cos_wide - second_half * sin_wide, second_half * cos_wide + first_half * sin_wide], axis=-1)

def attend(block_data):
    query_rows, gathered_keys, gathered_values, doc_ids = block_data
    batch_sequences = query_rows.shape[0]
    query_group_width = QUERY_HEADS // KEY_VALUE_HEADS
    query_per_head = query_rows.reshape(batch_sequences, SEQUENCE_TOKENS, KEY_VALUE_HEADS, query_group_width, HEAD_SIZE)
    scores = jnp.einsum('bqhrd,bkhd->bhrqk', query_per_head, gathered_keys, precision=highest) * HEAD_SIZE ** (-0.5)
    scores = low_back(scores)
    places = jnp.arange(SEQUENCE_TOKENS, dtype=jnp.int32)
    allowed = (places[:, None] >= places[None, :])[None] & (doc_ids[:, :, None] == doc_ids[:, None, :])
    scores = jnp.where(allowed[:, None, None], scores, -1e+30)
    probabilities = jax.nn.softmax(scores, axis=-1)
    attended = jnp.einsum('bhrqk,bkhd->bqhrd', narrow_precision(probabilities), gathered_values, precision=highest)
    return attended.reshape(batch_sequences, SEQUENCE_TOKENS, QUERY_HEADS * HEAD_SIZE)

def expert_apply(hidden, inputs):
    token_rows, gate_matrix, up_matrix, down_matrix = inputs
    rows_in = low_back(hidden[token_rows])
    gate_value = low_back(jnp.dot(rows_in, gate_matrix, precision=highest))
    up_value = low_back(jnp.dot(rows_in, up_matrix, precision=highest))
    activation = narrow_precision(jax.nn.silu(gate_value) * up_value)
    return low_back(narrow_precision(jnp.dot(activation, down_matrix, precision=highest)))

def reference(tokens, routes, documents, w_query, key_projection, value_projection, w_out, w_router, gain_attn, gain_ffn, gain_query, gain_key, w_gate, w_up, w_down, cotangent):
    flat_routes = routes.reshape(-1)
    pair_ids = jnp.arange(TOKENS * TOP, dtype=jnp.int32)
    most_rows = N_EXPERT * N_CONTEXT * CAP

    def choose(expert_id):
        marked = jnp.where(flat_routes == expert_id, pair_ids, TOKENS * TOP)
        return jnp.sort(marked)[:most_rows]
    chosen = lax.map(choose, jnp.arange(EXPERTS, dtype=jnp.int32))
    valid_rows = chosen < TOKENS * TOP
    pair_rows = jnp.where(valid_rows, chosen, 0).astype(jnp.int32)
    token_rows = (pair_rows // TOP).astype(jnp.int32)
    cosine_table, sine_table = rope_tables(jnp.arange(SEQUENCE_TOKENS, dtype=jnp.int32))
    block_seqs = math.gcd(SEQUENCE_COUNT, max(1, 4096 // SEQUENCE_TOKENS))

    def to_blocks(array_in):
        return array_in.reshape((SEQUENCE_COUNT // block_seqs, block_seqs) + array_in.shape[1:])

    def forward(token_values, query_matrix, key_matrix, value_matrix, out_matrix, router_matrix, attn_scale, ffn_scale, query_scale, key_norm_scale, gate_matrix, up_matrix, down_matrix):
        normed_attn = narrow_precision(root_mean_square_gain(token_values, attn_scale))
        query_raw = low_back(jnp.dot(normed_attn, query_matrix, precision=highest))
        unnormed_key = low_back(jnp.dot(normed_attn, key_matrix, precision=highest))
        unnormed_value = narrow_precision(low_back(jnp.dot(normed_attn, value_matrix, precision=highest)))
        query_rows = narrow_precision(apply_rotary(root_mean_square_gain(query_raw.reshape(SEQUENCE_COUNT, SEQUENCE_TOKENS, QUERY_HEADS, HEAD_SIZE), query_scale), cosine_table, sine_table))
        gathered_keys = narrow_precision(apply_rotary(root_mean_square_gain(unnormed_key.reshape(SEQUENCE_COUNT, SEQUENCE_TOKENS, KEY_VALUE_HEADS, HEAD_SIZE), key_norm_scale), cosine_table, sine_table))
        gathered_values = unnormed_value.reshape(SEQUENCE_COUNT, SEQUENCE_TOKENS, KEY_VALUE_HEADS, HEAD_SIZE)
        attended = lax.map(jax.checkpoint(attend), (to_blocks(query_rows), to_blocks(gathered_keys), to_blocks(gathered_values), to_blocks(documents)))
        attended = low_back(narrow_precision(attended.reshape(TOKENS, QUERY_HEADS * HEAD_SIZE)))
        attn_result = low_back(jnp.dot(attended, out_matrix, precision=highest))
        middle = token_values + attn_result
        normed_ffn = narrow_precision(root_mean_square_gain(middle, ffn_scale))
        logits = low_back(jnp.dot(normed_ffn, router_matrix, precision=highest))
        chosen_logits = jnp.take_along_axis(logits, routes, axis=1)
        route_weights = jax.nn.softmax(chosen_logits, axis=-1)
        expert_out = lax.map(jax.checkpoint(functools.partial(expert_apply, normed_ffn)), (token_rows, gate_matrix, up_matrix, down_matrix))
        slot_weights = jnp.where(valid_rows, route_weights.reshape(-1)[pair_rows], 0.0)
        weighted = expert_out * slot_weights[:, :, None]
        moe_result = jnp.zeros((TOKENS, MODEL_WIDTH), jnp.float32).at[token_rows.reshape(-1)].add(weighted.reshape(-1, MODEL_WIDTH))
        return middle + moe_result
    floats = tuple((array_in.astype(jnp.float32) for array_in in (tokens, w_query, key_projection, value_projection, w_out, w_router, gain_attn, gain_ffn, gain_query, gain_key, w_gate, w_up, w_down)))
    result, pullback = jax.vjp(forward, *floats)
    gradients = pullback(cotangent.astype(jnp.float32))
    return (result.astype(jnp.bfloat16), gradients[0], gradients[1], gradients[2], gradients[3], gradients[4], gradients[5], gradients[6], gradients[7], gradients[8], gradients[9], gradients[10], gradients[11], gradients[12])
```

```python
import functools
import math

import jax
import jax.numpy as jnp
from jax import lax
from jax.experimental import pallas as pl
from jax.experimental.pallas import tpu as pltpu
from jax.sharding import PartitionSpec as P

MESH_ID = pl.DeviceIdType.MESH
BF = jnp.bfloat16
F32 = jnp.float32


class Net:
    def __init__(self, n_expert):
        side = math.isqrt(n_expert // 4)
        self.dims = (4, side, side)
        self.chips = n_expert

    def enter(self):
        e = lax.axis_index("expert")
        _, A, B = self.dims
        self.e = e
        self.at = (e // (A * B), (e // B) % A, e % B)
        self.c = lax.axis_index("context")
        return self

    def chip(self, at):
        _, A, B = self.dims
        return (at[0] * A + at[1]) * B + at[2]

    def moved(self, axis, to):
        at = list(self.at)
        at[axis] = to
        return tuple(at)

    def near(self, axis):
        n, p = self.dims[axis], self.at[axis]
        if n == 2:
            return [(None, 1 - p)]
        return [(p < n - 1, p + 1), (p > 0, p - 1)]


def when(cond, fn):
    if cond is None:
        fn()
    else:
        pl.when(cond)(fn)


def rcopy(src, dst, ss, rs, dev):
    return pltpu.make_async_remote_copy(
        src_ref=src, dst_ref=dst, send_sem=ss, recv_sem=rs, device_id=dev, device_id_type=MESH_ID
    )


def greet(net, axes, partner=True):
    bar = pltpu.get_barrier_semaphore()
    count = 0
    for axis in axes:
        for cond, to in net.near(axis):
            dev = (net.chip(net.moved(axis, to)), net.c)
            when(cond, lambda dev=dev: pl.semaphore_signal(bar, inc=1, device_id=dev, device_id_type=MESH_ID))
            count = count + (1 if cond is None else jnp.where(cond, 1, 0))
    if partner:
        pl.semaphore_signal(bar, inc=1, device_id=(net.e, 1 - net.c), device_id_type=MESH_ID)
        count = count + 1
    pl.semaphore_wait(bar, count)


def greet_all(net):
    bar = pltpu.get_barrier_semaphore()
    total = net.chips * 2
    me = net.e * 2 + net.c

    def body(k, _):
        t = (me + k) % total
        pl.semaphore_signal(bar, inc=1, device_id=(t // 2, t % 2), device_id_type=MESH_ID)
        return 0

    lax.fori_loop(1, total, body, 0)
    pl.semaphore_wait(bar, total - 1)


def interleave(*gens):
    gens = list(gens)
    while gens:
        for g in list(gens):
            try:
                next(g)
            except StopIteration:
                gens.remove(g)


def ag_piece(net, order, block, rs, ss, done, partner=True):
    def send(cond, at, kind, dev):
        ch = net.chip(at)
        mk = lambda: rcopy(block(ch, net.c), block(ch, net.c), ss(ch, kind), rs(ch, net.c), dev)
        when(cond, lambda: mk().start())
        return lambda: when(cond, lambda: mk().wait_send())

    def spread(at, stage):
        outs = []
        for i in range(stage, len(order)):
            axis = order[i]
            for k, (cond, to) in enumerate(net.near(axis)):
                outs.append(send(cond, at, 2 * i + k, (net.chip(net.moved(axis, to)), net.c)))
        if partner:
            outs.append(send(None, at, 6, (net.e, 1 - net.c)))
        return outs

    done.extend(spread(net.at, 0))
    yield
    known = [(None, net.at)]

    for i, axis in enumerate(order):
        n, p = net.dims[axis], net.at[axis]
        fresh = []
        if n == 2:
            steps = [(None, 1 - p, None)]
        else:
            steps = []
            for k in range(1, n):
                steps.append((p - k >= 0, p - k, 0))
                steps.append((p + k <= n - 1, p + k, 1))
        for cond, o, way in steps:
            for kcond, kat in known:
                at = list(kat)
                at[axis] = o
                at = tuple(at)
                both = cond if kcond is None else (kcond if cond is None else jnp.logical_and(cond, kcond))

                def onward(at, way, i, axis):
                    outs = []
                    if way is not None:
                        cond2, to = net.near(axis)[way]
                        outs.append((cond2, 2 * i + way, (net.chip(net.moved(axis, to)), net.c)))
                    for j in range(i + 1, len(order)):
                        for k, (c2, to) in enumerate(net.near(order[j])):
                            outs.append((c2, 2 * j + k, (net.chip(net.moved(order[j], to)), net.c)))
                    if partner:
                        outs.append((None, 6, (net.e, 1 - net.c)))
                    return outs

                def arrive(at=at, way=way, i=i, axis=axis):
                    ch = net.chip(at)
                    rcopy(block(ch, net.c), block(ch, net.c), ss(ch, 0), rs(ch, net.c), (net.e, net.c)).wait_recv()
                    for c2, kind, dev in onward(at, way, i, axis):
                        send(c2, at, kind, dev)

                when(both, arrive)

                def drain(at=at, way=way, i=i, axis=axis, both=both):
                    def inner():
                        ch = net.chip(at)
                        for c2, kind, dev in onward(at, way, i, axis):
                            when(c2, lambda kind=kind, dev=dev: rcopy(
                                block(ch, net.c), block(ch, net.c), ss(ch, kind), rs(ch, net.c), dev).wait_send())
                    when(both, inner)

                done.append(drain)
                fresh.append((both, at))
                yield
        known = known + fresh
    if partner:
        for kcond, kat in known:
            def theirs(kat=kat):
                ch = net.chip(kat)
                rcopy(block(ch, 1 - net.c), block(ch, 1 - net.c), ss(ch, 0), rs(ch, 1 - net.c), (net.e, net.c)).wait_recv()
            done.append(lambda kcond=kcond, theirs=theirs: when(kcond, theirs))


def add_into(dst, src, rows):
    step = 16
    assert rows % step == 0

    def body(i, _):
        r = pl.ds(pl.multiple_of(i * step, step), step)
        dst[r, :] = (dst[r, :].astype(F32) + src[r, :].astype(F32)).astype(BF)
        return 0

    lax.fori_loop(0, rows // step, body, 0)


def rs_piece(net, order, mine, acc, bufs, key, rs, ss, rows, done, partner=True):
    def all_combos(axes_left):
        out = [()]
        for ax in axes_left:
            out = [o + (v,) for o in out for v in range(net.dims[ax])]
        return out

    def p_send(at):
        ch = net.chip(at)
        mk = lambda: rcopy(mine(ch, 1 - net.c), acc(ch), ss(0, ch), rs(0, ch), (net.e, 1 - net.c))
        mk().start()
        done.append(lambda: mk().wait_send())

    def p_recv(at):
        ch = net.chip(at)
        rcopy(acc(ch), acc(ch), ss(0, ch), rs(0, ch), (net.e, net.c)).wait_recv()
        add_into(acc(ch), mine(ch, net.c), rows)

    stages = []
    for i, axis in enumerate(order):
        left = order[i + 1:]
        combos = all_combos(left)
        stages.append((i, axis, left, combos))

    def targets_of(i, axis, left, combo, t):
        at = list(net.at)
        at[axis] = t
        for ax, v in zip(left, combo):
            at[ax] = v
        return tuple(at)

    for i, axis, left, combos in stages:
        n, p = net.dims[axis], net.at[axis]
        for combo in combos:
            for d in range(1, n):
                t = (p + d) % n
                p_send(targets_of(i, axis, left, combo, t))
        yield
    p_send(net.at)
    yield

    for i, axis, left, combos in stages:
        n, p = net.dims[axis], net.at[axis]
        nxt = lambda to, axis=axis: (net.chip(net.moved(axis, to)), net.c)

        def gather_prev(at):
            p_recv(at)
            for i2, axis2, left2, _ in stages[:i]:
                land(i2, axis2, left2, at)

        def land(i2, axis2, left2, at):
            n2, p2 = net.dims[axis2], net.at[axis2]
            ch = net.chip(at)

            def take(way):
                k = key(i2, way, at)
                rcopy(bufs(i2, k), bufs(i2, k), ss(i2 + 1, k), rs(i2 + 1, k), (net.e, net.c)).wait_recv()
                add_into(acc(ch), bufs(i2, k), rows)

            if n2 == 2:
                take(0)
            else:
                when(p2 > 0, lambda: take(0))
                when(p2 < n2 - 1, lambda: take(1))

        for combo in combos:
            if n == 2:
                at = targets_of(i, axis, left, combo, 1 - p)
                gather_prev(at)
                ch = net.chip(at)
                k = key(i, 0, at)
                mk = lambda ch=ch, k=k, i=i: rcopy(acc(ch), bufs(i, k), ss(i + 1, k), rs(i + 1, k), nxt(1 - p))
                mk().start()
                done.append(lambda mk=mk: mk().wait_send())
                yield
            else:
                for s in range(n - 1):
                    for way in (0, 1):
                        t = n - 1 - s if way == 0 else s
                        cond = (p < t) if way == 0 else (p > t)
                        to = p + 1 if way == 0 else p - 1
                        inner_cond = (p > 0) if way == 0 else (p < n - 1)
                        at = targets_of(i, axis, left, combo, t)
                        ch, k = net.chip(at), key(i, way, at)
                        mk = lambda ch=ch, k=k, i=i, to=to: rcopy(acc(ch), bufs(i, k), ss(i + 1, k), rs(i + 1, k), nxt(to))

                        def step(at=at, ch=ch, k=k, i=i, inner_cond=inner_cond, mk=mk):
                            gather_prev(at)

                            def relay():
                                rcopy(bufs(i, k), bufs(i, k), ss(i + 1, k), rs(i + 1, k), (net.e, net.c)).wait_recv()
                                add_into(acc(ch), bufs(i, k), rows)

                            pl.when(inner_cond)(relay)
                            mk().start()

                        pl.when(cond)(step)
                        done.append(lambda cond=cond, mk=mk: pl.when(cond)(lambda: mk().wait_send()))
                        yield
    at = net.at
    p_recv(at)
    for i2, axis2, left2, _ in stages:
        n2, p2 = net.dims[axis2], net.at[axis2]
        ch = net.chip(at)

        def take(way, i2=i2):
            k = key(i2, way, at)
            rcopy(bufs(i2, k), bufs(i2, k), ss(i2 + 1, k), rs(i2 + 1, k), (net.e, net.c)).wait_recv()
            add_into(acc(ch), bufs(i2, k), rows)

        if n2 == 2:
            take(0)
        else:
            when(p2 > 0, lambda: take(0))
            when(p2 < n2 - 1, lambda: take(1))
        yield


def rs_keys(net, order):
    def size(i):
        left = order[i + 1:]
        m = 1
        for ax in left:
            m *= net.dims[ax]
        n = net.dims[order[i]]
        return m if n == 2 else 2 * n * m

    def key(i, way, at):
        left = order[i + 1:]
        k = 0
        for ax in left:
            k = k * net.dims[ax] + at[ax]
        n = net.dims[order[i]]
        if n == 2:
            return k
        return (k * n + at[order[i]]) * 2 + way

    return key, [size(i) for i in range(len(order))]


def params(cid, vmem=None):
    return pltpu.CompilerParams(collective_id=cid, has_side_effects=True, vmem_limit_bytes=vmem)


ANY = pl.BlockSpec(memory_space=pl.ANY)
VM = pl.BlockSpec(memory_space=pltpu.VMEM)
DMA = pltpu.SemaphoreType.DMA

ORDER_A = (0, 1, 2)
ORDER_B = (0, 2, 1)


def all_gather_all(n_expert, x, cid):
    rows, cols = x.shape
    half = rows // 2

    def kernel(x_ref, o_ref, rsem, ssem, lsem):
        net = Net(n_expert).enter()
        cp = pltpu.make_async_copy(x_ref, o_ref.at[net.e, net.c], lsem)
        cp.start()
        greet(net, (0, 1, 2))
        cp.wait()
        done = []
        gens = []
        for i, order in enumerate((ORDER_A, ORDER_B)):
            gens.append(ag_piece(
                net, order,
                lambda ch, co, i=i: o_ref.at[ch, co, pl.ds(i * half, half)],
                lambda ch, co, i=i: rsem.at[i, ch, co],
                lambda ch, kind, i=i: ssem.at[i, ch, kind], done))
        interleave(*gens)
        for f in done:
            f()

    return pl.pallas_call(
        kernel, out_shape=jax.ShapeDtypeStruct((n_expert, 2, rows, cols), x.dtype),
        in_specs=[VM], out_specs=ANY,
        scratch_shapes=[DMA((2, n_expert, 2)), DMA((2, n_expert, 7)), DMA],
        compiler_params=params(cid), name="gather_all",
    )(x)


def reduce_scatter_all(n_expert, t, cid):
    _, _, rows, cols = t.shape
    half = rows // 2
    net0 = Net(n_expert)
    orders = ((2, 1, 0), (1, 2, 0))
    keys = [rs_keys(net0, o) for o in orders]
    sizes = keys[0][1]
    ns = max([n_expert] + sizes)

    def kernel(t_ref, o_ref, acc, b0, b1, b2, rsem, ssem):
        net = Net(n_expert).enter()
        greet(net, (0, 1, 2))
        done, gens = [], []
        bb = (b0, b1, b2)
        for i, order in enumerate(orders):
            key = keys[i][0]
            r = pl.ds(i * half, half)
            gens.append(rs_piece(
                net, order,
                lambda ch, co, r=r: t_ref.at[ch, co, r],
                lambda ch, r=r: acc.at[ch, r],
                lambda st, k, r=r: bb[st].at[k, r],
                key,
                lambda st, k, i=i: rsem.at[i, st, k],
                lambda st, k, i=i: ssem.at[i, st, k], half, done))
        interleave(*gens)
        o_ref[...] = acc[net.e]
        for f in done:
            f()

    return pl.pallas_call(
        kernel, out_shape=jax.ShapeDtypeStruct((rows, cols), BF),
        in_specs=[VM], out_specs=VM,
        scratch_shapes=[pltpu.VMEM((n_expert, rows, cols), BF)]
        + [pltpu.VMEM((s, rows, cols), BF) for s in sizes]
        + [DMA((2, 4, ns)), DMA((2, 4, ns))],
        compiler_params=params(cid, 60 << 20), name="reduce_all",
    )(t)


def local_copy(src, dst, sem, done):
    cp = lambda: pltpu.make_async_copy(src, dst, sem)
    cp().start()
    done.append(lambda: cp().wait())


def col_ag(net, src, dst, rs, ss, done):
    z, c = net.at[0], net.c
    n = net.dims[0]
    own = z // 2 == c
    s0 = z % 2

    def zdev(to):
        return (net.chip(net.moved(0, to)), c)

    def hop(cond, s, h, way, to, source=None):
        mk = lambda: rcopy(dst(s, h) if source is None else source, dst(s, h), ss(way, s, h), rs(s, h), zdev(to))
        when(cond, lambda: mk().start())
        return lambda: when(cond, lambda: mk().wait_send())

    def arrived(s, h):
        rcopy(dst(s, h), dst(s, h), ss(0, s, h), rs(s, h), (net.e, c)).wait_recv()

    across = lambda: rcopy(src, dst(s0, c), ss(2, 0, 0), rs(s0, c), (net.e, 1 - c))
    keep = lambda: pltpu.make_async_copy(src, dst(s0, c), ss(2, 0, 1))

    def begin():
        keep().start()
        hop(z < n - 1, s0, c, 0, z + 1, src)
        hop(z > 0, s0, c, 1, z - 1, src)

    pl.when(own)(begin)
    pl.when(jnp.logical_not(own))(lambda: across().start())
    yield

    def second():
        arrived(s0, 1 - c)
        hop(z < n - 1, s0, 1 - c, 0, z + 1)
        hop(z > 0, s0, 1 - c, 1, z - 1)

    pl.when(own)(second)
    yield

    def end():
        keep().wait()
        for h in (c, 1 - c):
            source = src if h is c else None
            when(z < n - 1, lambda h=h, source=source: rcopy(
                src if source is not None else dst(s0, h), dst(s0, h), ss(0, s0, h), rs(s0, h), zdev(z + 1)).wait_send())
            when(z > 0, lambda h=h, source=source: rcopy(
                src if source is not None else dst(s0, h), dst(s0, h), ss(1, s0, h), rs(s0, h), zdev(z - 1)).wait_send())

    done.append(lambda: pl.when(own)(end))
    done.append(lambda: pl.when(jnp.logical_not(own))(lambda: across().wait_send()))

    for k in range(1, n):
        for way in (0, 1):
            o = z - k if way == 0 else z + k
            inside = o >= 0 if way == 0 else o <= n - 1
            cond = jnp.logical_and(inside, o // 2 == c)
            more = z < n - 1 if way == 0 else z > 0
            to = z + 1 if way == 0 else z - 1

            def step(o=o, way=way, more=more, to=to):
                for h in (0, 1):
                    arrived(o % 2, h)
                    hop(more, o % 2, h, way, to)

            def finish(o=o, way=way, more=more, to=to):
                for h in (0, 1):
                    when(more, lambda h=h: rcopy(
                        dst(o % 2, h), dst(o % 2, h), ss(way, o % 2, h), rs(o % 2, h), zdev(to)).wait_send())

            pl.when(cond)(step)
            done.append(lambda cond=cond, finish=finish: pl.when(cond)(finish))
            yield


def col_rs(net, part, out, acc, buf, fin, rs, ss, rows, done):
    z, c = net.at[0], net.c
    n = net.dims[0]

    def zdev(to):
        return (net.chip(net.moved(0, to)), c)

    def msg(way, s, h, to):
        return rcopy(acc(way, s, h), buf(way, s, h), ss(way, s, h), rs(way, s, h), zdev(to))

    def arrived(way, s, h):
        rcopy(buf(way, s, h), buf(way, s, h), ss(way, s, h), rs(way, s, h), (net.e, c)).wait_recv()

    for k in range(n - 1):
        for way in (0, 1):
            t = n - 1 - k if way == 0 else k
            s = t % 2
            cond = jnp.logical_and(z < t if way == 0 else z > t, t // 2 == c)
            inner = z > 0 if way == 0 else z < n - 1
            to = z + 1 if way == 0 else z - 1
            for h in (0, 1):
                def step(way=way, s=s, h=h, inner=inner, to=to):
                    def relay():
                        arrived(way, s, h)
                        sum_to(acc(way, s, h), [part(s, h), buf(way, s, h)], rows)

                    pl.when(inner)(relay)
                    pl.when(jnp.logical_not(inner))(lambda: sum_to(acc(way, s, h), [part(s, h)], rows))
                    msg(way, s, h, to).start()

                pl.when(cond)(step)
                done.append(lambda cond=cond, way=way, s=s, h=h, to=to: pl.when(cond)(lambda: msg(way, s, h, to).wait_send()))
                yield

    own = z // 2 == c
    s0 = z % 2
    cross = lambda: rcopy(fin(0), fin(1), ss(2, 0, 0), rs(2, 0, 0), (net.e, 1 - c))

    def last(h, to_ref):
        low, high = z > 0, z < n - 1
        pl.when(low)(lambda: arrived(0, s0, h))
        pl.when(high)(lambda: arrived(1, s0, h))
        mid = jnp.logical_and(low, high)
        pl.when(mid)(lambda: sum_to(to_ref, [part(s0, h), buf(0, s0, h), buf(1, s0, h)], rows))
        pl.when(jnp.logical_not(low))(lambda: sum_to(to_ref, [part(s0, h), buf(1, s0, h)], rows))
        pl.when(jnp.logical_not(high))(lambda: sum_to(to_ref, [part(s0, h), buf(0, s0, h)], rows))

    def final():
        last(1 - c, fin(0))
        cross().start()
        last(c, out)

    pl.when(own)(final)
    done.append(lambda: pl.when(own)(lambda: cross().wait_send()))

    def take():
        cross().wait_recv()
        sum_to(out, [fin(1)], rows)

    yield
    pl.when(jnp.logical_not(own))(take)


def sum_to(dst, srcs, rows):
    step = 16

    def body(i, _):
        r = pl.ds(pl.multiple_of(i * step, step), step)
        v = srcs[0][r, :]
        if len(srcs) > 1:
            v = v.astype(F32)
            for s in srcs[1:]:
                v = v + s[r, :].astype(F32)
        dst[r, :] = v.astype(BF)
        return 0

    lax.fori_loop(0, rows // step, body, 0)


def to_all(net, src, dst, rs, ss, done):
    total = net.chips * 2
    me = net.e * 2 + net.c

    def put(k, _):
        t = (me + k) % total
        rcopy(src(t), dst(me), ss(k), rs(me), (t // 2, t % 2)).start()
        return 0

    lax.fori_loop(1, total, put, 0)
    yield

    def take(k, _):
        t = (me + k) % total
        rcopy(src(t), dst(me), ss(k), rs(me), (t // 2, t % 2)).wait_send()
        rcopy(dst(t), dst(t), ss(k), rs(t), (net.e, net.c)).wait_recv()
        return 0

    done.append(lambda: lax.fori_loop(1, total, take, 0))


def gather_start(n_expert, tokens, wqkv, w_out, aux, cot, cid):
    T, D = tokens.shape
    Z, R, C = wqkv.shape
    HR = w_out.shape[0]
    AR, AW = aux.shape
    plane = n_expert // Z
    nd = 2 * n_expert

    def kernel(t_ref, w_ref, o_ref, a_ref, g_ref, X, W, O, A, G,
               xr, xs, wr, ws, war, was, oar, oas, ar, as_, gr, gs, loc):
        net = Net(n_expert).enter()
        z, p, c = net.at[0], net.e % plane, net.c
        me = net.e * 2 + c
        done = []
        local_copy(w_ref.at[z], W.at[z, p, c], loc.at[0], [])
        local_copy(o_ref, O.at[p, c], loc.at[1], [])
        local_copy(a_ref, A.at[me], loc.at[2], done)
        local_copy(g_ref, G.at[net.e, c], loc.at[3], [])
        greet_all(net)

        def wgen():
            for k in range(1, Z):
                j = (z + k) % Z
                mk = lambda j=j, k=k: rcopy(w_ref.at[j], W.at[z, p, c], ws.at[k], wr.at[z], (j * plane + p, c))
                mk().start()
                done.append(lambda mk=mk: mk().wait_send())
            yield
            pltpu.make_async_copy(w_ref.at[z], W.at[z, p, c], loc.at[0]).wait()
            for k in range(1, Z):
                o = (z + k) % Z
                rcopy(W.at[o, p, c], W.at[o, p, c], ws.at[k], wr.at[o], (net.e, c)).wait_recv()
            gens = []
            for i, order in enumerate(((1, 2), (2, 1))):
                r = pl.ds(i * (Z // 2), Z // 2)
                gens.append(ag_piece(
                    net, order, lambda ch, co, r=r: W.at[r, ch % plane, co],
                    lambda ch, co, i=i: war.at[i, ch % plane, co], lambda ch, kind, i=i: was.at[i, ch % plane, kind], done))
            while gens:
                for g in list(gens):
                    try:
                        next(g)
                        yield
                    except StopIteration:
                        gens.remove(g)

        def ogen(i, order):
            if i == 0:
                pltpu.make_async_copy(o_ref, O.at[p, c], loc.at[1]).wait()
            r = pl.ds(i * (HR // 2), HR // 2)
            yield from ag_piece(
                net, order, lambda ch, co: O.at[ch % plane, co, r],
                lambda ch, co: oar.at[i, ch % plane, co], lambda ch, kind: oas.at[i, ch % plane, kind], done)

        def ggen(i, order):
            if i == 0:
                pltpu.make_async_copy(g_ref, G.at[net.e, c], loc.at[3]).wait()
            r = pl.ds(i * (T // 2), T // 2)
            yield from ag_piece(
                net, order, lambda ch, co: G.at[ch, co, r],
                lambda ch, co: gr.at[i, ch, co], lambda ch, kind: gs.at[i, ch, kind], done)

        interleave(
            wgen(),
            to_all(net, lambda t: a_ref, lambda s: A.at[s], lambda s: ar.at[s], lambda k: as_.at[k], done),
            col_ag(net, t_ref, lambda s, h: X.at[s, h], lambda s, h: xr.at[s, h], lambda w, s, h: xs.at[w, s, h], done),
            ogen(0, (1, 2)), ogen(1, (2, 1)), ggen(0, ORDER_A), ggen(1, ORDER_B))
        for f in done:
            f()

    S = jax.ShapeDtypeStruct
    return pl.pallas_call(
        kernel,
        out_shape=(S((2, 2, T, D), BF), S((Z, plane, 2, R, C), BF), S((plane, 2, HR, D), BF), S((nd, AR, AW), BF),
                   S((n_expert, 2, T, D), BF)),
        in_specs=[VM, VM, VM, VM, VM], out_specs=(ANY,) * 5,
        scratch_shapes=[DMA((2, 2)), DMA((3, 2, 2)), DMA((Z,)), DMA((Z,)), DMA((2, plane, 2)), DMA((2, plane, 7)),
                        DMA((2, plane, 2)), DMA((2, plane, 7)), DMA((nd,)), DMA((nd,)),
                        DMA((2, n_expert, 2)), DMA((2, n_expert, 7)), DMA((4,))],
        compiler_params=params(cid), name="gather_start",
    )(tokens, wqkv, w_out, aux, cot)


def column_sum(n_expert, part, cid):
    _, _, T, D = part.shape

    def kernel(p_ref, o_ref, acc, buf, fin, rsem, ssem):
        net = Net(n_expert).enter()
        greet(net, (0,))
        done = []
        interleave(col_rs(
            net, lambda s, h: p_ref.at[s, h], o_ref, lambda w, s, h: acc.at[w, s, h], lambda w, s, h: buf.at[w, s, h],
            lambda i: fin.at[i], lambda w, s, h: rsem.at[w, s, h], lambda w, s, h: ssem.at[w, s, h], T, done))
        for f in done:
            f()

    return pl.pallas_call(
        kernel, out_shape=jax.ShapeDtypeStruct((T, D), BF), in_specs=[VM], out_specs=VM,
        scratch_shapes=[pltpu.VMEM((2, 2, 2, T, D), BF), pltpu.VMEM((2, 2, 2, T, D), BF), pltpu.VMEM((2, T, D), BF),
                        DMA((3, 2, 2)), DMA((3, 2, 2))],
        compiler_params=params(cid, 40 << 20), name="column_sum",
    )(part)


def column_gather(n_expert, x, cid):
    T, D = x.shape

    def kernel(x_ref, X, rsem, ssem):
        net = Net(n_expert).enter()
        greet(net, (0,))
        done = []
        interleave(col_ag(net, x_ref, lambda s, h: X.at[s, h], lambda s, h: rsem.at[s, h], lambda w, s, h: ssem.at[w, s, h], done))
        for f in done:
            f()

    return pl.pallas_call(
        kernel, out_shape=jax.ShapeDtypeStruct((2, 2, T, D), BF), in_specs=[VM], out_specs=ANY,
        scratch_shapes=[DMA((2, 2)), DMA((3, 2, 2))],
        compiler_params=params(cid), name="column_gather",
    )(x)


def gather_all(n_expert, x, aux, cid):
    rows, cols = x.shape
    half = rows // 2
    nd = 2 * n_expert

    def kernel(x_ref, a_ref, o_ref, A, rsem, ssem, ar, as_, lsem):
        net = Net(n_expert).enter()
        me = net.e * 2 + net.c
        done = []
        local_copy(x_ref, o_ref.at[net.e, net.c], lsem.at[0], [])
        local_copy(a_ref, A.at[me], lsem.at[1], done)
        greet_all(net)
        pltpu.make_async_copy(x_ref, o_ref.at[net.e, net.c], lsem.at[0]).wait()
        gens = [to_all(net, lambda t: a_ref, lambda s: A.at[s], lambda s: ar.at[s], lambda k: as_.at[k], done)]
        for i, order in enumerate((ORDER_A, ORDER_B)):
            gens.append(ag_piece(
                net, order,
                lambda ch, co, i=i: o_ref.at[ch, co, pl.ds(i * half, half)],
                lambda ch, co, i=i: rsem.at[i, ch, co],
                lambda ch, kind, i=i: ssem.at[i, ch, kind], done))
        interleave(*gens)
        for f in done:
            f()

    return pl.pallas_call(
        kernel,
        out_shape=(jax.ShapeDtypeStruct((n_expert, 2, rows, cols), x.dtype), jax.ShapeDtypeStruct((nd,) + aux.shape, aux.dtype)),
        in_specs=[VM, VM], out_specs=(ANY, ANY),
        scratch_shapes=[DMA((2, n_expert, 2)), DMA((2, n_expert, 7)), DMA((nd,)), DMA((nd,)), DMA((2,))],
        compiler_params=params(cid), name="gather_all",
    )(x, aux)


def exchange(n_expert, x, cid):
    nd = 2 * n_expert

    def kernel(x_ref, o_ref, ar, as_, lsem):
        net = Net(n_expert).enter()
        me = net.e * 2 + net.c
        done = []
        local_copy(x_ref.at[me], o_ref.at[me], lsem.at[0], done)
        greet_all(net)
        interleave(to_all(net, lambda t: x_ref.at[t], lambda s: o_ref.at[s], lambda s: ar.at[s], lambda k: as_.at[k], done))
        for f in done:
            f()

    return pl.pallas_call(
        kernel, out_shape=jax.ShapeDtypeStruct(x.shape, x.dtype), in_specs=[VM], out_specs=VM,
        scratch_shapes=[DMA((nd,)), DMA((nd,)), DMA((2,))],
        compiler_params=params(cid), name="exchange",
    )(x)


def reduce_end(n_expert, part, dw, do, small, cid):
    _, _, T, D = part.shape
    Z, plane, _, R, C = dw.shape
    HR = do.shape[2]
    nd = 2 * n_expert
    net0 = Net(n_expert)
    orders = ((2, 1), (1, 2))
    keys = [rs_keys(net0, o) for o in orders]
    sizes = keys[0][1]
    ns = max([plane] + sizes)
    hr = HR // 2

    def kernel(p_ref, dw_ref, do_ref, s_ref, x_out, w_out, o_out, s_out,
               acc, buf, fin, wacc, wb0, wb1, oacc, ob0, ob1, wsh,
               xr, xs, wr, ws, our, ous, sr, s_s, zr, zs, loc):
        net = Net(n_expert).enter()
        z, p, c = net.at[0], net.e % plane, net.c
        me = net.e * 2 + c
        done = []
        local_copy(s_ref.at[me], s_out.at[me], loc.at[0], done)
        greet_all(net)

        def wgen(q):
            i = q // (Z // 2)
            key = keys[i][0]
            bb = (wb0, wb1)
            yield from rs_piece(
                net, orders[i], lambda ch, co: dw_ref.at[q, ch % plane, co], lambda ch: wacc.at[q, ch % plane],
                lambda st, k: bb[st].at[q, k], key, lambda st, k: wr.at[q, st, k if st else k % plane],
                lambda st, k: ws.at[q, st, k if st else k % plane], R, done)
            mk = lambda: rcopy(wacc.at[q, p], wsh.at[z], zs.at[q], zr.at[z], (q * plane + p, c))
            pl.when(z != q)(lambda: mk().start())
            done.append(lambda: pl.when(z != q)(lambda: mk().wait_send()))
            pl.when(z == q)(lambda: sum_to(w_out.at[q], [wacc.at[q, p]], R))

        def ogen(i):
            key = keys[i][0]
            bb = (ob0, ob1)
            r = pl.ds(i * hr, hr)
            yield from rs_piece(
                net, orders[i], lambda ch, co: do_ref.at[ch % plane, co, r], lambda ch: oacc.at[ch % plane, r],
                lambda st, k: bb[st].at[k, r], key, lambda st, k: our.at[i, st, k if st else k % plane],
                lambda st, k: ous.at[i, st, k if st else k % plane], hr, done)

        interleave(
            to_all(net, lambda t: s_ref.at[t], lambda s: s_out.at[s], lambda s: sr.at[s], lambda k: s_s.at[k], done),
            *[wgen(q) for q in range(Z)],
            col_rs(net, lambda s, h: p_ref.at[s, h], x_out, lambda w, s, h: acc.at[w, s, h], lambda w, s, h: buf.at[w, s, h],
                   lambda i: fin.at[i], lambda w, s, h: xr.at[w, s, h], lambda w, s, h: xs.at[w, s, h], T, done),
            ogen(0), ogen(1))
        o_out[...] = oacc[p]
        for k in range(1, Z):
            o = (z + k) % Z
            rcopy(wsh.at[o], wsh.at[o], zs.at[0], zr.at[o], (net.e, c)).wait_recv()
            sum_to(w_out.at[o], [wsh.at[o]], R)
        for f in done:
            f()

    S = jax.ShapeDtypeStruct
    V = pltpu.VMEM
    return pl.pallas_call(
        kernel, out_shape=(S((T, D), BF), S((Z, R, C), BF), S((HR, D), BF), S(small.shape, small.dtype)),
        in_specs=[VM] * 4, out_specs=(VM,) * 4,
        scratch_shapes=[V((2, 2, 2, T, D), BF), V((2, 2, 2, T, D), BF), V((2, T, D), BF),
                        V((Z, plane, R, C), BF), V((Z, sizes[0], R, C), BF), V((Z, sizes[1], R, C), BF),
                        V((plane, HR, D), BF), V((sizes[0], HR, D), BF), V((sizes[1], HR, D), BF), V((Z, R, C), BF),
                        DMA((3, 2, 2)), DMA((3, 2, 2)), DMA((Z, 3, ns)), DMA((Z, 3, ns)), DMA((2, 3, ns)), DMA((2, 3, ns)),
                        DMA((nd,)), DMA((nd,)), DMA((Z,)), DMA((Z,)), DMA((1,))],
        compiler_params=params(cid, 60 << 20), name="reduce_end",
    )(part, dw, do, small)


MODEL_WIDTH = 2048
QUERY_HEADS = 32
KEY_VALUE_HEADS = 4
HEAD_SIZE = 128
GROUP = QUERY_HEADS // KEY_VALUE_HEADS
TOP = 8
EXP_DEV = 2

epsilon = 1e-06
rope_base = 1000000.0


def norm_parts(values_in, gain_vec):
    inverse = lax.rsqrt(jnp.mean(values_in * values_in, axis=-1, keepdims=True) + epsilon)
    return (values_in * inverse * gain_vec, inverse)


def norm_back(values_in, inverse, gain_vec, grad_out):
    scaled = grad_out * gain_vec
    grad_in = inverse * (
        scaled
        - values_in * inverse * inverse * jnp.mean(scaled * values_in, axis=-1, keepdims=True)
    )
    return (grad_in, grad_out * values_in * inverse)


def rope_tables(positions):
    exponent = jnp.arange(HEAD_SIZE // 2).astype(F32) * (2.0 / HEAD_SIZE)
    frequency = jnp.exp(-math.log(rope_base) * exponent)
    angles = positions.astype(F32)[:, None] * frequency[None, :]
    return (jnp.cos(angles), jnp.sin(angles))


def rotate(v, cos, sin):
    half = v.shape[-1] // 2
    a, b = v[..., :half], v[..., half:]
    return jnp.concatenate([a * cos - b * sin, b * cos + a * sin], axis=-1)


def rotate_back(v, cos, sin):
    half = v.shape[-1] // 2
    a, b = v[..., :half], v[..., half:]
    return jnp.concatenate([a * cos + b * sin, b * cos - a * sin], axis=-1)


def mm(a, b):
    return jnp.dot(a, b, preferred_element_type=F32)


def ein(spec, *args):
    return jnp.einsum(spec, *args, preferred_element_type=F32)


def local(
    n_expert, tokens, routes, documents, w_query, key_projection, value_projection, w_out, w_router,
    gain_attn, gain_ffn, gain_query, gain_key, w_gate, w_up, w_down, cotangent,
):
    Z = KEY_VALUE_HEADS
    plane = n_expert // Z
    nd = 2 * n_expert
    T, D = tokens.shape
    R, HR, E = w_query.shape[0], w_out.shape[0], w_router.shape[1]
    Q = gain_query.shape[0]
    KV = HEAD_SIZE
    GQ = GROUP * HEAD_SIZE
    e, c = lax.axis_index("expert"), lax.axis_index("context")
    z, p = e // plane, e % plane
    capacity = T * TOP * 5 // (4 * E)
    score_scale = HEAD_SIZE ** (-0.5)

    wqkv = jnp.concatenate(
        [w_query.reshape(R, Z, GQ), key_projection.reshape(R, Z, KV), value_projection.reshape(R, Z, KV)], axis=-1
    ).transpose(1, 0, 2)
    width = -(-(E + 4) // 128) * 128
    pad = lambda v: jnp.pad(v, (0, R - v.shape[0]))[:, None]
    head = jnp.concatenate(
        [w_router, gain_attn[:, None], gain_ffn[:, None], pad(gain_query), pad(gain_key), jnp.zeros((R, width - E - 4), BF)], axis=1
    )
    docs_own = lax.dynamic_slice_in_dim(documents[0], c * T, T).astype(BF)[None]
    docs_own = jnp.pad(docs_own, ((0, 15), (0, width - T)))
    aux = jnp.concatenate([head, docs_own], axis=0)
    X, W, O, A, G = gather_start(n_expert, tokens, wqkv, w_out, aux, cotangent, 0)
    W = W.reshape(D, GQ + 2 * KV)
    O = O.reshape(GQ, D)
    table = A[:, :R].reshape(D, width)
    router_weight = table[:, :E]
    attn_gain = table[:, E].astype(F32)
    ffn_gain = table[:, E + 1].astype(F32)
    query_gain = A[:, :Q, E + 2].reshape(HEAD_SIZE).astype(F32)
    key_gain = A[:, :Q, E + 3].reshape(HEAD_SIZE).astype(F32)
    docs = A[:, R, :T].reshape(Z, plane, 2 * T)
    docs = lax.dynamic_slice(docs, (2 * c, p, 0), (2, 1, 2 * T)).reshape(2, 2 * T)

    L = 2 * T
    x = X.reshape(2 * L, D).astype(F32)
    normed, inverse_attn = norm_parts(x, attn_gain)
    first_in = normed.astype(BF)
    raw = mm(first_in, W)
    query_raw = raw[:, :GQ].reshape(2, L, GROUP, HEAD_SIZE)
    key_raw = raw[:, GQ:GQ + KV].reshape(2, L, HEAD_SIZE)
    value = raw[:, GQ + KV:].reshape(2, L, HEAD_SIZE).astype(BF)
    cos, sin = rope_tables(jnp.arange(L, dtype=jnp.int32))
    qcos, qsin = cos[:, None, :], sin[:, None, :]
    query_normed, query_inverse = norm_parts(query_raw, query_gain)
    queries = rotate(query_normed, qcos, qsin).astype(BF)
    key_normed, key_inverse = norm_parts(key_raw, key_gain)
    keys = rotate(key_normed, cos, sin).astype(BF)
    places = jnp.arange(L, dtype=jnp.int32)
    allowed = (places[:, None] >= places[None, :])[None] & (docs[:, :, None] == docs[:, None, :])
    scores = ein("sqhd,skd->shqk", queries, keys) * score_scale
    scores = jnp.where(allowed[:, None], scores, -1e30)
    top = jnp.max(scores, axis=-1, keepdims=True)
    ex = jnp.exp(scores - top)
    probs = ex / jnp.sum(ex, axis=-1, keepdims=True)
    probs_low = probs.astype(BF)
    attended = ein("shqk,skd->sqhd", probs_low, value).reshape(2 * L, GQ).astype(BF)
    part = mm(attended, O).astype(BF).reshape(2, 2, T, D)
    middle = tokens.astype(F32) + column_sum(n_expert, part, 1).astype(F32)

    normed_ffn, inverse_ffn = norm_parts(middle, ffn_gain)
    second_in = normed_ffn.astype(BF)
    logits = mm(second_in, router_weight)
    ids = jnp.arange(E, dtype=jnp.int32)
    chosen = jnp.any(routes[:, :, None] == ids[None, None, :], axis=1)
    masked = jnp.where(chosen, logits, -jnp.inf)
    best = jnp.max(masked, axis=-1, keepdims=True)
    ew = jnp.where(chosen, jnp.exp(logits - best), 0.0)
    weights = ew / jnp.sum(ew, axis=-1, keepdims=True)
    marked = jnp.where(chosen, weights, -1.0).T
    N, M = gather_all(n_expert, second_in, marked, 2)

    mine = lax.dynamic_slice(M, (0, EXP_DEV * e, 0), (nd, EXP_DEV, T))
    here = mine >= 0.0
    rank = jnp.cumsum(here.astype(jnp.int32), axis=-1) - 1
    slots = jnp.arange(capacity, dtype=jnp.int32)
    pick = here[:, :, None, :] & (rank[:, :, None, :] == slots[None, None, :, None])
    slot_weight = jnp.sum(jnp.where(pick, mine[:, :, None, :], 0.0), axis=-1).transpose(1, 0, 2)[..., None]
    pick = pick.astype(BF)
    N = N.reshape(nd, T, D)
    G = G.reshape(nd, T, D)
    rows = ein("sect,std->escd", pick, N).astype(BF)
    g_rows = ein("sect,std->escd", pick, G)
    flat = lambda v: v.reshape(EXP_DEV, nd * capacity, v.shape[-1])
    deep = lambda v: v.reshape(EXP_DEV, nd, capacity, v.shape[-1])
    rows = flat(rows)
    grad_rows = flat((slot_weight * g_rows).astype(BF))
    gate_value = ein("emd,edf->emf", rows, w_gate)
    up_value = ein("emd,edf->emf", rows, w_up)
    sig = jax.nn.sigmoid(gate_value)
    act = (gate_value * sig * up_value).astype(BF)
    expert_part = deep(ein("emf,efd->emd", act, w_down))
    dots = jnp.sum(g_rows * expert_part, axis=-1)
    out_part = ein("sect,escd->std", pick, (slot_weight * expert_part).astype(BF)).astype(BF)
    dots = ein("sect,esc->set", pick.astype(F32), dots)
    grad_act = ein("emd,efd->emf", grad_rows, w_down)
    grad_gate_v = (grad_act * up_value * sig * (1.0 + gate_value * (1.0 - sig))).astype(BF)
    grad_up_v = (grad_act * gate_value * sig).astype(BF)
    down_grad = ein("emf,emd->efd", act, grad_rows)
    gate_grad = ein("emd,emf->edf", rows, grad_gate_v)
    up_grad = ein("emd,emf->edf", rows, grad_up_v)
    back_rows = ein("emf,edf->emd", grad_gate_v, w_gate) + ein("emf,edf->emd", grad_up_v, w_up)
    back_part = ein("sect,escd->std", pick, deep(back_rows.astype(BF))).astype(BF)

    dots_out = jnp.pad(dots, ((0, 0), (0, 8 - EXP_DEV), (0, 0)))
    dots_in = exchange(n_expert, dots_out, 3)
    parts = max(1, n_expert // 16)

    def summed(v, cid):
        v = v.reshape(n_expert, 2, T, D)
        W_ = D // parts
        return jnp.concatenate(
            [reduce_scatter_all(n_expert, v[..., i * W_:(i + 1) * W_], cid + 2 * i) for i in range(parts)], axis=1).astype(F32)

    back_sum = summed(back_part, 8)
    out_sum = summed(out_part, 9)

    block_out = (middle + out_sum).astype(BF)
    grad_result = cotangent.astype(F32)
    grad_weights = jnp.sum(dots_in[:, :EXP_DEV].reshape(n_expert, 2, EXP_DEV, T), axis=1).reshape(E, T).T
    grad_chosen = weights * (grad_weights - jnp.sum(weights * grad_weights, axis=-1, keepdims=True))
    grad_logits = jnp.where(chosen, grad_chosen, 0.0).astype(BF)
    router_grad = mm(second_in.T, grad_logits)
    grad_second = mm(grad_logits, router_weight.T) + back_sum
    grad_middle_norm, ffn_terms = norm_back(middle, inverse_ffn, ffn_gain, grad_second)
    ffn_gain_grad = jnp.sum(ffn_terms, axis=0)
    grad_middle = grad_result + grad_middle_norm

    GA = column_gather(n_expert, grad_middle.astype(BF), 6).reshape(2 * L, D)
    out_grad = mm(attended.T, GA)
    grad_attended = ein("td,fd->tf", GA, O).astype(BF).reshape(2, L, GROUP, HEAD_SIZE)
    grad_probs = ein("sqhd,skd->shqk", grad_attended, value)
    grad_scores = (probs * (grad_probs - jnp.sum(probs * grad_probs, axis=-1, keepdims=True))).astype(BF)
    grad_queries = ein("shqk,skd->sqhd", grad_scores, keys) * score_scale
    grad_keys = ein("shqk,sqhd->skd", grad_scores, queries) * score_scale
    grad_values = ein("shqk,sqhd->skd", probs_low, grad_attended)
    grad_query_raw, query_terms = norm_back(query_raw, query_inverse, query_gain, rotate_back(grad_queries, qcos, qsin))
    grad_key_raw, key_terms = norm_back(key_raw, key_inverse, key_gain, rotate_back(grad_keys, cos, sin))
    grad_raw = jnp.concatenate(
        [grad_query_raw.reshape(2 * L, GQ).astype(BF), grad_key_raw.reshape(2 * L, KV).astype(BF),
         grad_values.reshape(2 * L, KV).astype(BF)], axis=-1)
    query_gain_grad = jnp.sum(query_terms, axis=(0, 1, 2))
    key_gain_grad = jnp.sum(key_terms, axis=(0, 1))
    grad_first = ein("tf,df->td", grad_raw, W)
    raw_grad = mm(first_in.T, grad_raw)
    attn_gain_grad = jnp.sum(grad_first * x * inverse_attn, axis=0)

    small = jnp.concatenate([
        router_grad.reshape(nd, R * E), attn_gain_grad.reshape(nd, R), ffn_gain_grad.reshape(nd, R),
        query_gain_grad.reshape(nd, Q), key_gain_grad.reshape(nd, Q)], axis=1)
    n_small = small.shape[1]
    small = jnp.pad(small, ((0, 0), (0, -n_small % 1024))).reshape(nd, -1, 128)
    grad_first_sum, raw_sum, out_sum2, small_in = reduce_end(
        n_expert, grad_first.astype(BF).reshape(2, 2, T, D), raw_grad.astype(BF).reshape(Z, plane, 2, R, GQ + 2 * KV),
        out_grad.astype(BF).reshape(plane, 2, HR, D), small, 7)
    small_sum = jnp.sum(small_in, axis=0).reshape(-1)
    router_grad = small_sum[:R * E].reshape(R, E)
    attn_gain_grad = small_sum[R * E:R * E + R]
    ffn_gain_grad = small_sum[R * E + R:R * E + 2 * R]
    query_gain_grad = small_sum[R * E + 2 * R:R * E + 2 * R + Q]
    key_gain_grad = small_sum[R * E + 2 * R + Q:n_small]
    raw_sum = raw_sum.astype(F32)
    query_grad = raw_sum[:, :, :GQ].transpose(1, 0, 2).reshape(R, QUERY_HEADS * HEAD_SIZE)
    key_grad = raw_sum[:, :, GQ:GQ + KV].transpose(1, 0, 2).reshape(R, Z * KV)
    value_grad = raw_sum[:, :, GQ + KV:].transpose(1, 0, 2).reshape(R, Z * KV)

    own = tokens.astype(F32)
    inverse_own = lax.rsqrt(jnp.mean(own * own, axis=-1, keepdims=True) + epsilon)
    grad_in, _ = norm_back(own, inverse_own, attn_gain, grad_first_sum.astype(F32))
    grad_tokens = grad_middle + grad_in
    return (
        block_out, grad_tokens, query_grad, key_grad, value_grad, out_sum2.astype(F32), router_grad,
        attn_gain_grad, ffn_gain_grad, query_gain_grad, key_gain_grad, gate_grad, up_grad, down_grad,
    )


def solution(mesh):
    row = P(("expert", "context"), None)
    vec = P(("expert", "context"))
    hidden = P("expert", None, "context")
    return jax.shard_map(
        functools.partial(local, mesh.shape["expert"]),
        mesh=mesh,
        in_specs=(row, row, P("expert", None), row, row, row, row, row, vec, vec, vec, vec, hidden, hidden,
                  P("expert", "context", None), row),
        out_specs=(row, row, row, row, row, row, row, vec, vec, vec, vec, hidden, hidden, P("expert", "context", None)),
        check_vma=False,
    )
```

```python
import functools
import math

import jax
import jax.numpy as jnp
from jax import lax
from jax.experimental import pallas as pl
from jax.experimental.pallas import tpu as pltpu
from jax.sharding import PartitionSpec as P

MESH_ID = pl.DeviceIdType.MESH
BF = jnp.bfloat16
F32 = jnp.float32


class Net:
    def __init__(self, n_expert):
        side = math.isqrt(n_expert // 4)
        self.dims = (4, side, side)
        self.chips = n_expert

    def enter(self):
        e = lax.axis_index("expert")
        _, A, B = self.dims
        self.e = e
        self.at = (e // (A * B), (e // B) % A, e % B)
        self.c = lax.axis_index("context")
        return self

    def chip(self, at):
        _, A, B = self.dims
        return (at[0] * A + at[1]) * B + at[2]

    def moved(self, axis, to):
        at = list(self.at)
        at[axis] = to
        return tuple(at)

    def near(self, axis):
        n, p = self.dims[axis], self.at[axis]
        if n == 2:
            return [(None, 1 - p)]
        return [(p < n - 1, p + 1), (p > 0, p - 1)]


def when(cond, fn):
    if cond is None:
        fn()
    else:
        pl.when(cond)(fn)


def rcopy(src, dst, ss, rs, dev):
    return pltpu.make_async_remote_copy(
        src_ref=src, dst_ref=dst, send_sem=ss, recv_sem=rs, device_id=dev, device_id_type=MESH_ID
    )


def greet(net, axes, partner=True):
    bar = pltpu.get_barrier_semaphore()
    count = 0
    for axis in axes:
        for cond, to in net.near(axis):
            dev = (net.chip(net.moved(axis, to)), net.c)
            when(cond, lambda dev=dev: pl.semaphore_signal(bar, inc=1, device_id=dev, device_id_type=MESH_ID))
            count = count + (1 if cond is None else jnp.where(cond, 1, 0))
    if partner:
        pl.semaphore_signal(bar, inc=1, device_id=(net.e, 1 - net.c), device_id_type=MESH_ID)
        count = count + 1
    pl.semaphore_wait(bar, count)


def greet_all(net):
    bar = pltpu.get_barrier_semaphore()
    total = net.chips * 2
    me = net.e * 2 + net.c

    def body(k, _):
        t = (me + k) % total
        pl.semaphore_signal(bar, inc=1, device_id=(t // 2, t % 2), device_id_type=MESH_ID)
        return 0

    lax.fori_loop(1, total, body, 0)
    pl.semaphore_wait(bar, total - 1)


def interleave(*gens):
    gens = list(gens)
    while gens:
        for g in list(gens):
            try:
                next(g)
            except StopIteration:
                gens.remove(g)


def ag_piece(net, order, block, rs, ss, done, partner=True):
    def send(cond, at, kind, dev):
        ch = net.chip(at)
        mk = lambda: rcopy(block(ch, net.c), block(ch, net.c), ss(ch, kind), rs(ch, net.c), dev)
        when(cond, lambda: mk().start())
        return lambda: when(cond, lambda: mk().wait_send())

    def spread(at, stage):
        outs = []
        for i in range(stage, len(order)):
            axis = order[i]
            for k, (cond, to) in enumerate(net.near(axis)):
                outs.append(send(cond, at, 2 * i + k, (net.chip(net.moved(axis, to)), net.c)))
        if partner:
            outs.append(send(None, at, 6, (net.e, 1 - net.c)))
        return outs

    done.extend(spread(net.at, 0))
    yield
    known = [(None, net.at)]

    for i, axis in enumerate(order):
        n, p = net.dims[axis], net.at[axis]
        fresh = []
        if n == 2:
            steps = [(None, 1 - p, None)]
        else:
            steps = []
            for k in range(1, n):
                steps.append((p - k >= 0, p - k, 0))
                steps.append((p + k <= n - 1, p + k, 1))
        for cond, o, way in steps:
            for kcond, kat in known:
                at = list(kat)
                at[axis] = o
                at = tuple(at)
                both = cond if kcond is None else (kcond if cond is None else jnp.logical_and(cond, kcond))

                def onward(at, way, i, axis):
                    outs = []
                    if way is not None:
                        cond2, to = net.near(axis)[way]
                        outs.append((cond2, 2 * i + way, (net.chip(net.moved(axis, to)), net.c)))
                    for j in range(i + 1, len(order)):
                        for k, (c2, to) in enumerate(net.near(order[j])):
                            outs.append((c2, 2 * j + k, (net.chip(net.moved(order[j], to)), net.c)))
                    if partner:
                        outs.append((None, 6, (net.e, 1 - net.c)))
                    return outs

                def arrive(at=at, way=way, i=i, axis=axis):
                    ch = net.chip(at)
                    rcopy(block(ch, net.c), block(ch, net.c), ss(ch, 0), rs(ch, net.c), (net.e, net.c)).wait_recv()
                    for c2, kind, dev in onward(at, way, i, axis):
                        send(c2, at, kind, dev)

                when(both, arrive)

                def drain(at=at, way=way, i=i, axis=axis, both=both):
                    def inner():
                        ch = net.chip(at)
                        for c2, kind, dev in onward(at, way, i, axis):
                            when(c2, lambda kind=kind, dev=dev: rcopy(
                                block(ch, net.c), block(ch, net.c), ss(ch, kind), rs(ch, net.c), dev).wait_send())
                    when(both, inner)

                done.append(drain)
                fresh.append((both, at))
                yield
        known = known + fresh
    if partner:
        for kcond, kat in known:
            def theirs(kat=kat):
                ch = net.chip(kat)
                rcopy(block(ch, 1 - net.c), block(ch, 1 - net.c), ss(ch, 0), rs(ch, 1 - net.c), (net.e, net.c)).wait_recv()
            done.append(lambda kcond=kcond, theirs=theirs: when(kcond, theirs))


def add_into(dst, src, rows):
    step = 16
    assert rows % step == 0

    def body(i, _):
        r = pl.ds(pl.multiple_of(i * step, step), step)
        dst[r, :] = (dst[r, :].astype(F32) + src[r, :].astype(F32)).astype(BF)
        return 0

    lax.fori_loop(0, rows // step, body, 0)


def rs_piece(net, order, mine, acc, bufs, key, rs, ss, rows, done, partner=True):
    def all_combos(axes_left):
        out = [()]
        for ax in axes_left:
            out = [o + (v,) for o in out for v in range(net.dims[ax])]
        return out

    def p_send(at):
        ch = net.chip(at)
        mk = lambda: rcopy(mine(ch, 1 - net.c), acc(ch), ss(0, ch), rs(0, ch), (net.e, 1 - net.c))
        mk().start()
        done.append(lambda: mk().wait_send())

    def p_recv(at):
        ch = net.chip(at)
        rcopy(acc(ch), acc(ch), ss(0, ch), rs(0, ch), (net.e, net.c)).wait_recv()
        add_into(acc(ch), mine(ch, net.c), rows)

    stages = []
    for i, axis in enumerate(order):
        left = order[i + 1:]
        combos = all_combos(left)
        stages.append((i, axis, left, combos))

    def targets_of(i, axis, left, combo, t):
        at = list(net.at)
        at[axis] = t
        for ax, v in zip(left, combo):
            at[ax] = v
        return tuple(at)

    for i, axis, left, combos in stages:
        n, p = net.dims[axis], net.at[axis]
        for combo in combos:
            for d in range(1, n):
                t = (p + d) % n
                p_send(targets_of(i, axis, left, combo, t))
        yield
    p_send(net.at)
    yield

    for i, axis, left, combos in stages:
        n, p = net.dims[axis], net.at[axis]
        nxt = lambda to, axis=axis: (net.chip(net.moved(axis, to)), net.c)

        def gather_prev(at):
            p_recv(at)
            for i2, axis2, left2, _ in stages[:i]:
                land(i2, axis2, left2, at)

        def land(i2, axis2, left2, at):
            n2, p2 = net.dims[axis2], net.at[axis2]
            ch = net.chip(at)

            def take(way):
                k = key(i2, way, at)
                rcopy(bufs(i2, k), bufs(i2, k), ss(i2 + 1, k), rs(i2 + 1, k), (net.e, net.c)).wait_recv()
                add_into(acc(ch), bufs(i2, k), rows)

            if n2 == 2:
                take(0)
            else:
                when(p2 > 0, lambda: take(0))
                when(p2 < n2 - 1, lambda: take(1))

        for combo in combos:
            if n == 2:
                at = targets_of(i, axis, left, combo, 1 - p)
                gather_prev(at)
                ch = net.chip(at)
                k = key(i, 0, at)
                mk = lambda ch=ch, k=k, i=i: rcopy(acc(ch), bufs(i, k), ss(i + 1, k), rs(i + 1, k), nxt(1 - p))
                mk().start()
                done.append(lambda mk=mk: mk().wait_send())
                yield
            else:
                for s in range(n - 1):
                    for way in (0, 1):
                        t = n - 1 - s if way == 0 else s
                        cond = (p < t) if way == 0 else (p > t)
                        to = p + 1 if way == 0 else p - 1
                        inner_cond = (p > 0) if way == 0 else (p < n - 1)
                        at = targets_of(i, axis, left, combo, t)
                        ch, k = net.chip(at), key(i, way, at)
                        mk = lambda ch=ch, k=k, i=i, to=to: rcopy(acc(ch), bufs(i, k), ss(i + 1, k), rs(i + 1, k), nxt(to))

                        def step(at=at, ch=ch, k=k, i=i, inner_cond=inner_cond, mk=mk):
                            gather_prev(at)

                            def relay():
                                rcopy(bufs(i, k), bufs(i, k), ss(i + 1, k), rs(i + 1, k), (net.e, net.c)).wait_recv()
                                add_into(acc(ch), bufs(i, k), rows)

                            pl.when(inner_cond)(relay)
                            mk().start()

                        pl.when(cond)(step)
                        done.append(lambda cond=cond, mk=mk: pl.when(cond)(lambda: mk().wait_send()))
                        yield
    at = net.at
    p_recv(at)
    for i2, axis2, left2, _ in stages:
        n2, p2 = net.dims[axis2], net.at[axis2]
        ch = net.chip(at)

        def take(way, i2=i2):
            k = key(i2, way, at)
            rcopy(bufs(i2, k), bufs(i2, k), ss(i2 + 1, k), rs(i2 + 1, k), (net.e, net.c)).wait_recv()
            add_into(acc(ch), bufs(i2, k), rows)

        if n2 == 2:
            take(0)
        else:
            when(p2 > 0, lambda: take(0))
            when(p2 < n2 - 1, lambda: take(1))
        yield


def rs_keys(net, order):
    def size(i):
        left = order[i + 1:]
        m = 1
        for ax in left:
            m *= net.dims[ax]
        n = net.dims[order[i]]
        return m if n == 2 else 2 * n * m

    def key(i, way, at):
        left = order[i + 1:]
        k = 0
        for ax in left:
            k = k * net.dims[ax] + at[ax]
        n = net.dims[order[i]]
        if n == 2:
            return k
        return (k * n + at[order[i]]) * 2 + way

    return key, [size(i) for i in range(len(order))]


def params(cid, vmem=None):
    return pltpu.CompilerParams(collective_id=cid, has_side_effects=True, vmem_limit_bytes=vmem)


ANY = pl.BlockSpec(memory_space=pl.ANY)
VM = pl.BlockSpec(memory_space=pltpu.VMEM)
DMA = pltpu.SemaphoreType.DMA

ORDER_A = (0, 1, 2)
ORDER_B = (0, 2, 1)


def all_gather_all(n_expert, x, cid):
    rows, cols = x.shape
    half = rows // 2

    def kernel(x_ref, o_ref, rsem, ssem, lsem):
        net = Net(n_expert).enter()
        cp = pltpu.make_async_copy(x_ref, o_ref.at[net.e, net.c], lsem)
        cp.start()
        greet(net, (0, 1, 2))
        cp.wait()
        done = []
        gens = []
        for i, order in enumerate((ORDER_A, ORDER_B)):
            gens.append(ag_piece(
                net, order,
                lambda ch, co, i=i: o_ref.at[ch, co, pl.ds(i * half, half)],
                lambda ch, co, i=i: rsem.at[i, ch, co],
                lambda ch, kind, i=i: ssem.at[i, ch, kind], done))
        interleave(*gens)
        for f in done:
            f()

    return pl.pallas_call(
        kernel, out_shape=jax.ShapeDtypeStruct((n_expert, 2, rows, cols), x.dtype),
        in_specs=[VM], out_specs=ANY,
        scratch_shapes=[DMA((2, n_expert, 2)), DMA((2, n_expert, 7)), DMA],
        compiler_params=params(cid), name="gather_all",
    )(x)


def reduce_scatter_all(n_expert, t, cid):
    _, _, rows, cols = t.shape
    half = rows // 2
    net0 = Net(n_expert)
    orders = ((2, 1, 0), (1, 2, 0))
    keys = [rs_keys(net0, o) for o in orders]
    sizes = keys[0][1]
    ns = max([n_expert] + sizes)

    def kernel(t_ref, o_ref, acc, b0, b1, b2, rsem, ssem):
        net = Net(n_expert).enter()
        greet(net, (0, 1, 2))
        done, gens = [], []
        bb = (b0, b1, b2)
        for i, order in enumerate(orders):
            key = keys[i][0]
            r = pl.ds(i * half, half)
            gens.append(rs_piece(
                net, order,
                lambda ch, co, r=r: t_ref.at[ch, co, r],
                lambda ch, r=r: acc.at[ch, r],
                lambda st, k, r=r: bb[st].at[k, r],
                key,
                lambda st, k, i=i: rsem.at[i, st, k],
                lambda st, k, i=i: ssem.at[i, st, k], half, done))
        interleave(*gens)
        o_ref[...] = acc[net.e]
        for f in done:
            f()

    return pl.pallas_call(
        kernel, out_shape=jax.ShapeDtypeStruct((rows, cols), BF),
        in_specs=[VM], out_specs=VM,
        scratch_shapes=[pltpu.VMEM((n_expert, rows, cols), BF)]
        + [pltpu.VMEM((s, rows, cols), BF) for s in sizes]
        + [DMA((2, 4, ns)), DMA((2, 4, ns))],
        compiler_params=params(cid, 60 << 20), name="reduce_all",
    )(t)


def local_copy(src, dst, sem, done):
    cp = lambda: pltpu.make_async_copy(src, dst, sem)
    cp().start()
    done.append(lambda: cp().wait())


def col_ag(net, src, dst, rs, ss, done):
    z, c = net.at[0], net.c
    n = net.dims[0]
    own = z // 2 == c
    s0 = z % 2

    def zdev(to):
        return (net.chip(net.moved(0, to)), c)

    def hop(cond, s, h, way, to, source=None):
        mk = lambda: rcopy(dst(s, h) if source is None else source, dst(s, h), ss(way, s, h), rs(s, h), zdev(to))
        when(cond, lambda: mk().start())
        return lambda: when(cond, lambda: mk().wait_send())

    def arrived(s, h):
        rcopy(dst(s, h), dst(s, h), ss(0, s, h), rs(s, h), (net.e, c)).wait_recv()

    across = lambda: rcopy(src, dst(s0, c), ss(2, 0, 0), rs(s0, c), (net.e, 1 - c))
    keep = lambda: pltpu.make_async_copy(src, dst(s0, c), ss(2, 0, 1))

    def begin():
        keep().start()
        hop(z < n - 1, s0, c, 0, z + 1, src)
        hop(z > 0, s0, c, 1, z - 1, src)

    pl.when(own)(begin)
    pl.when(jnp.logical_not(own))(lambda: across().start())
    yield

    def second():
        arrived(s0, 1 - c)
        hop(z < n - 1, s0, 1 - c, 0, z + 1)
        hop(z > 0, s0, 1 - c, 1, z - 1)

    pl.when(own)(second)
    yield

    def end():
        keep().wait()
        for h in (c, 1 - c):
            source = src if h is c else None
            when(z < n - 1, lambda h=h, source=source: rcopy(
                src if source is not None else dst(s0, h), dst(s0, h), ss(0, s0, h), rs(s0, h), zdev(z + 1)).wait_send())
            when(z > 0, lambda h=h, source=source: rcopy(
                src if source is not None else dst(s0, h), dst(s0, h), ss(1, s0, h), rs(s0, h), zdev(z - 1)).wait_send())

    done.append(lambda: pl.when(own)(end))
    done.append(lambda: pl.when(jnp.logical_not(own))(lambda: across().wait_send()))

    for k in range(1, n):
        for way in (0, 1):
            o = z - k if way == 0 else z + k
            inside = o >= 0 if way == 0 else o <= n - 1
            cond = jnp.logical_and(inside, o // 2 == c)
            more = z < n - 1 if way == 0 else z > 0
            to = z + 1 if way == 0 else z - 1

            def step(o=o, way=way, more=more, to=to):
                for h in (0, 1):
                    arrived(o % 2, h)
                    hop(more, o % 2, h, way, to)

            def finish(o=o, way=way, more=more, to=to):
                for h in (0, 1):
                    when(more, lambda h=h: rcopy(
                        dst(o % 2, h), dst(o % 2, h), ss(way, o % 2, h), rs(o % 2, h), zdev(to)).wait_send())

            pl.when(cond)(step)
            done.append(lambda cond=cond, finish=finish: pl.when(cond)(finish))
            yield


def col_rs(net, part, out, acc, buf, fin, rs, ss, rows, done):
    z, c = net.at[0], net.c
    n = net.dims[0]

    def zdev(to):
        return (net.chip(net.moved(0, to)), c)

    def msg(way, s, h, to):
        return rcopy(acc(way, s, h), buf(way, s, h), ss(way, s, h), rs(way, s, h), zdev(to))

    def arrived(way, s, h):
        rcopy(buf(way, s, h), buf(way, s, h), ss(way, s, h), rs(way, s, h), (net.e, c)).wait_recv()

    for k in range(n - 1):
        for way in (0, 1):
            t = n - 1 - k if way == 0 else k
            s = t % 2
            cond = jnp.logical_and(z < t if way == 0 else z > t, t // 2 == c)
            inner = z > 0 if way == 0 else z < n - 1
            to = z + 1 if way == 0 else z - 1
            for h in (0, 1):
                def step(way=way, s=s, h=h, inner=inner, to=to):
                    def relay():
                        arrived(way, s, h)
                        sum_to(acc(way, s, h), [part(s, h), buf(way, s, h)], rows)

                    pl.when(inner)(relay)
                    pl.when(jnp.logical_not(inner))(lambda: sum_to(acc(way, s, h), [part(s, h)], rows))
                    msg(way, s, h, to).start()

                pl.when(cond)(step)
                done.append(lambda cond=cond, way=way, s=s, h=h, to=to: pl.when(cond)(lambda: msg(way, s, h, to).wait_send()))
                yield

    own = z // 2 == c
    s0 = z % 2
    cross = lambda: rcopy(fin(0), fin(1), ss(2, 0, 0), rs(2, 0, 0), (net.e, 1 - c))

    def last(h, to_ref):
        low, high = z > 0, z < n - 1
        pl.when(low)(lambda: arrived(0, s0, h))
        pl.when(high)(lambda: arrived(1, s0, h))
        mid = jnp.logical_and(low, high)
        pl.when(mid)(lambda: sum_to(to_ref, [part(s0, h), buf(0, s0, h), buf(1, s0, h)], rows))
        pl.when(jnp.logical_not(low))(lambda: sum_to(to_ref, [part(s0, h), buf(1, s0, h)], rows))
        pl.when(jnp.logical_not(high))(lambda: sum_to(to_ref, [part(s0, h), buf(0, s0, h)], rows))

    def final():
        last(1 - c, fin(0))
        cross().start()
        last(c, out)

    pl.when(own)(final)
    done.append(lambda: pl.when(own)(lambda: cross().wait_send()))

    def take():
        cross().wait_recv()
        sum_to(out, [fin(1)], rows)

    yield
    pl.when(jnp.logical_not(own))(take)


def sum_to(dst, srcs, rows):
    step = 16

    def body(i, _):
        r = pl.ds(pl.multiple_of(i * step, step), step)
        v = srcs[0][r, :]
        if len(srcs) > 1:
            v = v.astype(F32)
            for s in srcs[1:]:
                v = v + s[r, :].astype(F32)
        dst[r, :] = v.astype(BF)
        return 0

    lax.fori_loop(0, rows // step, body, 0)


def to_all(net, src, dst, rs, ss, done):
    total = net.chips * 2
    me = net.e * 2 + net.c

    def put(k, _):
        t = (me + k) % total
        rcopy(src(t), dst(me), ss(k), rs(me), (t // 2, t % 2)).start()
        return 0

    lax.fori_loop(1, total, put, 0)
    yield

    def take(k, _):
        t = (me + k) % total
        rcopy(src(t), dst(me), ss(k), rs(me), (t // 2, t % 2)).wait_send()
        rcopy(dst(t), dst(t), ss(k), rs(t), (net.e, net.c)).wait_recv()
        return 0

    done.append(lambda: lax.fori_loop(1, total, take, 0))


def gather_start(n_expert, tokens, wqkv, w_out, aux, cot, cid):
    T, D = tokens.shape
    Z, R, C = wqkv.shape
    HR = w_out.shape[0]
    AR, AW = aux.shape
    plane = n_expert // Z
    nd = 2 * n_expert

    with_g = cot is not None

    def kernel(*refs):
        k = 5 if with_g else 4
        t_ref, w_ref, o_ref, a_ref = refs[:4]
        g_ref, G = (refs[4], refs[2 * k - 1]) if with_g else (None, None)
        X, W, O, A = refs[k:k + 4]
        xr, xs, wr, ws, war, was, oar, oas, ar, as_, gr, gs, loc = refs[2 * k:]
        net = Net(n_expert).enter()
        z, p, c = net.at[0], net.e % plane, net.c
        me = net.e * 2 + c
        done = []
        local_copy(w_ref.at[z], W.at[z, p, c], loc.at[0], [])
        local_copy(o_ref, O.at[p, c], loc.at[1], [])
        local_copy(a_ref, A.at[me], loc.at[2], done)
        if with_g:
            local_copy(g_ref, G.at[net.e, c], loc.at[3], [])
        greet_all(net)

        def wgen():
            for k in range(1, Z):
                j = (z + k) % Z
                mk = lambda j=j, k=k: rcopy(w_ref.at[j], W.at[z, p, c], ws.at[k], wr.at[z], (j * plane + p, c))
                mk().start()
                done.append(lambda mk=mk: mk().wait_send())
            yield
            pltpu.make_async_copy(w_ref.at[z], W.at[z, p, c], loc.at[0]).wait()
            for k in range(1, Z):
                o = (z + k) % Z
                rcopy(W.at[o, p, c], W.at[o, p, c], ws.at[k], wr.at[o], (net.e, c)).wait_recv()
            gens = []
            for i, order in enumerate(((1, 2), (2, 1))):
                r = pl.ds(i * (Z // 2), Z // 2)
                gens.append(ag_piece(
                    net, order, lambda ch, co, r=r: W.at[r, ch % plane, co],
                    lambda ch, co, i=i: war.at[i, ch % plane, co], lambda ch, kind, i=i: was.at[i, ch % plane, kind], done))
            while gens:
                for g in list(gens):
                    try:
                        next(g)
                        yield
                    except StopIteration:
                        gens.remove(g)

        def ogen(i, order):
            if i == 0:
                pltpu.make_async_copy(o_ref, O.at[p, c], loc.at[1]).wait()
            r = pl.ds(i * (HR // 2), HR // 2)
            yield from ag_piece(
                net, order, lambda ch, co: O.at[ch % plane, co, r],
                lambda ch, co: oar.at[i, ch % plane, co], lambda ch, kind: oas.at[i, ch % plane, kind], done)

        def ggen(i, order):
            if i == 0:
                pltpu.make_async_copy(g_ref, G.at[net.e, c], loc.at[3]).wait()
            r = pl.ds(i * (T // 2), T // 2)
            yield from ag_piece(
                net, order, lambda ch, co: G.at[ch, co, r],
                lambda ch, co: gr.at[i, ch, co], lambda ch, kind: gs.at[i, ch, kind], done)

        interleave(
            wgen(),
            to_all(net, lambda t: a_ref, lambda s: A.at[s], lambda s: ar.at[s], lambda k: as_.at[k], done),
            col_ag(net, t_ref, lambda s, h: X.at[s, h], lambda s, h: xr.at[s, h], lambda w, s, h: xs.at[w, s, h], done),
            ogen(0, (1, 2)), ogen(1, (2, 1)), *([ggen(0, ORDER_A), ggen(1, ORDER_B)] if with_g else []))
        for f in done:
            f()

    S = jax.ShapeDtypeStruct
    return pl.pallas_call(
        kernel,
        out_shape=(S((2, 2, T, D), BF), S((Z, plane, 2, R, C), BF), S((plane, 2, HR, D), BF), S((nd, AR, AW), BF))
        + ((S((n_expert, 2, T, D), BF),) if with_g else ()),
        in_specs=[VM] * (5 if with_g else 4), out_specs=(ANY,) * (5 if with_g else 4),
        scratch_shapes=[DMA((2, 2)), DMA((3, 2, 2)), DMA((Z,)), DMA((Z,)), DMA((2, plane, 2)), DMA((2, plane, 7)),
                        DMA((2, plane, 2)), DMA((2, plane, 7)), DMA((nd,)), DMA((nd,)),
                        DMA((2, n_expert, 2)), DMA((2, n_expert, 7)), DMA((4,))],
        compiler_params=params(cid), name="gather_start",
    )(tokens, wqkv, w_out, aux, *((cot,) if with_g else ()))


def column_sum(n_expert, part, cid):
    _, _, T, D = part.shape

    def kernel(p_ref, o_ref, acc, buf, fin, rsem, ssem):
        net = Net(n_expert).enter()
        greet(net, (0,))
        done = []
        interleave(col_rs(
            net, lambda s, h: p_ref.at[s, h], o_ref, lambda w, s, h: acc.at[w, s, h], lambda w, s, h: buf.at[w, s, h],
            lambda i: fin.at[i], lambda w, s, h: rsem.at[w, s, h], lambda w, s, h: ssem.at[w, s, h], T, done))
        for f in done:
            f()

    return pl.pallas_call(
        kernel, out_shape=jax.ShapeDtypeStruct((T, D), BF), in_specs=[VM], out_specs=VM,
        scratch_shapes=[pltpu.VMEM((2, 2, 2, T, D), BF), pltpu.VMEM((2, 2, 2, T, D), BF), pltpu.VMEM((2, T, D), BF),
                        DMA((3, 2, 2)), DMA((3, 2, 2))],
        compiler_params=params(cid, 40 << 20), name="column_sum",
    )(part)


def column_gather(n_expert, x, cid):
    T, D = x.shape

    def kernel(x_ref, X, rsem, ssem):
        net = Net(n_expert).enter()
        greet(net, (0,))
        done = []
        interleave(col_ag(net, x_ref, lambda s, h: X.at[s, h], lambda s, h: rsem.at[s, h], lambda w, s, h: ssem.at[w, s, h], done))
        for f in done:
            f()

    return pl.pallas_call(
        kernel, out_shape=jax.ShapeDtypeStruct((2, 2, T, D), BF), in_specs=[VM], out_specs=ANY,
        scratch_shapes=[DMA((2, 2)), DMA((3, 2, 2))],
        compiler_params=params(cid), name="column_gather",
    )(x)


def gather_all(n_expert, x, aux, cid):
    rows, cols = x.shape
    half = rows // 2
    nd = 2 * n_expert

    def kernel(x_ref, a_ref, o_ref, A, rsem, ssem, ar, as_, lsem):
        net = Net(n_expert).enter()
        me = net.e * 2 + net.c
        done = []
        local_copy(x_ref, o_ref.at[net.e, net.c], lsem.at[0], [])
        local_copy(a_ref, A.at[me], lsem.at[1], done)
        greet_all(net)
        pltpu.make_async_copy(x_ref, o_ref.at[net.e, net.c], lsem.at[0]).wait()
        gens = [to_all(net, lambda t: a_ref, lambda s: A.at[s], lambda s: ar.at[s], lambda k: as_.at[k], done)]
        for i, order in enumerate((ORDER_A, ORDER_B)):
            gens.append(ag_piece(
                net, order,
                lambda ch, co, i=i: o_ref.at[ch, co, pl.ds(i * half, half)],
                lambda ch, co, i=i: rsem.at[i, ch, co],
                lambda ch, kind, i=i: ssem.at[i, ch, kind], done))
        interleave(*gens)
        for f in done:
            f()

    return pl.pallas_call(
        kernel,
        out_shape=(jax.ShapeDtypeStruct((n_expert, 2, rows, cols), x.dtype), jax.ShapeDtypeStruct((nd,) + aux.shape, aux.dtype)),
        in_specs=[VM, VM], out_specs=(ANY, ANY),
        scratch_shapes=[DMA((2, n_expert, 2)), DMA((2, n_expert, 7)), DMA((nd,)), DMA((nd,)), DMA((2,))],
        compiler_params=params(cid), name="gather_all",
    )(x, aux)


def exchange(n_expert, x, cid):
    nd = 2 * n_expert

    def kernel(x_ref, o_ref, ar, as_, lsem):
        net = Net(n_expert).enter()
        me = net.e * 2 + net.c
        done = []
        local_copy(x_ref.at[me], o_ref.at[me], lsem.at[0], done)
        greet_all(net)
        interleave(to_all(net, lambda t: x_ref.at[t], lambda s: o_ref.at[s], lambda s: ar.at[s], lambda k: as_.at[k], done))
        for f in done:
            f()

    return pl.pallas_call(
        kernel, out_shape=jax.ShapeDtypeStruct(x.shape, x.dtype), in_specs=[VM], out_specs=VM,
        scratch_shapes=[DMA((nd,)), DMA((nd,)), DMA((2,))],
        compiler_params=params(cid), name="exchange",
    )(x)


def reduce_end(n_expert, part, dw, do, small, cid):
    _, _, T, D = part.shape
    Z, plane, _, R, C = dw.shape
    HR = do.shape[2]
    nd = 2 * n_expert
    net0 = Net(n_expert)
    orders = ((2, 1), (1, 2))
    keys = [rs_keys(net0, o) for o in orders]
    sizes = keys[0][1]
    ns = max([plane] + sizes)
    hr = HR // 2

    def kernel(p_ref, dw_ref, do_ref, s_ref, x_out, w_out, o_out, s_out,
               acc, buf, fin, wacc, wb0, wb1, oacc, ob0, ob1, wsh,
               xr, xs, wr, ws, our, ous, sr, s_s, zr, zs, loc):
        net = Net(n_expert).enter()
        z, p, c = net.at[0], net.e % plane, net.c
        me = net.e * 2 + c
        done = []
        local_copy(s_ref.at[me], s_out.at[me], loc.at[0], done)
        greet_all(net)

        def wgen(q):
            i = q // (Z // 2)
            key = keys[i][0]
            bb = (wb0, wb1)
            yield from rs_piece(
                net, orders[i], lambda ch, co: dw_ref.at[q, ch % plane, co], lambda ch: wacc.at[q, ch % plane],
                lambda st, k: bb[st].at[q, k], key, lambda st, k: wr.at[q, st, k if st else k % plane],
                lambda st, k: ws.at[q, st, k if st else k % plane], R, done)
            mk = lambda: rcopy(wacc.at[q, p], wsh.at[z], zs.at[q], zr.at[z], (q * plane + p, c))
            pl.when(z != q)(lambda: mk().start())
            done.append(lambda: pl.when(z != q)(lambda: mk().wait_send()))
            pl.when(z == q)(lambda: sum_to(w_out.at[q], [wacc.at[q, p]], R))

        def ogen(i):
            key = keys[i][0]
            bb = (ob0, ob1)
            r = pl.ds(i * hr, hr)
            yield from rs_piece(
                net, orders[i], lambda ch, co: do_ref.at[ch % plane, co, r], lambda ch: oacc.at[ch % plane, r],
                lambda st, k: bb[st].at[k, r], key, lambda st, k: our.at[i, st, k if st else k % plane],
                lambda st, k: ous.at[i, st, k if st else k % plane], hr, done)

        interleave(
            to_all(net, lambda t: s_ref.at[t], lambda s: s_out.at[s], lambda s: sr.at[s], lambda k: s_s.at[k], done),
            *[wgen(q) for q in range(Z)],
            col_rs(net, lambda s, h: p_ref.at[s, h], x_out, lambda w, s, h: acc.at[w, s, h], lambda w, s, h: buf.at[w, s, h],
                   lambda i: fin.at[i], lambda w, s, h: xr.at[w, s, h], lambda w, s, h: xs.at[w, s, h], T, done),
            ogen(0), ogen(1))
        o_out[...] = oacc[p]
        for k in range(1, Z):
            o = (z + k) % Z
            rcopy(wsh.at[o], wsh.at[o], zs.at[0], zr.at[o], (net.e, c)).wait_recv()
            sum_to(w_out.at[o], [wsh.at[o]], R)
        for f in done:
            f()

    S = jax.ShapeDtypeStruct
    V = pltpu.VMEM
    return pl.pallas_call(
        kernel, out_shape=(S((T, D), BF), S((Z, R, C), BF), S((HR, D), BF), S(small.shape, small.dtype)),
        in_specs=[VM] * 4, out_specs=(VM,) * 4,
        scratch_shapes=[V((2, 2, 2, T, D), BF), V((2, 2, 2, T, D), BF), V((2, T, D), BF),
                        V((Z, plane, R, C), BF), V((Z, sizes[0], R, C), BF), V((Z, sizes[1], R, C), BF),
                        V((plane, HR, D), BF), V((sizes[0], HR, D), BF), V((sizes[1], HR, D), BF), V((Z, R, C), BF),
                        DMA((3, 2, 2)), DMA((3, 2, 2)), DMA((Z, 3, ns)), DMA((Z, 3, ns)), DMA((2, 3, ns)), DMA((2, 3, ns)),
                        DMA((nd,)), DMA((nd,)), DMA((Z,)), DMA((Z,)), DMA((1,))],
        compiler_params=params(cid, 60 << 20), name="reduce_end",
    )(part, dw, do, small)


def slot_plane(z, i):
    near = jnp.where(z < 2, z, 3 - z)
    t = jnp.where(jnp.logical_and(near == 1, i < 2), 1 - i, i)
    return jnp.where(z < 2, t, 3 - t)


class Gather22:
    def __init__(self, net, N, T, rsem, ssem):
        self.net, self.N, self.T, self.rsem, self.ssem = net, N, T, rsem, ssem
        self.axes = ((1, 2), (2, 1))

    def blk(self, piece, chip, core):
        h = self.T // 2
        return self.N.at[chip, pl.ds(pl.multiple_of(core * self.T + piece * h, h), h)]

    def copy(self, piece, at, kind, dev):
        n = self.net
        ch = n.chip(at)
        b = self.blk(piece, ch, n.c)
        return rcopy(b, b, self.ssem.at[piece, ch, kind], self.rsem.at[piece, ch, n.c], dev)

    def wait(self, piece, at, core):
        n = self.net
        ch = n.chip(at)
        b = self.blk(piece, ch, core)
        rcopy(b, b, self.ssem.at[piece, ch, 0], self.rsem.at[piece, ch, core], (n.e, n.c)).wait_recv()

    def dev(self, axis, to=None):
        n = self.net
        return (n.chip(n.moved(axis, 1 - n.at[axis] if to is None else to)), n.c)

    def level(self, piece, zt, two, three):
        n = self.net
        at = [zt, n.at[1], n.at[2]]
        u, v = self.axes[piece]
        if two:
            at[u] = 1 - at[u]
        if three:
            at[v] = 1 - at[v]
        return tuple(at)

    def outs(self, piece, zt, two, three):
        u, v = self.axes[piece]
        at = self.level(piece, zt, two, three)
        r = []
        if not two and not three:
            r.append((2, self.dev(u)))
        if not three:
            r.append((3, self.dev(v)))
        r.append((4, (self.net.e, 1 - self.net.c)))
        return at, r

    def push(self, piece, zt, two, three):
        at, r = self.outs(piece, zt, two, three)
        for kind, dev in r:
            self.copy(piece, at, kind, dev).start()

    def begin(self):
        z = self.net.at[0]
        for piece in (0, 1):
            pl.when(z < 3)(lambda piece=piece: self.copy(piece, self.net.at, 0, self.dev(0, z + 1)).start())
            pl.when(z > 0)(lambda piece=piece: self.copy(piece, self.net.at, 1, self.dev(0, z - 1)).start())
            self.push(piece, z, False, False)

    def onward(self, zt):
        z = self.net.at[0]
        to = jnp.where(zt < z, z + 1, z - 1)
        return to, jnp.logical_and(to >= 0, to <= 3)

    def from_z(self, zt):
        to, more = self.onward(zt)
        for piece in (0, 1):
            at = self.level(piece, zt, False, False)
            self.wait(piece, at, self.net.c)
            pl.when(more)(lambda piece=piece, at=at: self.copy(piece, at, 0, self.dev(0, to)).start())
            self.push(piece, zt, False, False)

    def from_two(self, zt):
        for piece in (0, 1):
            self.wait(piece, self.level(piece, zt, True, False), self.net.c)
            self.push(piece, zt, True, False)

    def from_three(self, zt):
        for two in (False, True):
            for piece in (0, 1):
                self.wait(piece, self.level(piece, zt, two, True), self.net.c)
                self.push(piece, zt, two, True)

    def from_partner(self, zt):
        for piece in (0, 1):
            for a in (0, 1):
                for b in (0, 1):
                    self.wait(piece, (zt, a, b), 1 - self.net.c)

    def drain(self, i):
        z = self.net.at[0]
        zt = slot_plane(z, i)
        to, more = self.onward(zt)
        for piece in (0, 1):
            def own(piece=piece):
                pl.when(z < 3)(lambda: self.copy(piece, self.net.at, 0, self.dev(0, z + 1)).wait_send())
                pl.when(z > 0)(lambda: self.copy(piece, self.net.at, 1, self.dev(0, z - 1)).wait_send())

            pl.when(i == 0)(own)
            at0 = self.level(piece, zt, False, False)
            pl.when(jnp.logical_and(i > 0, more))(
                lambda piece=piece, at0=at0: self.copy(piece, at0, 0, self.dev(0, to)).wait_send())
            for two in (False, True):
                for three in (False, True):
                    at, r = self.outs(piece, zt, two, three)
                    for kind, dev in r:
                        self.copy(piece, at, kind, dev).wait_send()


def add_rows(dst, srcs, rows):
    step = 32

    def body(i, _):
        r = pl.ds(pl.multiple_of(i * step, step), step)
        v = dst[r, :].astype(F32)
        for s in srcs:
            v = v + s[r, :].astype(F32)
        dst[r, :] = v.astype(BF)
        return 0

    lax.fori_loop(0, rows // step, body, 0)


class Reduce22:
    def __init__(self, net, T, acc, buf1, buf2, zbuf, sems):
        self.net, self.T = net, T
        self.acc, self.buf1, self.buf2, self.zbuf = acc, buf1, buf2, zbuf
        (self.r0, self.s0, self.r1, self.s1, self.r2, self.s2, self.r3, self.s3) = sems
        self.first = (2, 1)
        self.second = (1, 2)

    @staticmethod
    def scratch(T, D):
        V = pltpu.VMEM
        return [V((16, T, D), BF), V((4, 2, T, D), BF), V((4, T, D), BF), V((2, 4, T, D), BF),
                DMA((16,)), DMA((16,)), DMA((2, 4, 2)), DMA((2, 4, 2)), DMA((2, 4)), DMA((2, 4)), DMA((2, 2, 4)), DMA((2, 2, 4))]

    def half(self, piece):
        h = self.T // 2
        return pl.ds(piece * h, h)

    def ring(self):
        n = self.net
        a, b = n.at[1], n.at[2]
        return [(1 - a, 1 - b), (a, 1 - b), (1 - a, b), (a, b)]

    def p_copy(self, Tb, zt, ab):
        n = self.net
        p = ab[0] * 2 + ab[1]
        ch = zt * 4 + p
        src = Tb.at[p, pl.ds(pl.multiple_of((1 - n.c) * self.T, self.T), self.T)]
        return rcopy(src, self.acc.at[ch], self.s0.at[ch], self.r0.at[ch], (n.e, 1 - n.c))

    def p_send(self, Tb, zt):
        for ab in self.ring():
            self.p_copy(Tb, zt, ab).start()

    def p_wait_send(self, Tb, zt):
        for ab in self.ring():
            self.p_copy(Tb, zt, ab).wait_send()

    def p_take(self, Tb, zt, ab):
        n = self.net
        p = ab[0] * 2 + ab[1]
        self.p_copy(Tb, zt, ab).wait_recv()
        add_rows(self.acc.at[zt * 4 + p], [Tb.at[p, pl.ds(pl.multiple_of(n.c * self.T, self.T), self.T)]], self.T)

    def one(self, piece, zt, idx):
        n = self.net
        ax = self.first[piece]
        at = [zt, n.at[1], n.at[2]]
        at[ax] = 1 - at[ax]
        at[self.second[piece]] = idx
        src = self.acc.at[n.chip(at), self.half(piece)]
        dst = self.buf1.at[zt, idx, self.half(piece)]
        return rcopy(src, dst, self.s1.at[piece, zt, idx], self.r1.at[piece, zt, idx], (n.chip(n.moved(ax, 1 - n.at[ax])), n.c))

    def two(self, piece, zt):
        n = self.net
        ax = self.second[piece]
        at = [zt, n.at[1], n.at[2]]
        at[ax] = 1 - at[ax]
        src = self.acc.at[n.chip(at), self.half(piece)]
        return rcopy(src, self.buf2.at[zt, self.half(piece)], self.s2.at[piece, zt], self.r2.at[piece, zt],
                     (n.chip(n.moved(ax, 1 - n.at[ax])), n.c))

    def three(self, piece, zt):
        n = self.net
        z = n.at[0]
        up = zt > z
        d = jnp.where(up, 0, 1)
        to = jnp.where(up, z + 1, z - 1)
        src = self.acc.at[n.chip((zt, n.at[1], n.at[2])), self.half(piece)]
        return rcopy(src, self.zbuf.at[d, zt, self.half(piece)], self.s3.at[piece, d, zt], self.r3.at[piece, d, zt],
                     (n.chip(n.moved(0, to)), n.c))

    def stage0(self, Tb, zt):
        n = self.net
        order = self.ring()
        self.p_take(Tb, zt, order[0])
        self.one(0, zt, 1 - n.at[1]).start()
        self.one(1, zt, 1 - n.at[2]).start()
        self.p_take(Tb, zt, order[1])
        self.one(0, zt, n.at[1]).start()
        self.p_take(Tb, zt, order[2])
        self.one(1, zt, n.at[2]).start()
        self.p_take(Tb, zt, order[3])

    def stage1(self, zt):
        n = self.net
        for part in (0, 1):
            for piece in (0, 1):
                own = n.at[self.second[piece]]
                idx = 1 - own if part == 0 else own
                at = [zt, n.at[1], n.at[2]]
                at[self.second[piece]] = idx
                self.one(piece, zt, idx).wait_recv()
                add_rows(self.acc.at[n.chip(at), self.half(piece)], [self.buf1.at[zt, idx, self.half(piece)]], self.T // 2)
                if part == 0:
                    self.two(piece, zt).start()

    def stage2(self, zt):
        n = self.net
        z = n.at[0]
        feeds = jnp.where(zt > z, z > 0, z < 3)
        for piece in (0, 1):
            self.two(piece, zt).wait_recv()
            add_rows(self.acc.at[n.chip((zt, n.at[1], n.at[2])), self.half(piece)], [self.buf2.at[zt, self.half(piece)]], self.T // 2)
            pl.when(jnp.logical_and(zt != z, jnp.logical_not(feeds)))(lambda piece=piece: self.three(piece, zt).start())

    def relay(self, zt):
        n = self.net
        z = n.at[0]
        d = jnp.where(zt > z, 0, 1)
        feeds = jnp.where(zt > z, z > 0, z < 3)

        def go():
            for piece in (0, 1):
                self.three(piece, zt).wait_recv()
                add_rows(self.acc.at[n.chip((zt, n.at[1], n.at[2])), self.half(piece)],
                         [self.zbuf.at[d, zt, self.half(piece)]], self.T // 2)
                self.three(piece, zt).start()

        pl.when(jnp.logical_and(zt != z, feeds))(go)

    def arrive(self, piece, d):
        n = self.net
        z = n.at[0]
        dst = self.zbuf.at[d, z, self.half(piece)]
        rcopy(dst, dst, self.s3.at[piece, d, z], self.r3.at[piece, d, z], (n.e, n.c)).wait_recv()
        add_rows(self.acc.at[n.e, self.half(piece)], [dst], self.T // 2)

    def last(self, out):
        z = self.net.at[0]
        for piece in (0, 1):
            pl.when(z > 0)(lambda piece=piece: self.arrive(piece, 0))
            pl.when(z < 3)(lambda piece=piece: self.arrive(piece, 1))
        out[...] = self.acc[self.net.e]

    def drain(self, zt):
        n = self.net
        for piece in (0, 1):
            for idx in (0, 1):
                self.one(piece, zt, idx).wait_send()
            self.two(piece, zt).wait_send()
            pl.when(zt != n.at[0])(lambda piece=piece: self.three(piece, zt).wait_send())


NT = (((1,), (1,)), ((), ()))
TN = (((0,), (0,)), ((), ()))


def experts_fused(x, marked, G, w_gate, w_up, w_down, cap, cid):
    T, D = x.shape
    E = marked.shape[0]
    X2, _, Fh = w_gate.shape
    chips = G.shape[0]
    nd = 2 * chips
    S2 = 2 * cap
    M = 4 * S2
    CW = 512
    PR = 64
    SW = 1024

    def kernel(x_ref, a_ref, g_ref, wg_ref, wu_ref, wd_ref, o_sum, o_part, o_dots, o_rows, o_grows, o_act, o_ggu, N,
               A, wgu, wdn, Nst, Gst, H, pk, pkt, sw, rowsb, growsb, h1, h2, actw, ggu, yb, To, Tb, dsend,
               acc, b1, b2, zb, r0, s0, r1, s1, r2, s2, r3, s3, ar, asd, xr, xs, dr, ds_, lsem):
        net = Net(chips).enter()
        z, c, e = net.at[0], net.c, net.e
        me = e * 2 + c
        copies = [(wg_ref.at[i], wgu.at[i, :, pl.ds(0, Fh)]) for i in range(2)]
        copies += [(wu_ref.at[i], wgu.at[i, :, pl.ds(Fh, Fh)]) for i in range(2)]
        copies += [(wd_ref, wdn)]
        loads = [lambda s=s, d=d, i=i: pltpu.make_async_copy(s, d, lsem.at[i]) for i, (s, d) in enumerate(copies)]
        own = lambda: pltpu.make_async_copy(x_ref, N.at[e, pl.ds(pl.multiple_of(c * T, T), T)], lsem.at[6])
        own().start()
        acopy = lambda: pltpu.make_async_copy(a_ref, A.at[me], lsem.at[7])
        acopy().start()
        greet_all(net)
        own().wait()
        acopy().wait()
        ag = Gather22(net, N, T, xr, xs)
        rs = Reduce22(net, T, acc, b1, b2, zb, (r0, s0, r1, s1, r2, s2, r3, s3))
        done = []
        ag.begin()
        interleave(to_all(net, lambda t: a_ref, lambda s: A.at[s], lambda s: ar.at[s], lambda k: asd.at[k], done))
        for f in loads:
            f().start()
        lane = lax.broadcasted_iota(jnp.int32, (256, 256), 1)
        sub = lax.broadcasted_iota(jnp.int32, (256, 256), 0)
        U = jnp.where(jnp.logical_and(sub < lane, sub // 128 == lane // 128), 1.0, 0.0).astype(BF)
        eye = jnp.where(sub == lane, 1.0, 0.0).astype(BF)
        place = ((lax.broadcasted_iota(jnp.int32, (8, 256), 1) // 128) * cap).astype(F32)
        ag.from_z(slot_plane(z, 1))
        ag.from_two(z)
        for f in done:
            f()
        for f in loads:
            f().wait()

        saves = lambda i: [
            (rowsb, o_rows.at[:, i], 8), (growsb, o_grows.at[:, i], 9), (actw, o_act.at[:, i], 10), (ggu, o_ggu.at[:, i], 11)]

        def body(i, _):
            zt = slot_plane(z, i)
            zn = slot_plane(z, i + 1)
            zp = slot_plane(z, i - 1)
            pltpu.make_async_copy(g_ref.at[pl.ds(zt * 4, 4)], Gst, lsem.at[13]).start()
            ag.from_three(zt)
            ag.from_partner(zt)
            cpn = pltpu.make_async_copy(N.at[pl.ds(zt * 4, 4)], Nst, lsem.at[12])
            cpn.start()
            for ch in range(4):
                for ei in range(2):
                    for co in range(2):
                        H[2 * ch + ei:2 * ch + ei + 1, co * 128:(co + 1) * 128] = A[(zt * 4 + ch) * 2 + co, pl.ds(2 * e + ei, 1), :]
            h = H[...]
            here = jnp.where(h >= 0.0, 1.0, 0.0)
            slot = jnp.dot(here.astype(BF), U, preferred_element_type=F32) + place
            slot = jnp.where(here > 0.0, slot, -1.0)
            row_id = lax.broadcasted_iota(jnp.int32, (S2, 256), 0).astype(F32)
            for ch in range(4):
                for ei in range(2):
                    q = 2 * ch + ei
                    hit = row_id == slot[q:q + 1, :]
                    pk[ch, ei * S2:(ei + 1) * S2, :] = jnp.where(hit, 1.0, 0.0).astype(BF)
                    wcol = jnp.sum(jnp.where(hit, h[q:q + 1, :], 0.0), axis=1, keepdims=True)
                    sw[ei, ch * S2:(ch + 1) * S2, :] = jnp.broadcast_to(wcol, (S2, 128))
                pkt[ch] = lax.dot_general(eye, pk[ch], NT, preferred_element_type=F32).astype(BF)

            def before():
                for src, dst, s in saves(i):
                    pltpu.make_async_copy(src, dst, lsem.at[s]).wait()

            pl.when(i > 0)(before)
            cpn.wait()
            pltpu.make_async_copy(g_ref.at[pl.ds(zt * 4, 4)], Gst, lsem.at[13]).wait()

            def picks(k, _):
                ch, j = k // 2, k % 2
                cols = pl.ds(pl.multiple_of(j * (D // 2), D // 2), D // 2)
                at = pl.ds(pl.multiple_of(ch * S2, S2), S2)
                for st, dst in ((Nst, rowsb), (Gst, growsb)):
                    r = jnp.dot(pk[ch], st[ch, :, cols], preferred_element_type=F32).astype(BF)
                    dst[0, at, cols] = r[:S2]
                    dst[1, at, cols] = r[S2:]
                return 0

            lax.fori_loop(0, 8, picks, 0)
            pltpu.make_async_copy(rowsb, o_rows.at[:, i], lsem.at[8]).start()
            pltpu.make_async_copy(growsb, o_grows.at[:, i], lsem.at[9]).start()
            pl.when(i < 2)(lambda: ag.from_z(slot_plane(z, i + 2)))
            pl.when(i > 0)(lambda: rs.stage1(zp))

            for ei in range(2):
                h1[...] = jnp.dot(rowsb[ei], wgu[ei], preferred_element_type=F32)
                h2[...] = lax.dot_general(growsb[ei], wdn[ei], NT, preferred_element_type=F32)

                def point(k, _):
                    r = pl.ds(pl.multiple_of(k * PR, PR), PR)
                    gate, up, ga = h1[r, :Fh], h1[r, Fh:], h2[r, :]
                    w = sw[ei, r, 0:1]
                    sig = 1.0 / (1.0 + jnp.exp(-gate))
                    silu = gate * sig
                    act = silu * up
                    actw[ei, r, :] = (w * act).astype(BF)
                    sw[ei, r, :] = jnp.broadcast_to(jnp.sum(act * ga, axis=1, keepdims=True), (PR, 128))
                    gact = w * ga
                    ggu[ei, r, :Fh] = (gact * up * (sig + silu * (1.0 - sig))).astype(BF)
                    ggu[ei, r, Fh:] = (gact * silu).astype(BF)
                    return 0

                lax.fori_loop(0, M // PR, point, 0)
                for ch in range(4):
                    dcol = sw[ei, ch * S2:(ch + 1) * S2, 0:1]
                    dd = jnp.sum(pk[ch, ei * S2:(ei + 1) * S2, :].astype(F32) * dcol, axis=0, keepdims=True)
                    for co in range(2):
                        dsend[(zt * 4 + ch) * 2 + co, ei:ei + 1, :] = dd[:, co * 128:(co + 1) * 128]
                if ei == 0:
                    pl.when(i < 3)(lambda: ag.from_two(zn))
            pltpu.make_async_copy(actw, o_act.at[:, i], lsem.at[10]).start()
            pltpu.make_async_copy(ggu, o_ggu.at[:, i], lsem.at[11]).start()
            pl.when(i > 0)(lambda: rs.stage2(zp))

            def back(j, _):
                rws = pl.ds(pl.multiple_of(j * CW, CW), CW)
                for ei in range(2):
                    r = lax.dot_general(ggu[ei], wgu[ei, rws, :], NT, preferred_element_type=F32).astype(BF)
                    for ch in range(4):
                        yb[ch, ei * S2:(ei + 1) * S2, rws] = r[ch * S2:(ch + 1) * S2]
                return 0

            lax.fori_loop(0, D // CW, back, 0)
            for ab in rs.ring():
                ch = ab[0] * 2 + ab[1]

                def spread_back(j, _, ch=ch):
                    cols = pl.ds(pl.multiple_of(j * SW, SW), SW)
                    Tb[ch, :, cols] = jnp.dot(pkt[ch], yb[ch, :, cols], preferred_element_type=F32).astype(BF)
                    return 0

                lax.fori_loop(0, D // SW, spread_back, 0)
                rs.p_copy(Tb, zt, ab).start()

            def down(j, _):
                cols = pl.ds(pl.multiple_of(j * CW, CW), CW)
                for ei in range(2):
                    r = jnp.dot(actw[ei], wdn[ei, :, cols], preferred_element_type=F32).astype(BF)
                    for ch in range(4):
                        yb[ch, ei * S2:(ei + 1) * S2, cols] = r[ch * S2:(ch + 1) * S2]
                return 0

            lax.fori_loop(0, D // CW, down, 0)
            rs.stage0(Tb, zt)
            rs.p_wait_send(Tb, zt)
            for ch in range(4):
                cp = lambda ch=ch: pltpu.make_async_copy(To.at[ch % 2], o_part.at[zt * 4 + ch], lsem.at[14 + ch % 2])
                if ch >= 2:
                    cp().wait()

                def spread(j, _, ch=ch):
                    cols = pl.ds(pl.multiple_of(j * SW, SW), SW)
                    To[ch % 2, :, cols] = jnp.dot(pkt[ch], yb[ch, :, cols], preferred_element_type=F32).astype(BF)
                    return 0

                lax.fori_loop(0, D // SW, spread, 0)
                cp().start()
            for ch in (2, 3):
                pltpu.make_async_copy(To.at[ch % 2], o_part.at[zt * 4 + ch], lsem.at[14 + ch % 2]).wait()
            return 0

        lax.fori_loop(0, 4, body, 0)
        z3 = slot_plane(z, 3)
        last_done = []
        own_dots = pltpu.make_async_copy(dsend.at[me], o_dots.at[me], lsem.at[5])
        own_dots.start()
        interleave(to_all(net, lambda t: dsend.at[t], lambda s: o_dots.at[s], lambda s: dr.at[s], lambda k: ds_.at[k], last_done))
        rs.stage1(z3)
        rs.relay(slot_plane(z, 2))
        rs.stage2(z3)
        rs.relay(z3)
        rs.relay(slot_plane(z, 1))
        rs.last(o_sum)
        own_dots.wait()
        for f in last_done:
            f()
        for src, dst, s in saves(3):
            pltpu.make_async_copy(src, dst, lsem.at[s]).wait()

        def finish(i, _):
            ag.drain(i)
            rs.drain(slot_plane(z, i))
            return 0

        lax.fori_loop(0, 4, finish, 0)

    S = jax.ShapeDtypeStruct
    V = pltpu.VMEM
    return pl.pallas_call(
        kernel,
        out_shape=(S((T, D), BF), S((chips, 2 * T, D), BF), S((nd, 8, 128), F32), S((2, 4, M, D), BF), S((2, 4, M, D), BF),
                   S((2, 4, M, Fh), BF), S((2, 4, M, 2 * Fh), BF), S((chips, 2 * T, D), BF)),
        in_specs=[VM, VM, ANY, ANY, ANY, ANY], out_specs=(VM, ANY, VM, ANY, ANY, ANY, ANY, ANY),
        scratch_shapes=[
            V((nd, E, T), F32), V((2, D, 2 * Fh), BF), V((2, Fh, D), BF), V((4, 2 * T, D), BF), V((4, 2 * T, D), BF),
            V((8, 2 * T), F32), V((4, 2 * S2, 2 * T), BF), V((4, 2 * T, 2 * S2), BF), V((2, M, 128), F32), V((2, M, D), BF), V((2, M, D), BF),
            V((M, 2 * Fh), F32), V((M, Fh), F32), V((2, M, Fh), BF), V((2, M, 2 * Fh), BF), V((4, 2 * S2, D), BF),
            V((2, 2 * T, D), BF), V((4, 2 * T, D), BF), V((nd, 8, 128), F32)]
        + Reduce22.scratch(T, D)
        + [DMA((nd,)), DMA((nd,)), DMA((2, chips, 2)), DMA((2, chips, 5)), DMA((nd,)), DMA((nd,)), DMA((16,))],
        compiler_params=params(cid, 64 << 20), name="experts",
    )(x, marked, G, w_gate, w_up, w_down)[:7]


def column_sum_gather(n_expert, part, x, cid):
    _, _, T, D = part.shape

    def kernel(p_ref, x_ref, o_ref, N, acc, buf, fin, rsem, ssem, xr, xs, lsem):
        net = Net(n_expert).enter()
        z, e, c = net.at[0], net.e, net.c
        own = lambda: pltpu.make_async_copy(x_ref, N.at[e, pl.ds(pl.multiple_of(c * T, T), T)], lsem)
        own().start()
        greet(net, (0, 1, 2))
        own().wait()
        ag = Gather22(net, N, T, xr, xs)
        done = []

        def gather():
            ag.begin()
            yield
            for i in range(4):
                if i < 3:
                    ag.from_z(slot_plane(z, i + 1))
                    yield
                ag.from_two(slot_plane(z, i))
                yield
                if i:
                    ag.from_three(slot_plane(z, i - 1))
                    yield
            ag.from_three(slot_plane(z, 3))
            for i in range(4):
                ag.from_partner(slot_plane(z, i))

        interleave(
            col_rs(net, lambda s, h: p_ref.at[s, h], o_ref, lambda w, s, h: acc.at[w, s, h], lambda w, s, h: buf.at[w, s, h],
                   lambda i: fin.at[i], lambda w, s, h: rsem.at[w, s, h], lambda w, s, h: ssem.at[w, s, h], T, done),
            gather())
        for f in done:
            f()

        def finish(i, _):
            ag.drain(i)
            return 0

        lax.fori_loop(0, 4, finish, 0)

    S = jax.ShapeDtypeStruct
    V = pltpu.VMEM
    return pl.pallas_call(
        kernel, out_shape=(S((T, D), BF), S((n_expert, 2 * T, D), BF)), in_specs=[VM, VM], out_specs=(VM, ANY),
        scratch_shapes=[V((2, 2, 2, T, D), BF), V((2, 2, 2, T, D), BF), V((2, T, D), BF),
                        DMA((3, 2, 2)), DMA((3, 2, 2)), DMA((2, n_expert, 2)), DMA((2, n_expert, 5)), DMA],
        compiler_params=params(cid, 40 << 20), name="column_sum_gather",
    )(part, x)


def reduce_and_column(n_expert, part, x, cid):
    T, D = x.shape

    def kernel(p_ref, x_ref, o_ref, X, Tb, acc, b1, b2, zb, r0, s0, r1, s1, r2, s2, r3, s3, xr, xs, lsem):
        net = Net(n_expert).enter()
        z = net.at[0]
        load = lambda i: pltpu.make_async_copy(p_ref.at[pl.ds(slot_plane(z, 3 - i) * 4, 4)], Tb.at[i % 2], lsem.at[i % 2])
        load(0).start()
        greet(net, (0, 1, 2))
        rs = Reduce22(net, T, acc, b1, b2, zb, (r0, s0, r1, s1, r2, s2, r3, s3))
        done = []
        far = lambda i: slot_plane(z, 3 - i)

        def reduce():
            for i in range(4):
                if i:
                    rs.p_wait_send(Tb.at[(i - 1) % 2], far(i - 1))
                if i < 3:
                    load(i + 1).start()
                load(i).wait()
                rs.p_send(Tb.at[i % 2], far(i))
                yield
                rs.stage0(Tb.at[i % 2], far(i))
                yield
                if i:
                    rs.stage1(far(i - 1))
                    yield
                if i > 1:
                    rs.stage2(far(i - 2))
                    yield
            rs.p_wait_send(Tb.at[1], far(3))
            rs.stage1(far(3))
            rs.stage2(far(2))
            yield
            for i in (0, 1, 2):
                rs.relay(far(i))
            rs.stage2(far(3))
            rs.last(o_ref)

        interleave(
            reduce(),
            col_ag(net, x_ref, lambda s, h: X.at[s, h], lambda s, h: xr.at[s, h], lambda w, s, h: xs.at[w, s, h], done))
        for f in done:
            f()

        def finish(i, _):
            rs.drain(slot_plane(z, i))
            return 0

        lax.fori_loop(0, 4, finish, 0)

    S = jax.ShapeDtypeStruct
    return pl.pallas_call(
        kernel, out_shape=(S((T, D), BF), S((2, 2, T, D), BF)), in_specs=[ANY, VM], out_specs=(VM, ANY),
        scratch_shapes=[pltpu.VMEM((2, 4, 2 * T, D), BF)] + Reduce22.scratch(T, D) + [DMA((2, 2)), DMA((3, 2, 2)), DMA((2,))],
        compiler_params=params(cid, 60 << 20), name="reduce_and_column",
    )(part, x)


MODEL_WIDTH = 2048
QUERY_HEADS = 32
KEY_VALUE_HEADS = 4
HEAD_SIZE = 128
GROUP = QUERY_HEADS // KEY_VALUE_HEADS
TOP = 8
EXP_DEV = 2

epsilon = 1e-06
rope_base = 1000000.0


def norm_parts(values_in, gain_vec):
    inverse = lax.rsqrt(jnp.mean(values_in * values_in, axis=-1, keepdims=True) + epsilon)
    return (values_in * inverse * gain_vec, inverse)


def norm_back(values_in, inverse, gain_vec, grad_out):
    scaled = grad_out * gain_vec
    grad_in = inverse * (
        scaled
        - values_in * inverse * inverse * jnp.mean(scaled * values_in, axis=-1, keepdims=True)
    )
    return (grad_in, grad_out * values_in * inverse)


def rope_tables(positions):
    exponent = jnp.arange(HEAD_SIZE // 2).astype(F32) * (2.0 / HEAD_SIZE)
    frequency = jnp.exp(-math.log(rope_base) * exponent)
    angles = positions.astype(F32)[:, None] * frequency[None, :]
    return (jnp.cos(angles), jnp.sin(angles))


def rotate(v, cos, sin):
    half = v.shape[-1] // 2
    a, b = v[..., :half], v[..., half:]
    return jnp.concatenate([a * cos - b * sin, b * cos + a * sin], axis=-1)


def rotate_back(v, cos, sin):
    half = v.shape[-1] // 2
    a, b = v[..., :half], v[..., half:]
    return jnp.concatenate([a * cos + b * sin, b * cos - a * sin], axis=-1)


def mm(a, b):
    return jnp.dot(a, b, preferred_element_type=F32)


def ein(spec, *args):
    return jnp.einsum(spec, *args, preferred_element_type=F32)


def experts_wide(n_expert, second_in, marked, G, w_gate, w_up, w_down, capacity):
    T, D = second_in.shape
    nd = 2 * n_expert
    e = lax.axis_index("expert")
    N, M = gather_all(n_expert, second_in, marked, 2)

    mine = lax.dynamic_slice(M, (0, EXP_DEV * e, 0), (nd, EXP_DEV, T))
    here = mine >= 0.0
    rank = jnp.cumsum(here.astype(jnp.int32), axis=-1) - 1
    slots = jnp.arange(capacity, dtype=jnp.int32)
    pick = here[:, :, None, :] & (rank[:, :, None, :] == slots[None, None, :, None])
    slot_weight = jnp.sum(jnp.where(pick, mine[:, :, None, :], 0.0), axis=-1).transpose(1, 0, 2)[..., None]
    pick = pick.astype(BF)
    N = N.reshape(nd, T, D)
    G = G.reshape(nd, T, D)
    rows = ein("sect,std->escd", pick, N).astype(BF)
    g_rows = ein("sect,std->escd", pick, G)
    flat = lambda v: v.reshape(EXP_DEV, nd * capacity, v.shape[-1])
    deep = lambda v: v.reshape(EXP_DEV, nd, capacity, v.shape[-1])
    rows = flat(rows)
    grad_rows = flat((slot_weight * g_rows).astype(BF))
    gate_value = ein("emd,edf->emf", rows, w_gate)
    up_value = ein("emd,edf->emf", rows, w_up)
    sig = jax.nn.sigmoid(gate_value)
    act = (gate_value * sig * up_value).astype(BF)
    expert_part = deep(ein("emf,efd->emd", act, w_down))
    dots = jnp.sum(g_rows * expert_part, axis=-1)
    out_part = ein("sect,escd->std", pick, (slot_weight * expert_part).astype(BF)).astype(BF)
    dots = ein("sect,esc->set", pick.astype(F32), dots)
    grad_act = ein("emd,efd->emf", grad_rows, w_down)
    grad_gate_v = (grad_act * up_value * sig * (1.0 + gate_value * (1.0 - sig))).astype(BF)
    grad_up_v = (grad_act * gate_value * sig).astype(BF)
    down_grad = ein("emf,emd->efd", act, grad_rows)
    gate_grad = ein("emd,emf->edf", rows, grad_gate_v)
    up_grad = ein("emd,emf->edf", rows, grad_up_v)
    back_rows = ein("emf,edf->emd", grad_gate_v, w_gate) + ein("emf,edf->emd", grad_up_v, w_up)
    back_part = ein("sect,escd->std", pick, deep(back_rows.astype(BF))).astype(BF)

    dots_out = jnp.pad(dots, ((0, 0), (0, 8 - EXP_DEV), (0, 0)))
    dots_in = exchange(n_expert, dots_out, 3)
    parts = max(1, n_expert // 16)

    def summed(v, cid):
        v = v.reshape(n_expert, 2, T, D)
        W_ = D // parts
        return jnp.concatenate(
            [reduce_scatter_all(n_expert, v[..., i * W_:(i + 1) * W_], cid + 2 * i) for i in range(parts)], axis=1).astype(F32)

    back_sum = summed(back_part, 8)
    out_sum = summed(out_part, 9)

    return back_sum, out_sum, dots_in, gate_grad, up_grad, down_grad


def local(
    n_expert, tokens, routes, documents, w_query, key_projection, value_projection, w_out, w_router,
    gain_attn, gain_ffn, gain_query, gain_key, w_gate, w_up, w_down, cotangent,
):
    Z = KEY_VALUE_HEADS
    plane = n_expert // Z
    nd = 2 * n_expert
    T, D = tokens.shape
    R, HR, E = w_query.shape[0], w_out.shape[0], w_router.shape[1]
    Q = gain_query.shape[0]
    KV = HEAD_SIZE
    GQ = GROUP * HEAD_SIZE
    e, c = lax.axis_index("expert"), lax.axis_index("context")
    z, p = e // plane, e % plane
    capacity = T * TOP * 5 // (4 * E)
    score_scale = HEAD_SIZE ** (-0.5)

    wqkv = jnp.concatenate(
        [w_query.reshape(R, Z, GQ), key_projection.reshape(R, Z, KV), value_projection.reshape(R, Z, KV)], axis=-1
    ).transpose(1, 0, 2)
    width = -(-(E + 4) // 128) * 128
    pad = lambda v: jnp.pad(v, (0, R - v.shape[0]))[:, None]
    head = jnp.concatenate(
        [w_router, gain_attn[:, None], gain_ffn[:, None], pad(gain_query), pad(gain_key), jnp.zeros((R, width - E - 4), BF)], axis=1
    )
    docs_own = lax.dynamic_slice_in_dim(documents[0], c * T, T).astype(BF)[None]
    docs_own = jnp.pad(docs_own, ((0, 15), (0, width - T)))
    aux = jnp.concatenate([head, docs_own], axis=0)
    small_plane = plane == 4
    X, W, O, A, *G = gather_start(n_expert, tokens, wqkv, w_out, aux, None if small_plane else cotangent, 0)
    W = W.reshape(D, GQ + 2 * KV)
    O = O.reshape(GQ, D)
    table = A[:, :R].reshape(D, width)
    router_weight = table[:, :E]
    attn_gain = table[:, E].astype(F32)
    ffn_gain = table[:, E + 1].astype(F32)
    query_gain = A[:, :Q, E + 2].reshape(HEAD_SIZE).astype(F32)
    key_gain = A[:, :Q, E + 3].reshape(HEAD_SIZE).astype(F32)
    docs = A[:, R, :T].reshape(Z, plane, 2 * T)
    docs = lax.dynamic_slice(docs, (2 * c, p, 0), (2, 1, 2 * T)).reshape(2, 2 * T)

    L = 2 * T
    x = X.reshape(2 * L, D).astype(F32)
    normed, inverse_attn = norm_parts(x, attn_gain)
    first_in = normed.astype(BF)
    raw = mm(first_in, W)
    query_raw = raw[:, :GQ].reshape(2, L, GROUP, HEAD_SIZE)
    key_raw = raw[:, GQ:GQ + KV].reshape(2, L, HEAD_SIZE)
    value = raw[:, GQ + KV:].reshape(2, L, HEAD_SIZE).astype(BF)
    cos, sin = rope_tables(jnp.arange(L, dtype=jnp.int32))
    qcos, qsin = cos[:, None, :], sin[:, None, :]
    query_normed, query_inverse = norm_parts(query_raw, query_gain)
    queries = rotate(query_normed, qcos, qsin).astype(BF)
    key_normed, key_inverse = norm_parts(key_raw, key_gain)
    keys = rotate(key_normed, cos, sin).astype(BF)
    places = jnp.arange(L, dtype=jnp.int32)
    allowed = (places[:, None] >= places[None, :])[None] & (docs[:, :, None] == docs[:, None, :])
    scores = ein("sqhd,skd->shqk", queries, keys) * score_scale
    scores = jnp.where(allowed[:, None], scores, -1e30)
    top = jnp.max(scores, axis=-1, keepdims=True)
    ex = jnp.exp(scores - top)
    probs = ex / jnp.sum(ex, axis=-1, keepdims=True)
    probs_low = probs.astype(BF)
    attended = ein("shqk,skd->sqhd", probs_low, value).reshape(2 * L, GQ).astype(BF)
    part = mm(attended, O).astype(BF).reshape(2, 2, T, D)
    if small_plane:
        attn_sum, G = column_sum_gather(n_expert, part, cotangent, 1)
    else:
        attn_sum, G = column_sum(n_expert, part, 1), G[0]
    middle = tokens.astype(F32) + attn_sum.astype(F32)

    normed_ffn, inverse_ffn = norm_parts(middle, ffn_gain)
    second_in = normed_ffn.astype(BF)
    logits = mm(second_in, router_weight)
    ids = jnp.arange(E, dtype=jnp.int32)
    chosen = jnp.any(routes[:, :, None] == ids[None, None, :], axis=1)
    masked = jnp.where(chosen, logits, -jnp.inf)
    best = jnp.max(masked, axis=-1, keepdims=True)
    ew = jnp.where(chosen, jnp.exp(logits - best), 0.0)
    weights = ew / jnp.sum(ew, axis=-1, keepdims=True)
    marked = jnp.where(chosen, weights, -1.0).T
    if small_plane:
        back_sum, out_part, dots_in, rows, g_rows, act_w, gate_up = experts_fused(
            second_in, marked, G, w_gate, w_up, w_down, capacity, 3)
        flat = lambda v: v.reshape(EXP_DEV, -1, v.shape[-1])
        Fh = act_w.shape[-1]
        rows = flat(rows)
        down_grad = ein("emf,emd->efd", flat(act_w), flat(g_rows))
        gate_grad = ein("emd,emf->edf", rows, flat(gate_up[..., :Fh]))
        up_grad = ein("emd,emf->edf", rows, flat(gate_up[..., Fh:]))
    else:
        back_sum, out_sum, dots_in, gate_grad, up_grad, down_grad = experts_wide(
            n_expert, second_in, marked, G, w_gate, w_up, w_down, capacity)
    back_sum = back_sum.astype(F32)

    grad_result = cotangent.astype(F32)
    grad_weights = jnp.sum(dots_in[:, :EXP_DEV].reshape(n_expert, 2, EXP_DEV, T), axis=1).reshape(E, T).T
    grad_chosen = weights * (grad_weights - jnp.sum(weights * grad_weights, axis=-1, keepdims=True))
    grad_logits = jnp.where(chosen, grad_chosen, 0.0).astype(BF)
    router_grad = mm(second_in.T, grad_logits)
    grad_second = mm(grad_logits, router_weight.T) + back_sum
    grad_middle_norm, ffn_terms = norm_back(middle, inverse_ffn, ffn_gain, grad_second)
    ffn_gain_grad = jnp.sum(ffn_terms, axis=0)
    grad_middle = grad_result + grad_middle_norm

    if small_plane:
        out_sum, GA = reduce_and_column(n_expert, out_part, grad_middle.astype(BF), 6)
    else:
        GA = column_gather(n_expert, grad_middle.astype(BF), 6)
    block_out = (middle + out_sum.astype(F32)).astype(BF)
    GA = GA.reshape(2 * L, D)
    out_grad = mm(attended.T, GA)
    grad_attended = ein("td,fd->tf", GA, O).astype(BF).reshape(2, L, GROUP, HEAD_SIZE)
    grad_probs = ein("sqhd,skd->shqk", grad_attended, value)
    grad_scores = (probs * (grad_probs - jnp.sum(probs * grad_probs, axis=-1, keepdims=True))).astype(BF)
    grad_queries = ein("shqk,skd->sqhd", grad_scores, keys) * score_scale
    grad_keys = ein("shqk,sqhd->skd", grad_scores, queries) * score_scale
    grad_values = ein("shqk,sqhd->skd", probs_low, grad_attended)
    grad_query_raw, query_terms = norm_back(query_raw, query_inverse, query_gain, rotate_back(grad_queries, qcos, qsin))
    grad_key_raw, key_terms = norm_back(key_raw, key_inverse, key_gain, rotate_back(grad_keys, cos, sin))
    grad_raw = jnp.concatenate(
        [grad_query_raw.reshape(2 * L, GQ).astype(BF), grad_key_raw.reshape(2 * L, KV).astype(BF),
         grad_values.reshape(2 * L, KV).astype(BF)], axis=-1)
    query_gain_grad = jnp.sum(query_terms, axis=(0, 1, 2))
    key_gain_grad = jnp.sum(key_terms, axis=(0, 1))
    grad_first = ein("tf,df->td", grad_raw, W)
    raw_grad = mm(first_in.T, grad_raw)
    attn_gain_grad = jnp.sum(grad_first * x * inverse_attn, axis=0)

    small = jnp.concatenate([
        router_grad.reshape(nd, R * E), attn_gain_grad.reshape(nd, R), ffn_gain_grad.reshape(nd, R),
        query_gain_grad.reshape(nd, Q), key_gain_grad.reshape(nd, Q)], axis=1)
    n_small = small.shape[1]
    small = jnp.pad(small, ((0, 0), (0, -n_small % 1024))).reshape(nd, -1, 128)
    grad_first_sum, raw_sum, out_sum2, small_in = reduce_end(
        n_expert, grad_first.astype(BF).reshape(2, 2, T, D), raw_grad.astype(BF).reshape(Z, plane, 2, R, GQ + 2 * KV),
        out_grad.astype(BF).reshape(plane, 2, HR, D), small, 7)
    small_sum = jnp.sum(small_in, axis=0).reshape(-1)
    router_grad = small_sum[:R * E].reshape(R, E)
    attn_gain_grad = small_sum[R * E:R * E + R]
    ffn_gain_grad = small_sum[R * E + R:R * E + 2 * R]
    query_gain_grad = small_sum[R * E + 2 * R:R * E + 2 * R + Q]
    key_gain_grad = small_sum[R * E + 2 * R + Q:n_small]
    raw_sum = raw_sum.astype(F32)
    query_grad = raw_sum[:, :, :GQ].transpose(1, 0, 2).reshape(R, QUERY_HEADS * HEAD_SIZE)
    key_grad = raw_sum[:, :, GQ:GQ + KV].transpose(1, 0, 2).reshape(R, Z * KV)
    value_grad = raw_sum[:, :, GQ + KV:].transpose(1, 0, 2).reshape(R, Z * KV)

    own = tokens.astype(F32)
    inverse_own = lax.rsqrt(jnp.mean(own * own, axis=-1, keepdims=True) + epsilon)
    grad_in, _ = norm_back(own, inverse_own, attn_gain, grad_first_sum.astype(F32))
    grad_tokens = grad_middle + grad_in
    return (
        block_out, grad_tokens, query_grad, key_grad, value_grad, out_sum2.astype(F32), router_grad,
        attn_gain_grad, ffn_gain_grad, query_gain_grad, key_gain_grad, gate_grad, up_grad, down_grad,
    )


def solution(mesh):
    row = P(("expert", "context"), None)
    vec = P(("expert", "context"))
    hidden = P("expert", None, "context")
    return jax.shard_map(
        functools.partial(local, mesh.shape["expert"]),
        mesh=mesh,
        in_specs=(row, row, P("expert", None), row, row, row, row, row, vec, vec, vec, vec, hidden, hidden,
                  P("expert", "context", None), row),
        out_specs=(row, row, row, row, row, row, row, vec, vec, vec, vec, hidden, hidden, P("expert", "context", None)),
        check_vma=False,
    )
```

```python
import functools
import math

import jax
import jax.numpy as jnp
from jax import lax
from jax.experimental import pallas as pl
from jax.experimental.pallas import tpu as pltpu
from jax.sharding import PartitionSpec as P

MESH_ID = pl.DeviceIdType.MESH
BF = jnp.bfloat16
F32 = jnp.float32


class Net:
    def __init__(self, n_expert):
        side = math.isqrt(n_expert // 4)
        self.dims = (4, side, side)
        self.chips = n_expert

    def enter(self):
        e = lax.axis_index("expert")
        _, A, B = self.dims
        self.e = e
        self.at = (e // (A * B), (e // B) % A, e % B)
        self.c = lax.axis_index("context")
        return self

    def chip(self, at):
        _, A, B = self.dims
        return (at[0] * A + at[1]) * B + at[2]

    def moved(self, axis, to):
        at = list(self.at)
        at[axis] = to
        return tuple(at)

    def near(self, axis):
        n, p = self.dims[axis], self.at[axis]
        if n == 2:
            return [(None, 1 - p)]
        return [(p < n - 1, p + 1), (p > 0, p - 1)]


def when(cond, fn):
    if cond is None:
        fn()
    else:
        pl.when(cond)(fn)


def rcopy(src, dst, ss, rs, dev):
    return pltpu.make_async_remote_copy(
        src_ref=src, dst_ref=dst, send_sem=ss, recv_sem=rs, device_id=dev, device_id_type=MESH_ID
    )


def greet(net, axes, partner=True):
    bar = pltpu.get_barrier_semaphore()
    count = 0
    for axis in axes:
        for cond, to in net.near(axis):
            dev = (net.chip(net.moved(axis, to)), net.c)
            when(cond, lambda dev=dev: pl.semaphore_signal(bar, inc=1, device_id=dev, device_id_type=MESH_ID))
            count = count + (1 if cond is None else jnp.where(cond, 1, 0))
    if partner:
        pl.semaphore_signal(bar, inc=1, device_id=(net.e, 1 - net.c), device_id_type=MESH_ID)
        count = count + 1
    pl.semaphore_wait(bar, count)


def greet_all(net):
    bar = pltpu.get_barrier_semaphore()
    total = net.chips * 2
    me = net.e * 2 + net.c

    def body(k, _):
        t = (me + k) % total
        pl.semaphore_signal(bar, inc=1, device_id=(t // 2, t % 2), device_id_type=MESH_ID)
        return 0

    lax.fori_loop(1, total, body, 0)
    pl.semaphore_wait(bar, total - 1)


def interleave(*gens):
    gens = list(gens)
    while gens:
        for g in list(gens):
            try:
                next(g)
            except StopIteration:
                gens.remove(g)


def ag_piece(net, order, block, rs, ss, done, partner=True):
    def send(cond, at, kind, dev):
        ch = net.chip(at)
        mk = lambda: rcopy(block(ch, net.c), block(ch, net.c), ss(ch, kind), rs(ch, net.c), dev)
        when(cond, lambda: mk().start())
        return lambda: when(cond, lambda: mk().wait_send())

    def spread(at, stage):
        outs = []
        for i in range(stage, len(order)):
            axis = order[i]
            for k, (cond, to) in enumerate(net.near(axis)):
                outs.append(send(cond, at, 2 * i + k, (net.chip(net.moved(axis, to)), net.c)))
        if partner:
            outs.append(send(None, at, 6, (net.e, 1 - net.c)))
        return outs

    done.extend(spread(net.at, 0))
    yield
    known = [(None, net.at)]

    for i, axis in enumerate(order):
        n, p = net.dims[axis], net.at[axis]
        fresh = []
        if n == 2:
            steps = [(None, 1 - p, None)]
        else:
            steps = []
            for k in range(1, n):
                steps.append((p - k >= 0, p - k, 0))
                steps.append((p + k <= n - 1, p + k, 1))
        for cond, o, way in steps:
            for kcond, kat in known:
                at = list(kat)
                at[axis] = o
                at = tuple(at)
                both = cond if kcond is None else (kcond if cond is None else jnp.logical_and(cond, kcond))

                def onward(at, way, i, axis):
                    outs = []
                    if way is not None:
                        cond2, to = net.near(axis)[way]
                        outs.append((cond2, 2 * i + way, (net.chip(net.moved(axis, to)), net.c)))
                    for j in range(i + 1, len(order)):
                        for k, (c2, to) in enumerate(net.near(order[j])):
                            outs.append((c2, 2 * j + k, (net.chip(net.moved(order[j], to)), net.c)))
                    if partner:
                        outs.append((None, 6, (net.e, 1 - net.c)))
                    return outs

                def arrive(at=at, way=way, i=i, axis=axis):
                    ch = net.chip(at)
                    rcopy(block(ch, net.c), block(ch, net.c), ss(ch, 0), rs(ch, net.c), (net.e, net.c)).wait_recv()
                    for c2, kind, dev in onward(at, way, i, axis):
                        send(c2, at, kind, dev)

                when(both, arrive)

                def drain(at=at, way=way, i=i, axis=axis, both=both):
                    def inner():
                        ch = net.chip(at)
                        for c2, kind, dev in onward(at, way, i, axis):
                            when(c2, lambda kind=kind, dev=dev: rcopy(
                                block(ch, net.c), block(ch, net.c), ss(ch, kind), rs(ch, net.c), dev).wait_send())
                    when(both, inner)

                done.append(drain)
                fresh.append((both, at))
                yield
        known = known + fresh
    if partner:
        for kcond, kat in known:
            def theirs(kat=kat):
                ch = net.chip(kat)
                rcopy(block(ch, 1 - net.c), block(ch, 1 - net.c), ss(ch, 0), rs(ch, 1 - net.c), (net.e, net.c)).wait_recv()
            done.append(lambda kcond=kcond, theirs=theirs: when(kcond, theirs))


def add_into(dst, src, rows):
    step = 16
    assert rows % step == 0

    def body(i, _):
        r = pl.ds(pl.multiple_of(i * step, step), step)
        dst[r, :] = (dst[r, :].astype(F32) + src[r, :].astype(F32)).astype(BF)
        return 0

    lax.fori_loop(0, rows // step, body, 0)


def rs_piece(net, order, mine, acc, bufs, key, rs, ss, rows, done, partner=True):
    def all_combos(axes_left):
        out = [()]
        for ax in axes_left:
            out = [o + (v,) for o in out for v in range(net.dims[ax])]
        return out

    def p_send(at):
        ch = net.chip(at)
        mk = lambda: rcopy(mine(ch, 1 - net.c), acc(ch), ss(0, ch), rs(0, ch), (net.e, 1 - net.c))
        mk().start()
        done.append(lambda: mk().wait_send())

    def p_recv(at):
        ch = net.chip(at)
        rcopy(acc(ch), acc(ch), ss(0, ch), rs(0, ch), (net.e, net.c)).wait_recv()
        add_into(acc(ch), mine(ch, net.c), rows)

    stages = []
    for i, axis in enumerate(order):
        left = order[i + 1:]
        combos = all_combos(left)
        stages.append((i, axis, left, combos))

    def targets_of(i, axis, left, combo, t):
        at = list(net.at)
        at[axis] = t
        for ax, v in zip(left, combo):
            at[ax] = v
        return tuple(at)

    for i, axis, left, combos in stages:
        n, p = net.dims[axis], net.at[axis]
        for combo in combos:
            for d in range(1, n):
                t = (p + d) % n
                p_send(targets_of(i, axis, left, combo, t))
        yield
    p_send(net.at)
    yield

    for i, axis, left, combos in stages:
        n, p = net.dims[axis], net.at[axis]
        nxt = lambda to, axis=axis: (net.chip(net.moved(axis, to)), net.c)

        def gather_prev(at):
            p_recv(at)
            for i2, axis2, left2, _ in stages[:i]:
                land(i2, axis2, left2, at)

        def land(i2, axis2, left2, at):
            n2, p2 = net.dims[axis2], net.at[axis2]
            ch = net.chip(at)

            def take(way):
                k = key(i2, way, at)
                rcopy(bufs(i2, k), bufs(i2, k), ss(i2 + 1, k), rs(i2 + 1, k), (net.e, net.c)).wait_recv()
                add_into(acc(ch), bufs(i2, k), rows)

            if n2 == 2:
                take(0)
            else:
                when(p2 > 0, lambda: take(0))
                when(p2 < n2 - 1, lambda: take(1))

        for combo in combos:
            if n == 2:
                at = targets_of(i, axis, left, combo, 1 - p)
                gather_prev(at)
                ch = net.chip(at)
                k = key(i, 0, at)
                mk = lambda ch=ch, k=k, i=i: rcopy(acc(ch), bufs(i, k), ss(i + 1, k), rs(i + 1, k), nxt(1 - p))
                mk().start()
                done.append(lambda mk=mk: mk().wait_send())
                yield
            else:
                for s in range(n - 1):
                    for way in (0, 1):
                        t = n - 1 - s if way == 0 else s
                        cond = (p < t) if way == 0 else (p > t)
                        to = p + 1 if way == 0 else p - 1
                        inner_cond = (p > 0) if way == 0 else (p < n - 1)
                        at = targets_of(i, axis, left, combo, t)
                        ch, k = net.chip(at), key(i, way, at)
                        mk = lambda ch=ch, k=k, i=i, to=to: rcopy(acc(ch), bufs(i, k), ss(i + 1, k), rs(i + 1, k), nxt(to))

                        def step(at=at, ch=ch, k=k, i=i, inner_cond=inner_cond, mk=mk):
                            gather_prev(at)

                            def relay():
                                rcopy(bufs(i, k), bufs(i, k), ss(i + 1, k), rs(i + 1, k), (net.e, net.c)).wait_recv()
                                add_into(acc(ch), bufs(i, k), rows)

                            pl.when(inner_cond)(relay)
                            mk().start()

                        pl.when(cond)(step)
                        done.append(lambda cond=cond, mk=mk: pl.when(cond)(lambda: mk().wait_send()))
                        yield
    at = net.at
    p_recv(at)
    for i2, axis2, left2, _ in stages:
        n2, p2 = net.dims[axis2], net.at[axis2]
        ch = net.chip(at)

        def take(way, i2=i2):
            k = key(i2, way, at)
            rcopy(bufs(i2, k), bufs(i2, k), ss(i2 + 1, k), rs(i2 + 1, k), (net.e, net.c)).wait_recv()
            add_into(acc(ch), bufs(i2, k), rows)

        if n2 == 2:
            take(0)
        else:
            when(p2 > 0, lambda: take(0))
            when(p2 < n2 - 1, lambda: take(1))
        yield


def rs_keys(net, order):
    def size(i):
        left = order[i + 1:]
        m = 1
        for ax in left:
            m *= net.dims[ax]
        n = net.dims[order[i]]
        return m if n == 2 else 2 * n * m

    def key(i, way, at):
        left = order[i + 1:]
        k = 0
        for ax in left:
            k = k * net.dims[ax] + at[ax]
        n = net.dims[order[i]]
        if n == 2:
            return k
        return (k * n + at[order[i]]) * 2 + way

    return key, [size(i) for i in range(len(order))]


def params(cid, vmem=None):
    return pltpu.CompilerParams(collective_id=cid, has_side_effects=True, vmem_limit_bytes=vmem)


ANY = pl.BlockSpec(memory_space=pl.ANY)
VM = pl.BlockSpec(memory_space=pltpu.VMEM)
DMA = pltpu.SemaphoreType.DMA

ORDER_A = (0, 1, 2)
ORDER_B = (0, 2, 1)


def all_gather_all(n_expert, x, cid):
    rows, cols = x.shape
    half = rows // 2

    def kernel(x_ref, o_ref, rsem, ssem, lsem):
        net = Net(n_expert).enter()
        cp = pltpu.make_async_copy(x_ref, o_ref.at[net.e, net.c], lsem)
        cp.start()
        greet(net, (0, 1, 2))
        cp.wait()
        done = []
        gens = []
        for i, order in enumerate((ORDER_A, ORDER_B)):
            gens.append(ag_piece(
                net, order,
                lambda ch, co, i=i: o_ref.at[ch, co, pl.ds(i * half, half)],
                lambda ch, co, i=i: rsem.at[i, ch, co],
                lambda ch, kind, i=i: ssem.at[i, ch, kind], done))
        interleave(*gens)
        for f in done:
            f()

    return pl.pallas_call(
        kernel, out_shape=jax.ShapeDtypeStruct((n_expert, 2, rows, cols), x.dtype),
        in_specs=[VM], out_specs=ANY,
        scratch_shapes=[DMA((2, n_expert, 2)), DMA((2, n_expert, 7)), DMA],
        compiler_params=params(cid), name="gather_all",
    )(x)


def reduce_scatter_all(n_expert, t, cid):
    _, _, rows, cols = t.shape
    half = rows // 2
    net0 = Net(n_expert)
    orders = ((2, 1, 0), (1, 2, 0))
    keys = [rs_keys(net0, o) for o in orders]
    sizes = keys[0][1]
    ns = max([n_expert] + sizes)

    def kernel(t_ref, o_ref, acc, b0, b1, b2, rsem, ssem):
        net = Net(n_expert).enter()
        greet(net, (0, 1, 2))
        done, gens = [], []
        bb = (b0, b1, b2)
        for i, order in enumerate(orders):
            key = keys[i][0]
            r = pl.ds(i * half, half)
            gens.append(rs_piece(
                net, order,
                lambda ch, co, r=r: t_ref.at[ch, co, r],
                lambda ch, r=r: acc.at[ch, r],
                lambda st, k, r=r: bb[st].at[k, r],
                key,
                lambda st, k, i=i: rsem.at[i, st, k],
                lambda st, k, i=i: ssem.at[i, st, k], half, done))
        interleave(*gens)
        o_ref[...] = acc[net.e]
        for f in done:
            f()

    return pl.pallas_call(
        kernel, out_shape=jax.ShapeDtypeStruct((rows, cols), BF),
        in_specs=[VM], out_specs=VM,
        scratch_shapes=[pltpu.VMEM((n_expert, rows, cols), BF)]
        + [pltpu.VMEM((s, rows, cols), BF) for s in sizes]
        + [DMA((2, 4, ns)), DMA((2, 4, ns))],
        compiler_params=params(cid, 60 << 20), name="reduce_all",
    )(t)


def local_copy(src, dst, sem, done):
    cp = lambda: pltpu.make_async_copy(src, dst, sem)
    cp().start()
    done.append(lambda: cp().wait())


def col_ag(net, src, dst, rs, ss, done):
    z, c = net.at[0], net.c
    n = net.dims[0]
    own = z // 2 == c
    s0 = z % 2

    def zdev(to):
        return (net.chip(net.moved(0, to)), c)

    def hop(cond, s, h, way, to, source=None):
        mk = lambda: rcopy(dst(s, h) if source is None else source, dst(s, h), ss(way, s, h), rs(s, h), zdev(to))
        when(cond, lambda: mk().start())
        return lambda: when(cond, lambda: mk().wait_send())

    def arrived(s, h):
        rcopy(dst(s, h), dst(s, h), ss(0, s, h), rs(s, h), (net.e, c)).wait_recv()

    across = lambda: rcopy(src, dst(s0, c), ss(2, 0, 0), rs(s0, c), (net.e, 1 - c))
    keep = lambda: pltpu.make_async_copy(src, dst(s0, c), ss(2, 0, 1))

    def begin():
        keep().start()
        hop(z < n - 1, s0, c, 0, z + 1, src)
        hop(z > 0, s0, c, 1, z - 1, src)

    pl.when(own)(begin)
    pl.when(jnp.logical_not(own))(lambda: across().start())
    yield

    def second():
        arrived(s0, 1 - c)
        hop(z < n - 1, s0, 1 - c, 0, z + 1)
        hop(z > 0, s0, 1 - c, 1, z - 1)

    pl.when(own)(second)
    yield

    def end():
        keep().wait()
        for h in (c, 1 - c):
            source = src if h is c else None
            when(z < n - 1, lambda h=h, source=source: rcopy(
                src if source is not None else dst(s0, h), dst(s0, h), ss(0, s0, h), rs(s0, h), zdev(z + 1)).wait_send())
            when(z > 0, lambda h=h, source=source: rcopy(
                src if source is not None else dst(s0, h), dst(s0, h), ss(1, s0, h), rs(s0, h), zdev(z - 1)).wait_send())

    done.append(lambda: pl.when(own)(end))
    done.append(lambda: pl.when(jnp.logical_not(own))(lambda: across().wait_send()))

    for k in range(1, n):
        for way in (0, 1):
            o = z - k if way == 0 else z + k
            inside = o >= 0 if way == 0 else o <= n - 1
            cond = jnp.logical_and(inside, o // 2 == c)
            more = z < n - 1 if way == 0 else z > 0
            to = z + 1 if way == 0 else z - 1

            def step(o=o, way=way, more=more, to=to):
                for h in (0, 1):
                    arrived(o % 2, h)
                    hop(more, o % 2, h, way, to)

            def finish(o=o, way=way, more=more, to=to):
                for h in (0, 1):
                    when(more, lambda h=h: rcopy(
                        dst(o % 2, h), dst(o % 2, h), ss(way, o % 2, h), rs(o % 2, h), zdev(to)).wait_send())

            pl.when(cond)(step)
            done.append(lambda cond=cond, finish=finish: pl.when(cond)(finish))
            yield


def col_rs(net, part, out, acc, buf, fin, rs, ss, rows, done):
    z, c = net.at[0], net.c
    n = net.dims[0]

    def zdev(to):
        return (net.chip(net.moved(0, to)), c)

    def msg(way, s, h, to):
        return rcopy(acc(way, s, h), buf(way, s, h), ss(way, s, h), rs(way, s, h), zdev(to))

    def arrived(way, s, h):
        rcopy(buf(way, s, h), buf(way, s, h), ss(way, s, h), rs(way, s, h), (net.e, c)).wait_recv()

    for k in range(n - 1):
        for way in (0, 1):
            t = n - 1 - k if way == 0 else k
            s = t % 2
            cond = jnp.logical_and(z < t if way == 0 else z > t, t // 2 == c)
            inner = z > 0 if way == 0 else z < n - 1
            to = z + 1 if way == 0 else z - 1
            for h in (0, 1):
                def step(way=way, s=s, h=h, inner=inner, to=to):
                    def relay():
                        arrived(way, s, h)
                        sum_to(acc(way, s, h), [part(s, h), buf(way, s, h)], rows)

                    pl.when(inner)(relay)
                    pl.when(jnp.logical_not(inner))(lambda: sum_to(acc(way, s, h), [part(s, h)], rows))
                    msg(way, s, h, to).start()

                pl.when(cond)(step)
                done.append(lambda cond=cond, way=way, s=s, h=h, to=to: pl.when(cond)(lambda: msg(way, s, h, to).wait_send()))
                yield

    own = z // 2 == c
    s0 = z % 2
    cross = lambda: rcopy(fin(0), fin(1), ss(2, 0, 0), rs(2, 0, 0), (net.e, 1 - c))

    def last(h, to_ref):
        low, high = z > 0, z < n - 1
        pl.when(low)(lambda: arrived(0, s0, h))
        pl.when(high)(lambda: arrived(1, s0, h))
        mid = jnp.logical_and(low, high)
        pl.when(mid)(lambda: sum_to(to_ref, [part(s0, h), buf(0, s0, h), buf(1, s0, h)], rows))
        pl.when(jnp.logical_not(low))(lambda: sum_to(to_ref, [part(s0, h), buf(1, s0, h)], rows))
        pl.when(jnp.logical_not(high))(lambda: sum_to(to_ref, [part(s0, h), buf(0, s0, h)], rows))

    def final():
        last(1 - c, fin(0))
        cross().start()
        last(c, out)

    pl.when(own)(final)
    done.append(lambda: pl.when(own)(lambda: cross().wait_send()))

    def take():
        cross().wait_recv()
        sum_to(out, [fin(1)], rows)

    yield
    pl.when(jnp.logical_not(own))(take)


def sum_to(dst, srcs, rows):
    step = 16

    def body(i, _):
        r = pl.ds(pl.multiple_of(i * step, step), step)
        v = srcs[0][r, :]
        if len(srcs) > 1:
            v = v.astype(F32)
            for s in srcs[1:]:
                v = v + s[r, :].astype(F32)
        dst[r, :] = v.astype(BF)
        return 0

    lax.fori_loop(0, rows // step, body, 0)


def to_all(net, src, dst, rs, ss, done):
    total = net.chips * 2
    me = net.e * 2 + net.c

    def put(k, _):
        t = (me + k) % total
        rcopy(src(t), dst(me), ss(k), rs(me), (t // 2, t % 2)).start()
        return 0

    lax.fori_loop(1, total, put, 0)
    yield

    def take(k, _):
        t = (me + k) % total
        rcopy(src(t), dst(me), ss(k), rs(me), (t // 2, t % 2)).wait_send()
        rcopy(dst(t), dst(t), ss(k), rs(t), (net.e, net.c)).wait_recv()
        return 0

    done.append(lambda: lax.fori_loop(1, total, take, 0))


def gather_start(n_expert, tokens, wqkv, w_out, aux, cot, cid):
    T, D = tokens.shape
    Z, R, C = wqkv.shape
    HR = w_out.shape[0]
    AR, AW = aux.shape
    plane = n_expert // Z
    nd = 2 * n_expert

    with_g = cot is not None

    def kernel(*refs):
        k = 5 if with_g else 4
        t_ref, w_ref, o_ref, a_ref = refs[:4]
        g_ref, G = (refs[4], refs[2 * k - 1]) if with_g else (None, None)
        X, W, O, A = refs[k:k + 4]
        xr, xs, wr, ws, war, was, oar, oas, ar, as_, gr, gs, loc = refs[2 * k:]
        net = Net(n_expert).enter()
        z, p, c = net.at[0], net.e % plane, net.c
        me = net.e * 2 + c
        done = []
        local_copy(w_ref.at[z], W.at[z, p, c], loc.at[0], [])
        local_copy(o_ref, O.at[p, c], loc.at[1], [])
        local_copy(a_ref, A.at[me], loc.at[2], done)
        if with_g:
            local_copy(g_ref, G.at[net.e, c], loc.at[3], [])
        greet_all(net)

        def wgen():
            for k in range(1, Z):
                j = (z + k) % Z
                mk = lambda j=j, k=k: rcopy(w_ref.at[j], W.at[z, p, c], ws.at[k], wr.at[z], (j * plane + p, c))
                mk().start()
                done.append(lambda mk=mk: mk().wait_send())
            yield
            pltpu.make_async_copy(w_ref.at[z], W.at[z, p, c], loc.at[0]).wait()
            for k in range(1, Z):
                o = (z + k) % Z
                rcopy(W.at[o, p, c], W.at[o, p, c], ws.at[k], wr.at[o], (net.e, c)).wait_recv()
            gens = []
            for i, order in enumerate(((1, 2), (2, 1))):
                r = pl.ds(i * (Z // 2), Z // 2)
                gens.append(ag_piece(
                    net, order, lambda ch, co, r=r: W.at[r, ch % plane, co],
                    lambda ch, co, i=i: war.at[i, ch % plane, co], lambda ch, kind, i=i: was.at[i, ch % plane, kind], done))
            while gens:
                for g in list(gens):
                    try:
                        next(g)
                        yield
                    except StopIteration:
                        gens.remove(g)

        def ogen(i, order):
            if i == 0:
                pltpu.make_async_copy(o_ref, O.at[p, c], loc.at[1]).wait()
            r = pl.ds(i * (HR // 2), HR // 2)
            yield from ag_piece(
                net, order, lambda ch, co: O.at[ch % plane, co, r],
                lambda ch, co: oar.at[i, ch % plane, co], lambda ch, kind: oas.at[i, ch % plane, kind], done)

        def ggen(i, order):
            if i == 0:
                pltpu.make_async_copy(g_ref, G.at[net.e, c], loc.at[3]).wait()
            r = pl.ds(i * (T // 2), T // 2)
            yield from ag_piece(
                net, order, lambda ch, co: G.at[ch, co, r],
                lambda ch, co: gr.at[i, ch, co], lambda ch, kind: gs.at[i, ch, kind], done)

        interleave(
            wgen(),
            to_all(net, lambda t: a_ref, lambda s: A.at[s], lambda s: ar.at[s], lambda k: as_.at[k], done),
            col_ag(net, t_ref, lambda s, h: X.at[s, h], lambda s, h: xr.at[s, h], lambda w, s, h: xs.at[w, s, h], done),
            ogen(0, (1, 2)), ogen(1, (2, 1)), *([ggen(0, ORDER_A), ggen(1, ORDER_B)] if with_g else []))
        for f in done:
            f()

    S = jax.ShapeDtypeStruct
    return pl.pallas_call(
        kernel,
        out_shape=(S((2, 2, T, D), BF), S((Z, plane, 2, R, C), BF), S((plane, 2, HR, D), BF), S((nd, AR, AW), BF))
        + ((S((n_expert, 2, T, D), BF),) if with_g else ()),
        in_specs=[VM] * (5 if with_g else 4), out_specs=(ANY,) * (5 if with_g else 4),
        scratch_shapes=[DMA((2, 2)), DMA((3, 2, 2)), DMA((Z,)), DMA((Z,)), DMA((2, plane, 2)), DMA((2, plane, 7)),
                        DMA((2, plane, 2)), DMA((2, plane, 7)), DMA((nd,)), DMA((nd,)),
                        DMA((2, n_expert, 2)), DMA((2, n_expert, 7)), DMA((4,))],
        compiler_params=params(cid), name="gather_start",
    )(tokens, wqkv, w_out, aux, *((cot,) if with_g else ()))


def column_sum(n_expert, part, cid):
    _, _, T, D = part.shape

    def kernel(p_ref, o_ref, acc, buf, fin, rsem, ssem):
        net = Net(n_expert).enter()
        greet(net, (0,))
        done = []
        interleave(col_rs(
            net, lambda s, h: p_ref.at[s, h], o_ref, lambda w, s, h: acc.at[w, s, h], lambda w, s, h: buf.at[w, s, h],
            lambda i: fin.at[i], lambda w, s, h: rsem.at[w, s, h], lambda w, s, h: ssem.at[w, s, h], T, done))
        for f in done:
            f()

    return pl.pallas_call(
        kernel, out_shape=jax.ShapeDtypeStruct((T, D), BF), in_specs=[VM], out_specs=VM,
        scratch_shapes=[pltpu.VMEM((2, 2, 2, T, D), BF), pltpu.VMEM((2, 2, 2, T, D), BF), pltpu.VMEM((2, T, D), BF),
                        DMA((3, 2, 2)), DMA((3, 2, 2))],
        compiler_params=params(cid, 40 << 20), name="column_sum",
    )(part)


def column_gather(n_expert, x, cid):
    T, D = x.shape

    def kernel(x_ref, X, rsem, ssem):
        net = Net(n_expert).enter()
        greet(net, (0,))
        done = []
        interleave(col_ag(net, x_ref, lambda s, h: X.at[s, h], lambda s, h: rsem.at[s, h], lambda w, s, h: ssem.at[w, s, h], done))
        for f in done:
            f()

    return pl.pallas_call(
        kernel, out_shape=jax.ShapeDtypeStruct((2, 2, T, D), BF), in_specs=[VM], out_specs=ANY,
        scratch_shapes=[DMA((2, 2)), DMA((3, 2, 2))],
        compiler_params=params(cid), name="column_gather",
    )(x)


def gather_all(n_expert, x, aux, cid):
    rows, cols = x.shape
    half = rows // 2
    nd = 2 * n_expert

    def kernel(x_ref, a_ref, o_ref, A, rsem, ssem, ar, as_, lsem):
        net = Net(n_expert).enter()
        me = net.e * 2 + net.c
        done = []
        local_copy(x_ref, o_ref.at[net.e, net.c], lsem.at[0], [])
        local_copy(a_ref, A.at[me], lsem.at[1], done)
        greet_all(net)
        pltpu.make_async_copy(x_ref, o_ref.at[net.e, net.c], lsem.at[0]).wait()
        gens = [to_all(net, lambda t: a_ref, lambda s: A.at[s], lambda s: ar.at[s], lambda k: as_.at[k], done)]
        for i, order in enumerate((ORDER_A, ORDER_B)):
            gens.append(ag_piece(
                net, order,
                lambda ch, co, i=i: o_ref.at[ch, co, pl.ds(i * half, half)],
                lambda ch, co, i=i: rsem.at[i, ch, co],
                lambda ch, kind, i=i: ssem.at[i, ch, kind], done))
        interleave(*gens)
        for f in done:
            f()

    return pl.pallas_call(
        kernel,
        out_shape=(jax.ShapeDtypeStruct((n_expert, 2, rows, cols), x.dtype), jax.ShapeDtypeStruct((nd,) + aux.shape, aux.dtype)),
        in_specs=[VM, VM], out_specs=(ANY, ANY),
        scratch_shapes=[DMA((2, n_expert, 2)), DMA((2, n_expert, 7)), DMA((nd,)), DMA((nd,)), DMA((2,))],
        compiler_params=params(cid), name="gather_all",
    )(x, aux)


def exchange(n_expert, x, cid):
    nd = 2 * n_expert

    def kernel(x_ref, o_ref, ar, as_, lsem):
        net = Net(n_expert).enter()
        me = net.e * 2 + net.c
        done = []
        local_copy(x_ref.at[me], o_ref.at[me], lsem.at[0], done)
        greet_all(net)
        interleave(to_all(net, lambda t: x_ref.at[t], lambda s: o_ref.at[s], lambda s: ar.at[s], lambda k: as_.at[k], done))
        for f in done:
            f()

    return pl.pallas_call(
        kernel, out_shape=jax.ShapeDtypeStruct(x.shape, x.dtype), in_specs=[VM], out_specs=VM,
        scratch_shapes=[DMA((nd,)), DMA((nd,)), DMA((2,))],
        compiler_params=params(cid), name="exchange",
    )(x)


def reduce_end(n_expert, part, dw, do, small, cid):
    _, _, T, D = part.shape
    Z, plane, _, R, C = dw.shape
    HR = do.shape[2]
    nd = 2 * n_expert
    net0 = Net(n_expert)
    orders = ((2, 1), (1, 2))
    keys = [rs_keys(net0, o) for o in orders]
    sizes = keys[0][1]
    ns = max([plane] + sizes)
    hr = HR // 2

    def kernel(p_ref, dw_ref, do_ref, s_ref, x_out, w_out, o_out, s_out,
               acc, buf, fin, wacc, wb0, wb1, oacc, ob0, ob1, wsh,
               xr, xs, wr, ws, our, ous, sr, s_s, zr, zs, loc):
        net = Net(n_expert).enter()
        z, p, c = net.at[0], net.e % plane, net.c
        me = net.e * 2 + c
        done = []
        local_copy(s_ref.at[me], s_out.at[me], loc.at[0], done)
        greet_all(net)

        def wgen(q):
            i = q // (Z // 2)
            key = keys[i][0]
            bb = (wb0, wb1)
            yield from rs_piece(
                net, orders[i], lambda ch, co: dw_ref.at[q, ch % plane, co], lambda ch: wacc.at[q, ch % plane],
                lambda st, k: bb[st].at[q, k], key, lambda st, k: wr.at[q, st, k if st else k % plane],
                lambda st, k: ws.at[q, st, k if st else k % plane], R, done)
            mk = lambda: rcopy(wacc.at[q, p], wsh.at[z], zs.at[q], zr.at[z], (q * plane + p, c))
            pl.when(z != q)(lambda: mk().start())
            done.append(lambda: pl.when(z != q)(lambda: mk().wait_send()))
            pl.when(z == q)(lambda: sum_to(w_out.at[q], [wacc.at[q, p]], R))

        def ogen(i):
            key = keys[i][0]
            bb = (ob0, ob1)
            r = pl.ds(i * hr, hr)
            yield from rs_piece(
                net, orders[i], lambda ch, co: do_ref.at[ch % plane, co, r], lambda ch: oacc.at[ch % plane, r],
                lambda st, k: bb[st].at[k, r], key, lambda st, k: our.at[i, st, k if st else k % plane],
                lambda st, k: ous.at[i, st, k if st else k % plane], hr, done)

        interleave(
            to_all(net, lambda t: s_ref.at[t], lambda s: s_out.at[s], lambda s: sr.at[s], lambda k: s_s.at[k], done),
            *[wgen(q) for q in range(Z)],
            col_rs(net, lambda s, h: p_ref.at[s, h], x_out, lambda w, s, h: acc.at[w, s, h], lambda w, s, h: buf.at[w, s, h],
                   lambda i: fin.at[i], lambda w, s, h: xr.at[w, s, h], lambda w, s, h: xs.at[w, s, h], T, done),
            ogen(0), ogen(1))
        o_out[...] = oacc[p]
        for k in range(1, Z):
            o = (z + k) % Z
            rcopy(wsh.at[o], wsh.at[o], zs.at[0], zr.at[o], (net.e, c)).wait_recv()
            sum_to(w_out.at[o], [wsh.at[o]], R)
        for f in done:
            f()

    S = jax.ShapeDtypeStruct
    V = pltpu.VMEM
    return pl.pallas_call(
        kernel, out_shape=(S((T, D), BF), S((Z, R, C), BF), S((HR, D), BF), S(small.shape, small.dtype)),
        in_specs=[VM] * 4, out_specs=(VM,) * 4,
        scratch_shapes=[V((2, 2, 2, T, D), BF), V((2, 2, 2, T, D), BF), V((2, T, D), BF),
                        V((Z, plane, R, C), BF), V((Z, sizes[0], R, C), BF), V((Z, sizes[1], R, C), BF),
                        V((plane, HR, D), BF), V((sizes[0], HR, D), BF), V((sizes[1], HR, D), BF), V((Z, R, C), BF),
                        DMA((3, 2, 2)), DMA((3, 2, 2)), DMA((Z, 3, ns)), DMA((Z, 3, ns)), DMA((2, 3, ns)), DMA((2, 3, ns)),
                        DMA((nd,)), DMA((nd,)), DMA((Z,)), DMA((Z,)), DMA((1,))],
        compiler_params=params(cid, 60 << 20), name="reduce_end",
    )(part, dw, do, small)


def slot_plane(z, i):
    near = jnp.where(z < 2, z, 3 - z)
    t = jnp.where(jnp.logical_and(near == 1, i < 2), 1 - i, i)
    return jnp.where(z < 2, t, 3 - t)


class Gather22:
    def __init__(self, net, N, T, rsem, ssem):
        self.net, self.N, self.T, self.rsem, self.ssem = net, N, T, rsem, ssem
        self.axes = ((1, 2), (2, 1))

    def blk(self, piece, chip, core):
        h = self.T // 2
        return self.N.at[chip, pl.ds(pl.multiple_of(core * self.T + piece * h, h), h)]

    def copy(self, piece, at, kind, dev):
        n = self.net
        ch = n.chip(at)
        b = self.blk(piece, ch, n.c)
        return rcopy(b, b, self.ssem.at[piece, ch, kind], self.rsem.at[piece, ch, n.c], dev)

    def wait(self, piece, at, core):
        n = self.net
        ch = n.chip(at)
        b = self.blk(piece, ch, core)
        rcopy(b, b, self.ssem.at[piece, ch, 0], self.rsem.at[piece, ch, core], (n.e, n.c)).wait_recv()

    def dev(self, axis, to=None):
        n = self.net
        return (n.chip(n.moved(axis, 1 - n.at[axis] if to is None else to)), n.c)

    def level(self, piece, zt, two, three):
        n = self.net
        at = [zt, n.at[1], n.at[2]]
        u, v = self.axes[piece]
        if two:
            at[u] = 1 - at[u]
        if three:
            at[v] = 1 - at[v]
        return tuple(at)

    def outs(self, piece, zt, two, three):
        u, v = self.axes[piece]
        at = self.level(piece, zt, two, three)
        r = []
        if not two and not three:
            r.append((2, self.dev(u)))
        if not three:
            r.append((3, self.dev(v)))
        r.append((4, (self.net.e, 1 - self.net.c)))
        return at, r

    def push(self, piece, zt, two, three):
        at, r = self.outs(piece, zt, two, three)
        for kind, dev in r:
            self.copy(piece, at, kind, dev).start()

    def begin(self):
        z = self.net.at[0]
        for piece in (0, 1):
            pl.when(z < 3)(lambda piece=piece: self.copy(piece, self.net.at, 0, self.dev(0, z + 1)).start())
            pl.when(z > 0)(lambda piece=piece: self.copy(piece, self.net.at, 1, self.dev(0, z - 1)).start())
            self.push(piece, z, False, False)

    def onward(self, zt):
        z = self.net.at[0]
        to = jnp.where(zt < z, z + 1, z - 1)
        return to, jnp.logical_and(to >= 0, to <= 3)

    def from_z(self, zt):
        to, more = self.onward(zt)
        for piece in (0, 1):
            at = self.level(piece, zt, False, False)
            self.wait(piece, at, self.net.c)
            pl.when(more)(lambda piece=piece, at=at: self.copy(piece, at, 0, self.dev(0, to)).start())
            self.push(piece, zt, False, False)

    def from_two(self, zt):
        for piece in (0, 1):
            self.wait(piece, self.level(piece, zt, True, False), self.net.c)
            self.push(piece, zt, True, False)

    def from_three(self, zt):
        for two in (False, True):
            for piece in (0, 1):
                self.wait(piece, self.level(piece, zt, two, True), self.net.c)
                self.push(piece, zt, two, True)

    def from_partner(self, zt):
        for piece in (0, 1):
            for a in (0, 1):
                for b in (0, 1):
                    self.wait(piece, (zt, a, b), 1 - self.net.c)

    def drain(self, i):
        z = self.net.at[0]
        zt = slot_plane(z, i)
        to, more = self.onward(zt)
        for piece in (0, 1):
            def own(piece=piece):
                pl.when(z < 3)(lambda: self.copy(piece, self.net.at, 0, self.dev(0, z + 1)).wait_send())
                pl.when(z > 0)(lambda: self.copy(piece, self.net.at, 1, self.dev(0, z - 1)).wait_send())

            pl.when(i == 0)(own)
            at0 = self.level(piece, zt, False, False)
            pl.when(jnp.logical_and(i > 0, more))(
                lambda piece=piece, at0=at0: self.copy(piece, at0, 0, self.dev(0, to)).wait_send())
            for two in (False, True):
                for three in (False, True):
                    at, r = self.outs(piece, zt, two, three)
                    for kind, dev in r:
                        self.copy(piece, at, kind, dev).wait_send()


def add_rows(dst, srcs, rows):
    step = 32

    def body(i, _):
        r = pl.ds(pl.multiple_of(i * step, step), step)
        v = dst[r, :].astype(F32)
        for s in srcs:
            v = v + s[r, :].astype(F32)
        dst[r, :] = v.astype(BF)
        return 0

    lax.fori_loop(0, rows // step, body, 0)


class Reduce22:
    def __init__(self, net, T, acc, buf1, buf2, zbuf, sems):
        self.net, self.T = net, T
        self.acc, self.buf1, self.buf2, self.zbuf = acc, buf1, buf2, zbuf
        (self.r0, self.s0, self.r1, self.s1, self.r2, self.s2, self.r3, self.s3) = sems
        self.first = (2, 1)
        self.second = (1, 2)

    @staticmethod
    def scratch(T, D):
        V = pltpu.VMEM
        return [V((16, T, D), BF), V((4, 2, T, D), BF), V((4, T, D), BF), V((2, 4, T, D), BF),
                DMA((16,)), DMA((16,)), DMA((2, 4, 2)), DMA((2, 4, 2)), DMA((2, 4)), DMA((2, 4)), DMA((2, 2, 4)), DMA((2, 2, 4))]

    def half(self, piece):
        h = self.T // 2
        return pl.ds(piece * h, h)

    def ring(self):
        n = self.net
        a, b = n.at[1], n.at[2]
        return [(1 - a, 1 - b), (a, 1 - b), (1 - a, b), (a, b)]

    def p_copy(self, Tb, zt, ab):
        n = self.net
        p = ab[0] * 2 + ab[1]
        ch = zt * 4 + p
        src = Tb.at[p, pl.ds(pl.multiple_of((1 - n.c) * self.T, self.T), self.T)]
        return rcopy(src, self.acc.at[ch], self.s0.at[ch], self.r0.at[ch], (n.e, 1 - n.c))

    def p_send(self, Tb, zt):
        for ab in self.ring():
            self.p_copy(Tb, zt, ab).start()

    def p_wait_send(self, Tb, zt):
        for ab in self.ring():
            self.p_copy(Tb, zt, ab).wait_send()

    def p_take(self, Tb, zt, ab):
        n = self.net
        p = ab[0] * 2 + ab[1]
        self.p_copy(Tb, zt, ab).wait_recv()
        add_rows(self.acc.at[zt * 4 + p], [Tb.at[p, pl.ds(pl.multiple_of(n.c * self.T, self.T), self.T)]], self.T)

    def one(self, piece, zt, idx):
        n = self.net
        ax = self.first[piece]
        at = [zt, n.at[1], n.at[2]]
        at[ax] = 1 - at[ax]
        at[self.second[piece]] = idx
        src = self.acc.at[n.chip(at), self.half(piece)]
        dst = self.buf1.at[zt, idx, self.half(piece)]
        return rcopy(src, dst, self.s1.at[piece, zt, idx], self.r1.at[piece, zt, idx], (n.chip(n.moved(ax, 1 - n.at[ax])), n.c))

    def two(self, piece, zt):
        n = self.net
        ax = self.second[piece]
        at = [zt, n.at[1], n.at[2]]
        at[ax] = 1 - at[ax]
        src = self.acc.at[n.chip(at), self.half(piece)]
        return rcopy(src, self.buf2.at[zt, self.half(piece)], self.s2.at[piece, zt], self.r2.at[piece, zt],
                     (n.chip(n.moved(ax, 1 - n.at[ax])), n.c))

    def three(self, piece, zt):
        n = self.net
        z = n.at[0]
        up = zt > z
        d = jnp.where(up, 0, 1)
        to = jnp.where(up, z + 1, z - 1)
        src = self.acc.at[n.chip((zt, n.at[1], n.at[2])), self.half(piece)]
        return rcopy(src, self.zbuf.at[d, zt, self.half(piece)], self.s3.at[piece, d, zt], self.r3.at[piece, d, zt],
                     (n.chip(n.moved(0, to)), n.c))

    def stage0(self, Tb, zt):
        n = self.net
        order = self.ring()
        self.p_take(Tb, zt, order[0])
        self.one(0, zt, 1 - n.at[1]).start()
        self.one(1, zt, 1 - n.at[2]).start()
        self.p_take(Tb, zt, order[1])
        self.one(0, zt, n.at[1]).start()
        self.p_take(Tb, zt, order[2])
        self.one(1, zt, n.at[2]).start()
        self.p_take(Tb, zt, order[3])

    def stage1(self, zt):
        n = self.net
        for part in (0, 1):
            for piece in (0, 1):
                own = n.at[self.second[piece]]
                idx = 1 - own if part == 0 else own
                at = [zt, n.at[1], n.at[2]]
                at[self.second[piece]] = idx
                self.one(piece, zt, idx).wait_recv()
                add_rows(self.acc.at[n.chip(at), self.half(piece)], [self.buf1.at[zt, idx, self.half(piece)]], self.T // 2)
                if part == 0:
                    self.two(piece, zt).start()

    def stage2(self, zt):
        n = self.net
        z = n.at[0]
        feeds = jnp.where(zt > z, z > 0, z < 3)
        for piece in (0, 1):
            self.two(piece, zt).wait_recv()
            add_rows(self.acc.at[n.chip((zt, n.at[1], n.at[2])), self.half(piece)], [self.buf2.at[zt, self.half(piece)]], self.T // 2)
            pl.when(jnp.logical_and(zt != z, jnp.logical_not(feeds)))(lambda piece=piece: self.three(piece, zt).start())

    def relay(self, zt):
        n = self.net
        z = n.at[0]
        d = jnp.where(zt > z, 0, 1)
        feeds = jnp.where(zt > z, z > 0, z < 3)

        def go():
            for piece in (0, 1):
                self.three(piece, zt).wait_recv()
                add_rows(self.acc.at[n.chip((zt, n.at[1], n.at[2])), self.half(piece)],
                         [self.zbuf.at[d, zt, self.half(piece)]], self.T // 2)
                self.three(piece, zt).start()

        pl.when(jnp.logical_and(zt != z, feeds))(go)

    def arrive(self, piece, d):
        n = self.net
        z = n.at[0]
        dst = self.zbuf.at[d, z, self.half(piece)]
        rcopy(dst, dst, self.s3.at[piece, d, z], self.r3.at[piece, d, z], (n.e, n.c)).wait_recv()
        add_rows(self.acc.at[n.e, self.half(piece)], [dst], self.T // 2)

    def last(self, out):
        z = self.net.at[0]
        for piece in (0, 1):
            pl.when(z > 0)(lambda piece=piece: self.arrive(piece, 0))
            pl.when(z < 3)(lambda piece=piece: self.arrive(piece, 1))
        out[...] = self.acc[self.net.e]

    def drain(self, zt):
        n = self.net
        for piece in (0, 1):
            for idx in (0, 1):
                self.one(piece, zt, idx).wait_send()
            self.two(piece, zt).wait_send()
            pl.when(zt != n.at[0])(lambda piece=piece: self.three(piece, zt).wait_send())


NT = (((1,), (1,)), ((), ()))
TN = (((0,), (0,)), ((), ()))


def experts_fused(x, marked, G, w_gate, w_up, w_down, cap, cid):
    T, D = x.shape
    E = marked.shape[0]
    X2, _, Fh = w_gate.shape
    chips = G.shape[0]
    nd = 2 * chips
    S2 = 2 * cap
    M = 4 * S2
    CW = 512
    PR = 64
    SW = 1024

    def kernel(x_ref, a_ref, g_ref, wg_ref, wu_ref, wd_ref, o_sum, o_part, o_dots, o_rows, o_grows, o_act, o_ggu, N,
               A, wgu, wdn, Nst, Gst, H, pk, pkt, sw, rowsb, growsb, h1, h2, actw, ggu, yb, To, Tb, dsend,
               acc, b1, b2, zb, r0, s0, r1, s1, r2, s2, r3, s3, ar, asd, xr, xs, dr, ds_, lsem):
        net = Net(chips).enter()
        z, c, e = net.at[0], net.c, net.e
        me = e * 2 + c
        copies = [(wg_ref.at[i], wgu.at[i, :, pl.ds(0, Fh)]) for i in range(2)]
        copies += [(wu_ref.at[i], wgu.at[i, :, pl.ds(Fh, Fh)]) for i in range(2)]
        copies += [(wd_ref, wdn)]
        loads = [lambda s=s, d=d, i=i: pltpu.make_async_copy(s, d, lsem.at[i]) for i, (s, d) in enumerate(copies)]
        own = lambda: pltpu.make_async_copy(x_ref, N.at[e, pl.ds(pl.multiple_of(c * T, T), T)], lsem.at[6])
        own().start()
        acopy = lambda: pltpu.make_async_copy(a_ref, A.at[me], lsem.at[7])
        acopy().start()
        greet_all(net)
        own().wait()
        acopy().wait()
        ag = Gather22(net, N, T, xr, xs)
        rs = Reduce22(net, T, acc, b1, b2, zb, (r0, s0, r1, s1, r2, s2, r3, s3))
        done = []
        ag.begin()
        interleave(to_all(net, lambda t: a_ref, lambda s: A.at[s], lambda s: ar.at[s], lambda k: asd.at[k], done))
        for f in loads:
            f().start()
        lane = lax.broadcasted_iota(jnp.int32, (256, 256), 1)
        sub = lax.broadcasted_iota(jnp.int32, (256, 256), 0)
        U = jnp.where(jnp.logical_and(sub < lane, sub // 128 == lane // 128), 1.0, 0.0).astype(BF)
        eye = jnp.where(sub == lane, 1.0, 0.0).astype(BF)
        place = ((lax.broadcasted_iota(jnp.int32, (8, 256), 1) // 128) * cap).astype(F32)
        ag.from_z(slot_plane(z, 1))
        ag.from_two(z)
        for f in done:
            f()
        for f in loads:
            f().wait()

        saves = lambda i: [
            (rowsb, o_rows.at[:, i], 8), (growsb, o_grows.at[:, i], 9), (actw, o_act.at[:, i], 10), (ggu, o_ggu.at[:, i], 11)]

        def body(i, _):
            zt = slot_plane(z, i)
            zn = slot_plane(z, i + 1)
            zp = slot_plane(z, i - 1)
            pltpu.make_async_copy(g_ref.at[pl.ds(zt * 4, 4)], Gst, lsem.at[13]).start()
            ag.from_three(zt)
            ag.from_partner(zt)
            cpn = pltpu.make_async_copy(N.at[pl.ds(zt * 4, 4)], Nst, lsem.at[12])
            cpn.start()
            for ch in range(4):
                for ei in range(2):
                    for co in range(2):
                        H[2 * ch + ei:2 * ch + ei + 1, co * 128:(co + 1) * 128] = A[(zt * 4 + ch) * 2 + co, pl.ds(2 * e + ei, 1), :]
            h = H[...]
            here = jnp.where(h >= 0.0, 1.0, 0.0)
            slot = jnp.dot(here.astype(BF), U, preferred_element_type=F32) + place
            slot = jnp.where(here > 0.0, slot, -1.0)
            row_id = lax.broadcasted_iota(jnp.int32, (S2, 256), 0).astype(F32)
            for ch in range(4):
                for ei in range(2):
                    q = 2 * ch + ei
                    hit = row_id == slot[q:q + 1, :]
                    pk[ch, ei * S2:(ei + 1) * S2, :] = jnp.where(hit, 1.0, 0.0).astype(BF)
                    wcol = jnp.sum(jnp.where(hit, h[q:q + 1, :], 0.0), axis=1, keepdims=True)
                    sw[ei, ch * S2:(ch + 1) * S2, :] = jnp.broadcast_to(wcol, (S2, 128))
                pkt[ch] = lax.dot_general(eye, pk[ch], NT, preferred_element_type=F32).astype(BF)

            def before():
                for src, dst, s in saves(i):
                    pltpu.make_async_copy(src, dst, lsem.at[s]).wait()

            pl.when(i > 0)(before)
            cpn.wait()
            pltpu.make_async_copy(g_ref.at[pl.ds(zt * 4, 4)], Gst, lsem.at[13]).wait()

            def picks(k, _):
                ch, j = k // 2, k % 2
                cols = pl.ds(pl.multiple_of(j * (D // 2), D // 2), D // 2)
                at = pl.ds(pl.multiple_of(ch * S2, S2), S2)
                for st, dst in ((Nst, rowsb), (Gst, growsb)):
                    r = jnp.dot(pk[ch], st[ch, :, cols], preferred_element_type=F32).astype(BF)
                    dst[0, at, cols] = r[:S2]
                    dst[1, at, cols] = r[S2:]
                return 0

            lax.fori_loop(0, 8, picks, 0)
            pltpu.make_async_copy(rowsb, o_rows.at[:, i], lsem.at[8]).start()
            pltpu.make_async_copy(growsb, o_grows.at[:, i], lsem.at[9]).start()
            pl.when(i < 2)(lambda: ag.from_z(slot_plane(z, i + 2)))
            pl.when(i > 0)(lambda: rs.stage1(zp))

            for ei in range(2):
                h1[...] = jnp.dot(rowsb[ei], wgu[ei], preferred_element_type=F32)
                h2[...] = lax.dot_general(growsb[ei], wdn[ei], NT, preferred_element_type=F32)

                def point(k, _):
                    r = pl.ds(pl.multiple_of(k * PR, PR), PR)
                    gate, up, ga = h1[r, :Fh], h1[r, Fh:], h2[r, :]
                    w = sw[ei, r, 0:1]
                    sig = 1.0 / (1.0 + jnp.exp(-gate))
                    silu = gate * sig
                    act = silu * up
                    actw[ei, r, :] = (w * act).astype(BF)
                    sw[ei, r, :] = jnp.broadcast_to(jnp.sum(act * ga, axis=1, keepdims=True), (PR, 128))
                    gact = w * ga
                    ggu[ei, r, :Fh] = (gact * up * (sig + silu * (1.0 - sig))).astype(BF)
                    ggu[ei, r, Fh:] = (gact * silu).astype(BF)
                    return 0

                lax.fori_loop(0, M // PR, point, 0)
                for ch in range(4):
                    dcol = sw[ei, ch * S2:(ch + 1) * S2, 0:1]
                    dd = jnp.sum(pk[ch, ei * S2:(ei + 1) * S2, :].astype(F32) * dcol, axis=0, keepdims=True)
                    for co in range(2):
                        dsend[(zt * 4 + ch) * 2 + co, ei:ei + 1, :] = dd[:, co * 128:(co + 1) * 128]
                if ei == 0:
                    pl.when(i < 3)(lambda: ag.from_two(zn))
            pltpu.make_async_copy(actw, o_act.at[:, i], lsem.at[10]).start()
            pltpu.make_async_copy(ggu, o_ggu.at[:, i], lsem.at[11]).start()
            pl.when(i > 0)(lambda: rs.stage2(zp))

            def back(j, _):
                rws = pl.ds(pl.multiple_of(j * CW, CW), CW)
                for ei in range(2):
                    r = lax.dot_general(ggu[ei], wgu[ei, rws, :], NT, preferred_element_type=F32).astype(BF)
                    for ch in range(4):
                        yb[ch, ei * S2:(ei + 1) * S2, rws] = r[ch * S2:(ch + 1) * S2]
                return 0

            lax.fori_loop(0, D // CW, back, 0)
            for ab in rs.ring():
                ch = ab[0] * 2 + ab[1]

                def spread_back(j, _, ch=ch):
                    cols = pl.ds(pl.multiple_of(j * SW, SW), SW)
                    Tb[ch, :, cols] = jnp.dot(pkt[ch], yb[ch, :, cols], preferred_element_type=F32).astype(BF)
                    return 0

                lax.fori_loop(0, D // SW, spread_back, 0)
                rs.p_copy(Tb, zt, ab).start()

            def down(j, _):
                cols = pl.ds(pl.multiple_of(j * CW, CW), CW)
                for ei in range(2):
                    r = jnp.dot(actw[ei], wdn[ei, :, cols], preferred_element_type=F32).astype(BF)
                    for ch in range(4):
                        yb[ch, ei * S2:(ei + 1) * S2, cols] = r[ch * S2:(ch + 1) * S2]
                return 0

            lax.fori_loop(0, D // CW, down, 0)
            rs.stage0(Tb, zt)
            rs.p_wait_send(Tb, zt)
            for ch in range(4):
                cp = lambda ch=ch: pltpu.make_async_copy(To.at[ch % 2], o_part.at[zt * 4 + ch], lsem.at[14 + ch % 2])
                if ch >= 2:
                    cp().wait()

                def spread(j, _, ch=ch):
                    cols = pl.ds(pl.multiple_of(j * SW, SW), SW)
                    To[ch % 2, :, cols] = jnp.dot(pkt[ch], yb[ch, :, cols], preferred_element_type=F32).astype(BF)
                    return 0

                lax.fori_loop(0, D // SW, spread, 0)
                cp().start()
            for ch in (2, 3):
                pltpu.make_async_copy(To.at[ch % 2], o_part.at[zt * 4 + ch], lsem.at[14 + ch % 2]).wait()
            return 0

        lax.fori_loop(0, 4, body, 0)
        z3 = slot_plane(z, 3)
        last_done = []
        own_dots = pltpu.make_async_copy(dsend.at[me], o_dots.at[me], lsem.at[5])
        own_dots.start()
        interleave(to_all(net, lambda t: dsend.at[t], lambda s: o_dots.at[s], lambda s: dr.at[s], lambda k: ds_.at[k], last_done))
        rs.stage1(z3)
        rs.relay(slot_plane(z, 2))
        rs.stage2(z3)
        rs.relay(z3)
        rs.relay(slot_plane(z, 1))
        rs.last(o_sum)
        own_dots.wait()
        for f in last_done:
            f()
        for src, dst, s in saves(3):
            pltpu.make_async_copy(src, dst, lsem.at[s]).wait()

        def finish(i, _):
            ag.drain(i)
            rs.drain(slot_plane(z, i))
            return 0

        lax.fori_loop(0, 4, finish, 0)

    S = jax.ShapeDtypeStruct
    V = pltpu.VMEM
    return pl.pallas_call(
        kernel,
        out_shape=(S((T, D), BF), S((chips, 2 * T, D), BF), S((nd, 8, 128), F32), S((2, 4, M, D), BF), S((2, 4, M, D), BF),
                   S((2, 4, M, Fh), BF), S((2, 4, M, 2 * Fh), BF), S((chips, 2 * T, D), BF)),
        in_specs=[VM, VM, ANY, ANY, ANY, ANY], out_specs=(VM, ANY, VM, ANY, ANY, ANY, ANY, ANY),
        scratch_shapes=[
            V((nd, E, T), F32), V((2, D, 2 * Fh), BF), V((2, Fh, D), BF), V((4, 2 * T, D), BF), V((4, 2 * T, D), BF),
            V((8, 2 * T), F32), V((4, 2 * S2, 2 * T), BF), V((4, 2 * T, 2 * S2), BF), V((2, M, 128), F32), V((2, M, D), BF), V((2, M, D), BF),
            V((M, 2 * Fh), F32), V((M, Fh), F32), V((2, M, Fh), BF), V((2, M, 2 * Fh), BF), V((4, 2 * S2, D), BF),
            V((2, 2 * T, D), BF), V((4, 2 * T, D), BF), V((nd, 8, 128), F32)]
        + Reduce22.scratch(T, D)
        + [DMA((nd,)), DMA((nd,)), DMA((2, chips, 2)), DMA((2, chips, 5)), DMA((nd,)), DMA((nd,)), DMA((16,))],
        compiler_params=params(cid, 64 << 20), name="experts",
    )(x, marked, G, w_gate, w_up, w_down)[:7]


def column_sum_gather(n_expert, part, x, cid):
    _, _, T, D = part.shape

    def kernel(p_ref, x_ref, o_ref, N, acc, buf, fin, rsem, ssem, xr, xs, lsem):
        net = Net(n_expert).enter()
        z, e, c = net.at[0], net.e, net.c
        own = lambda: pltpu.make_async_copy(x_ref, N.at[e, pl.ds(pl.multiple_of(c * T, T), T)], lsem)
        own().start()
        greet(net, (0, 1, 2))
        own().wait()
        ag = Gather22(net, N, T, xr, xs)
        done = []

        def gather():
            ag.begin()
            yield
            for i in range(4):
                if i < 3:
                    ag.from_z(slot_plane(z, i + 1))
                    yield
                ag.from_two(slot_plane(z, i))
                yield
                if i:
                    ag.from_three(slot_plane(z, i - 1))
                    yield
            ag.from_three(slot_plane(z, 3))
            for i in range(4):
                ag.from_partner(slot_plane(z, i))

        interleave(
            col_rs(net, lambda s, h: p_ref.at[s, h], o_ref, lambda w, s, h: acc.at[w, s, h], lambda w, s, h: buf.at[w, s, h],
                   lambda i: fin.at[i], lambda w, s, h: rsem.at[w, s, h], lambda w, s, h: ssem.at[w, s, h], T, done),
            gather())
        for f in done:
            f()

        def finish(i, _):
            ag.drain(i)
            return 0

        lax.fori_loop(0, 4, finish, 0)

    S = jax.ShapeDtypeStruct
    V = pltpu.VMEM
    return pl.pallas_call(
        kernel, out_shape=(S((T, D), BF), S((n_expert, 2 * T, D), BF)), in_specs=[VM, VM], out_specs=(VM, ANY),
        scratch_shapes=[V((2, 2, 2, T, D), BF), V((2, 2, 2, T, D), BF), V((2, T, D), BF),
                        DMA((3, 2, 2)), DMA((3, 2, 2)), DMA((2, n_expert, 2)), DMA((2, n_expert, 5)), DMA],
        compiler_params=params(cid, 40 << 20), name="column_sum_gather",
    )(part, x)


def reduce_and_column(n_expert, part, x, cid):
    T, D = x.shape

    def kernel(p_ref, x_ref, o_ref, X, Tb, acc, b1, b2, zb, r0, s0, r1, s1, r2, s2, r3, s3, xr, xs, lsem):
        net = Net(n_expert).enter()
        z = net.at[0]
        load = lambda i: pltpu.make_async_copy(p_ref.at[pl.ds(slot_plane(z, 3 - i) * 4, 4)], Tb.at[i % 2], lsem.at[i % 2])
        load(0).start()
        greet(net, (0, 1, 2))
        rs = Reduce22(net, T, acc, b1, b2, zb, (r0, s0, r1, s1, r2, s2, r3, s3))
        done = []
        far = lambda i: slot_plane(z, 3 - i)

        def reduce():
            for i in range(4):
                if i:
                    rs.p_wait_send(Tb.at[(i - 1) % 2], far(i - 1))
                if i < 3:
                    load(i + 1).start()
                load(i).wait()
                rs.p_send(Tb.at[i % 2], far(i))
                yield
                rs.stage0(Tb.at[i % 2], far(i))
                yield
                if i:
                    rs.stage1(far(i - 1))
                    yield
                if i > 1:
                    rs.stage2(far(i - 2))
                    yield
            rs.p_wait_send(Tb.at[1], far(3))
            rs.stage1(far(3))
            rs.stage2(far(2))
            yield
            for i in (0, 1, 2):
                rs.relay(far(i))
            rs.stage2(far(3))
            rs.last(o_ref)

        interleave(
            reduce(),
            col_ag(net, x_ref, lambda s, h: X.at[s, h], lambda s, h: xr.at[s, h], lambda w, s, h: xs.at[w, s, h], done))
        for f in done:
            f()

        def finish(i, _):
            rs.drain(slot_plane(z, i))
            return 0

        lax.fori_loop(0, 4, finish, 0)

    S = jax.ShapeDtypeStruct
    return pl.pallas_call(
        kernel, out_shape=(S((T, D), BF), S((2, 2, T, D), BF)), in_specs=[ANY, VM], out_specs=(VM, ANY),
        scratch_shapes=[pltpu.VMEM((2, 4, 2 * T, D), BF)] + Reduce22.scratch(T, D) + [DMA((2, 2)), DMA((3, 2, 2)), DMA((2,))],
        compiler_params=params(cid, 60 << 20), name="reduce_and_column",
    )(part, x)


def head_rotated(v, gain, cos, sin):
    inv = lax.rsqrt(jnp.mean(v * v, axis=-1, keepdims=True) + epsilon)
    n = v * inv * gain
    return n * cos + pltpu.roll(n, HEAD_SIZE // 2, 1) * sin, inv


def head_back(v, gain, cos, sin, grad):
    inv = lax.rsqrt(jnp.mean(v * v, axis=-1, keepdims=True) + epsilon)
    g = grad * cos - pltpu.roll(grad, HEAD_SIZE // 2, 1) * sin
    s = g * gain
    return inv * (s - v * (inv * inv * jnp.mean(s * v, axis=-1, keepdims=True))), g * v * inv


def softmax_rows(q, k, allowed):
    s = lax.dot_general(q, k, NT, preferred_element_type=F32) * (HEAD_SIZE ** -0.5)
    s = jnp.where(allowed > 0.0, s, -1e30)
    ex = jnp.exp(s - jnp.max(s, axis=-1, keepdims=True))
    return ex * (1.0 / jnp.sum(ex, axis=-1, keepdims=True))


def attention_forward(n_expert, X, W, O, gain, gq, gk, cos, sin, allowed, cot, cid):
    T, D = cot.shape
    L = 2 * T
    rows = 2 * L
    GQ = O.shape[0]
    heads = GQ // HEAD_SIZE
    C = W.shape[1]
    HS = HEAD_SIZE

    def kernel(X_ref, W_ref, O_ref, gain_ref, gq_ref, gk_ref, cos_ref, sin_ref, ok_ref, x_ref,
               o_ref, N, first, raw, qs, ks, vs, att, part, acc, buf, fin, rsem, ssem, xr, xs, lsem):
        net = Net(n_expert).enter()
        z, e, c = net.at[0], net.e, net.c
        own = lambda: pltpu.make_async_copy(x_ref, N.at[e, pl.ds(pl.multiple_of(c * T, T), T)], lsem)
        own().start()
        greet(net, (0, 1, 2))
        own().wait()
        ag = Gather22(net, N, T, xr, xs)
        done = []

        def gather():
            ag.begin()
            yield
            for i in range(4):
                if i < 3:
                    ag.from_z(slot_plane(z, i + 1))
                    yield
                ag.from_two(slot_plane(z, i))
                yield
                if i:
                    ag.from_three(slot_plane(z, i - 1))
                    yield
            ag.from_three(slot_plane(z, 3))
            for i in range(4):
                ag.from_partner(slot_plane(z, i))

        def compute():
            def norm(i, _):
                r = pl.ds(pl.multiple_of(i * 32, 32), 32)
                x = X_ref[r, :].astype(F32)
                inv = lax.rsqrt(jnp.mean(x * x, axis=-1, keepdims=True) + epsilon)
                first[r, :] = (x * inv * gain_ref[...]).astype(BF)
                return 0

            lax.fori_loop(0, rows // 32, norm, 0)

            def project(j, _):
                cols = pl.ds(pl.multiple_of(j * 256, 256), 256)
                raw[:, cols] = jnp.dot(first[...], W_ref[:, cols], preferred_element_type=F32)
                return 0

            lax.fori_loop(0, 2, project, 0)
            yield
            lax.fori_loop(2, C // 256, project, 0)
            yield
            for s in range(2):
                r = slice(s * L, (s + 1) * L)
                k, _ = head_rotated(raw[r, GQ:GQ + HS], gk_ref[...], cos_ref[...], sin_ref[...])
                ks[r, :] = k.astype(BF)
                vs[r, :] = raw[r, GQ + HS:].astype(BF)
            for s in range(2):
                r = pl.ds(s * L, L)

                def one_head(h, _):
                    cols = pl.ds(pl.multiple_of(h * HS, HS), HS)
                    q, _ = head_rotated(raw[r, cols], gq_ref[...], cos_ref[...], sin_ref[...])
                    q = q.astype(BF)
                    qs[r, cols] = q
                    p = softmax_rows(q, ks[r, :], ok_ref[s]).astype(BF)
                    att[r, cols] = jnp.dot(p, vs[r, :], preferred_element_type=F32).astype(BF)
                    return 0

                for g in range(2):
                    lax.fori_loop(g * heads // 2, (g + 1) * heads // 2, one_head, 0)
                    yield

            def project_out(j, _):
                cols = pl.ds(pl.multiple_of(j * 512, 512), 512)
                part[:, cols] = jnp.dot(att[...], O_ref[:, cols], preferred_element_type=F32).astype(BF)
                return 0

            lax.fori_loop(0, D // 512, project_out, 0)
            yield
            yield from col_rs(
                net, lambda s, h: part.at[pl.ds(s * L + h * T, T)], o_ref, lambda w, s, h: acc.at[w, s, h],
                lambda w, s, h: buf.at[w, s, h], lambda i: fin.at[i], lambda w, s, h: rsem.at[w, s, h],
                lambda w, s, h: ssem.at[w, s, h], T, done)

        interleave(gather(), compute())
        for f in done:
            f()

        def finish(i, _):
            ag.drain(i)
            return 0

        lax.fori_loop(0, 4, finish, 0)

    S = jax.ShapeDtypeStruct
    V = pltpu.VMEM
    return pl.pallas_call(
        kernel,
        out_shape=(S((T, D), BF), S((n_expert, 2 * T, D), BF), S((rows, D), BF), S((rows, C), F32), S((rows, GQ), BF),
                   S((rows, HS), BF), S((rows, HS), BF), S((rows, GQ), BF)),
        in_specs=[VM] * 10, out_specs=(VM, ANY, VM, VM, VM, VM, VM, VM),
        scratch_shapes=[V((rows, D), BF), V((2, 2, 2, T, D), BF), V((2, 2, 2, T, D), BF), V((2, T, D), BF),
                        DMA((3, 2, 2)), DMA((3, 2, 2)), DMA((2, n_expert, 2)), DMA((2, n_expert, 5)), DMA],
        compiler_params=params(cid, 60 << 20), name="attention_forward",
    )(X, W, O, gain, gq, gk, cos, sin, allowed, cot)


def attention_backward(n_expert, out_part, gx, X, first, raw, qs, ks, vs, att, W, O, gain, gq, gk, cos, sin, allowed, cid):
    T, D = gx.shape
    L = 2 * T
    rows = 2 * L
    GQ = O.shape[0]
    heads = GQ // HEAD_SIZE
    C = W.shape[1]
    HS = HEAD_SIZE
    scale = HS ** -0.5

    def kernel(p_ref, gx_ref, X_ref, first, raw, qs, ks, vs, att, W_ref, O_ref, gain_ref, gq_ref, gk_ref, cos_ref, sin_ref, ok_ref,
               o_ref, dX, dW, dO, ga_out, gq_out, gk_out,
               GA, gatt, graw, dk, dv, invc, Tb, acc, b1, b2, zb, r0, s0, r1, s1, r2, s2, r3, s3, xr, xs, lsem):
        net = Net(n_expert).enter()
        z = net.at[0]
        far = lambda i: slot_plane(z, 3 - i)
        load = lambda i: pltpu.make_async_copy(p_ref.at[pl.ds(far(i) * 4, 4)], Tb, lsem)
        load(0).start()
        greet(net, (0, 1, 2))
        rs = Reduce22(net, T, acc, b1, b2, zb, (r0, s0, r1, s1, r2, s2, r3, s3))
        lane = lax.broadcasted_iota(jnp.int32, (256, 256), 1)
        sub = lax.broadcasted_iota(jnp.int32, (256, 256), 0)
        eye = jnp.where(sub == lane, 1.0, 0.0).astype(BF)

        def flip(v):
            return lax.dot_general(eye[:v.shape[1], :v.shape[1]], v, NT, preferred_element_type=F32).astype(BF)

        def reduce():
            for i in range(4):
                load(i).wait()
                rs.p_send(Tb, far(i))
                yield
                rs.stage0(Tb, far(i))
                rs.p_wait_send(Tb, far(i))
                if i < 3:
                    load(i + 1).start()
                yield
                if i:
                    rs.stage1(far(i - 1))
                    yield
                if i > 1:
                    rs.stage2(far(i - 2))
                    yield
            rs.stage1(far(3))
            yield
            rs.stage2(far(2))
            yield
            for i in (0, 1, 2):
                rs.relay(far(i))
                yield
            rs.stage2(far(3))
            yield
            rs.last(o_ref)

        def compute():
            done = []
            place = lambda s, h: GA.at[pl.ds(pl.multiple_of(s * L + h * T, T), T)]
            yield from col_ag(net, gx_ref, place, lambda s, h: xr.at[s, h], lambda w, s, h: xs.at[w, s, h], done)
            for f in done:
                f()

            def grad_att(j, _):
                cols = pl.ds(pl.multiple_of(j * 256, 256), 256)
                gatt[:, cols] = lax.dot_general(GA[...], O_ref[cols, :], NT, preferred_element_type=F32).astype(BF)
                return 0

            lax.fori_loop(0, GQ // 256, grad_att, 0)
            yield
            gq_out[...] = jnp.zeros_like(gq_out)
            gk_out[...] = jnp.zeros_like(gk_out)

            def inverse(i, _):
                r = pl.ds(pl.multiple_of(i * 32, 32), 32)
                x = X_ref[r, :].astype(F32)
                inv = lax.rsqrt(jnp.mean(x * x, axis=-1, keepdims=True) + epsilon)
                invc[r, :] = jnp.broadcast_to(inv, (32, 128))
                return 0

            lax.fori_loop(0, rows // 32, inverse, 0)
            for s in range(2):
                r = pl.ds(s * L, L)
                dk[...] = jnp.zeros_like(dk)
                dv[...] = jnp.zeros_like(dv)

                def one_head(h, _):
                    cols = pl.ds(pl.multiple_of(h * HS, HS), HS)
                    q, k, v, g = qs[r, cols], ks[r, :], vs[r, :], gatt[r, cols]
                    p = softmax_rows(q, k, ok_ref[s])
                    dp = lax.dot_general(g, v, NT, preferred_element_type=F32)
                    ds = (p * (dp - jnp.sum(p * dp, axis=-1, keepdims=True))).astype(BF)
                    dv[...] += jnp.dot(flip(p.astype(BF)), g, preferred_element_type=F32)
                    dk[...] += jnp.dot(flip(ds), q, preferred_element_type=F32)
                    dq = jnp.dot(ds, k, preferred_element_type=F32) * scale
                    gr, terms = head_back(raw[r, cols], gq_ref[...], cos_ref[...], sin_ref[...], dq)
                    graw[r, cols] = gr.astype(BF)
                    gq_out[...] += jnp.sum(terms, axis=0, keepdims=True)
                    return 0

                for g in range(2):
                    lax.fori_loop(g * heads // 2, (g + 1) * heads // 2, one_head, 0)
                    yield
                gr, terms = head_back(raw[r, GQ:GQ + HS], gk_ref[...], cos_ref[...], sin_ref[...], dk[...] * scale)
                graw[r, GQ:GQ + HS] = gr.astype(BF)
                gk_out[...] += jnp.sum(terms, axis=0, keepdims=True)
                graw[r, GQ + HS:] = dv[...].astype(BF)

            def grad_o(h, _):
                cols = pl.ds(pl.multiple_of(h * HS, HS), HS)
                aT = flip(att[:, cols])
                for j in range(2):
                    w = slice(j * (D // 2), (j + 1) * (D // 2))
                    dO[cols, w] = jnp.dot(aT, GA[:, w], preferred_element_type=F32).astype(BF)
                return 0

            lax.fori_loop(0, heads, grad_o, 0)
            yield

            def grad_x(j, _):
                cols = pl.ds(pl.multiple_of(j * 256, 256), 256)
                dx = lax.dot_general(graw[...], W_ref[cols, :], NT, preferred_element_type=F32)
                dX[:, cols] = dx.astype(BF)
                ga_out[:, cols] = jnp.sum(dx * X_ref[:, cols].astype(F32) * invc[:, 0:1], axis=0, keepdims=True)
                return 0

            for g in range(2):
                lax.fori_loop(g * D // 512, (g + 1) * D // 512, grad_x, 0)
                yield

            def grad_w(j, _):
                cols = pl.ds(pl.multiple_of(j * 256, 256), 256)
                dW[cols, :] = jnp.dot(flip(first[:, cols]), graw[...], preferred_element_type=F32).astype(BF)
                return 0

            for g in range(2):
                lax.fori_loop(g * D // 512, (g + 1) * D // 512, grad_w, 0)
                yield

        interleave(reduce(), compute())

        def finish(i, _):
            rs.drain(slot_plane(z, i))
            return 0

        lax.fori_loop(0, 4, finish, 0)

    S = jax.ShapeDtypeStruct
    V = pltpu.VMEM
    return pl.pallas_call(
        kernel,
        out_shape=(S((T, D), BF), S((rows, D), BF), S((D, C), BF), S((GQ, D), BF), S((1, D), F32), S((1, HS), F32), S((1, HS), F32)),
        in_specs=[ANY] + [VM] * 16, out_specs=(VM,) * 7,
        scratch_shapes=[V((rows, D), BF), V((rows, GQ), BF), V((rows, C), BF), V((L, HS), F32), V((L, HS), F32), V((rows, 128), F32),
                        V((4, 2 * T, D), BF)] + Reduce22.scratch(T, D) + [DMA((2, 2)), DMA((3, 2, 2)), DMA],
        compiler_params=params(cid, 64 << 20), name="attention_backward",
    )(out_part, gx, X, first, raw, qs, ks, vs, att, W, O, gain, gq, gk, cos, sin, allowed)


MODEL_WIDTH = 2048
QUERY_HEADS = 32
KEY_VALUE_HEADS = 4
HEAD_SIZE = 128
GROUP = QUERY_HEADS // KEY_VALUE_HEADS
TOP = 8
EXP_DEV = 2

epsilon = 1e-06
rope_base = 1000000.0


def norm_parts(values_in, gain_vec):
    inverse = lax.rsqrt(jnp.mean(values_in * values_in, axis=-1, keepdims=True) + epsilon)
    return (values_in * inverse * gain_vec, inverse)


def norm_back(values_in, inverse, gain_vec, grad_out):
    scaled = grad_out * gain_vec
    grad_in = inverse * (
        scaled
        - values_in * inverse * inverse * jnp.mean(scaled * values_in, axis=-1, keepdims=True)
    )
    return (grad_in, grad_out * values_in * inverse)


def rope_tables(positions):
    exponent = jnp.arange(HEAD_SIZE // 2).astype(F32) * (2.0 / HEAD_SIZE)
    frequency = jnp.exp(-math.log(rope_base) * exponent)
    angles = positions.astype(F32)[:, None] * frequency[None, :]
    return (jnp.cos(angles), jnp.sin(angles))


def rotate(v, cos, sin):
    half = v.shape[-1] // 2
    a, b = v[..., :half], v[..., half:]
    return jnp.concatenate([a * cos - b * sin, b * cos + a * sin], axis=-1)


def rotate_back(v, cos, sin):
    half = v.shape[-1] // 2
    a, b = v[..., :half], v[..., half:]
    return jnp.concatenate([a * cos + b * sin, b * cos - a * sin], axis=-1)


def mm(a, b):
    return jnp.dot(a, b, preferred_element_type=F32)


def ein(spec, *args):
    return jnp.einsum(spec, *args, preferred_element_type=F32)


def experts_wide(n_expert, second_in, marked, G, w_gate, w_up, w_down, capacity):
    T, D = second_in.shape
    nd = 2 * n_expert
    e = lax.axis_index("expert")
    N, M = gather_all(n_expert, second_in, marked, 2)

    mine = lax.dynamic_slice(M, (0, EXP_DEV * e, 0), (nd, EXP_DEV, T))
    here = mine >= 0.0
    rank = jnp.cumsum(here.astype(jnp.int32), axis=-1) - 1
    slots = jnp.arange(capacity, dtype=jnp.int32)
    pick = here[:, :, None, :] & (rank[:, :, None, :] == slots[None, None, :, None])
    slot_weight = jnp.sum(jnp.where(pick, mine[:, :, None, :], 0.0), axis=-1).transpose(1, 0, 2)[..., None]
    pick = pick.astype(BF)
    N = N.reshape(nd, T, D)
    G = G.reshape(nd, T, D)
    rows = ein("sect,std->escd", pick, N).astype(BF)
    g_rows = ein("sect,std->escd", pick, G)
    flat = lambda v: v.reshape(EXP_DEV, nd * capacity, v.shape[-1])
    deep = lambda v: v.reshape(EXP_DEV, nd, capacity, v.shape[-1])
    rows = flat(rows)
    grad_rows = flat((slot_weight * g_rows).astype(BF))
    gate_value = ein("emd,edf->emf", rows, w_gate)
    up_value = ein("emd,edf->emf", rows, w_up)
    sig = jax.nn.sigmoid(gate_value)
    act = (gate_value * sig * up_value).astype(BF)
    expert_part = deep(ein("emf,efd->emd", act, w_down))
    dots = jnp.sum(g_rows * expert_part, axis=-1)
    out_part = ein("sect,escd->std", pick, (slot_weight * expert_part).astype(BF)).astype(BF)
    dots = ein("sect,esc->set", pick.astype(F32), dots)
    grad_act = ein("emd,efd->emf", grad_rows, w_down)
    grad_gate_v = (grad_act * up_value * sig * (1.0 + gate_value * (1.0 - sig))).astype(BF)
    grad_up_v = (grad_act * gate_value * sig).astype(BF)
    down_grad = ein("emf,emd->efd", act, grad_rows)
    gate_grad = ein("emd,emf->edf", rows, grad_gate_v)
    up_grad = ein("emd,emf->edf", rows, grad_up_v)
    back_rows = ein("emf,edf->emd", grad_gate_v, w_gate) + ein("emf,edf->emd", grad_up_v, w_up)
    back_part = ein("sect,escd->std", pick, deep(back_rows.astype(BF))).astype(BF)

    dots_out = jnp.pad(dots, ((0, 0), (0, 8 - EXP_DEV), (0, 0)))
    dots_in = exchange(n_expert, dots_out, 3)
    parts = max(1, n_expert // 16)
    cols = D // parts

    def summed(v, cid):
        v = v.reshape(n_expert, 2, T, D)
        part = lambda i: reduce_scatter_all(n_expert, lax.dynamic_slice_in_dim(v, i * cols, cols, axis=3), cid)
        return lax.map(part, jnp.arange(parts)).transpose(1, 0, 2).reshape(T, D)

    back_sum, out_sum = summed(back_part, 4), summed(out_part, 5)
    return back_sum, out_sum, dots_in, gate_grad, up_grad, down_grad


def local(
    n_expert, tokens, routes, documents, w_query, key_projection, value_projection, w_out, w_router,
    gain_attn, gain_ffn, gain_query, gain_key, w_gate, w_up, w_down, cotangent,
):
    Z = KEY_VALUE_HEADS
    plane = n_expert // Z
    nd = 2 * n_expert
    T, D = tokens.shape
    R, HR, E = w_query.shape[0], w_out.shape[0], w_router.shape[1]
    Q = gain_query.shape[0]
    KV = HEAD_SIZE
    GQ = GROUP * HEAD_SIZE
    e, c = lax.axis_index("expert"), lax.axis_index("context")
    z, p = e // plane, e % plane
    capacity = T * TOP * 5 // (4 * E)
    score_scale = HEAD_SIZE ** (-0.5)

    wqkv = jnp.concatenate(
        [w_query.reshape(R, Z, GQ), key_projection.reshape(R, Z, KV), value_projection.reshape(R, Z, KV)], axis=-1
    ).transpose(1, 0, 2)
    width = -(-(E + 4) // 128) * 128
    pad = lambda v: jnp.pad(v, (0, R - v.shape[0]))[:, None]
    head = jnp.concatenate(
        [w_router, gain_attn[:, None], gain_ffn[:, None], pad(gain_query), pad(gain_key), jnp.zeros((R, width - E - 4), BF)], axis=1
    )
    docs_own = lax.dynamic_slice_in_dim(documents[0], c * T, T).astype(BF)[None]
    docs_own = jnp.pad(docs_own, ((0, 15), (0, width - T)))
    aux = jnp.concatenate([head, docs_own], axis=0)
    small_plane = plane == 4
    X, W, O, A, *G = gather_start(n_expert, tokens, wqkv, w_out, aux, None if small_plane else cotangent, 0)
    W = W.reshape(D, GQ + 2 * KV)
    O = O.reshape(GQ, D)
    table = A[:, :R].reshape(D, width)
    router_weight = table[:, :E]
    attn_gain = table[:, E].astype(F32)
    ffn_gain = table[:, E + 1].astype(F32)
    query_gain = A[:, :Q, E + 2].reshape(HEAD_SIZE).astype(F32)
    key_gain = A[:, :Q, E + 3].reshape(HEAD_SIZE).astype(F32)
    docs = A[:, R, :T].reshape(Z, plane, 2 * T)
    docs = lax.dynamic_slice(docs, (2 * c, p, 0), (2, 1, 2 * T)).reshape(2, 2 * T)

    L = 2 * T
    places = jnp.arange(L, dtype=jnp.int32)
    cos, sin = rope_tables(places)
    qcos, qsin = cos[:, None, :], sin[:, None, :]
    allowed = (places[:, None] >= places[None, :])[None] & (docs[:, :, None] == docs[:, None, :])
    if small_plane:
        cos2 = jnp.concatenate([cos, cos], axis=1)
        sin2 = jnp.concatenate([-sin, sin], axis=1)
        attn_sum, G, first_in, raw, queries, keys, value, attended = attention_forward(
            n_expert, X.reshape(2 * L, D), W, O, attn_gain[None], query_gain[None], key_gain[None], cos2, sin2,
            allowed.astype(F32), cotangent, 1)
    else:
        x = X.reshape(2 * L, D).astype(F32)
        normed, inverse_attn = norm_parts(x, attn_gain)
        first_in = normed.astype(BF)
        raw = mm(first_in, W)
        query_raw = raw[:, :GQ].reshape(2, L, GROUP, HEAD_SIZE)
        key_raw = raw[:, GQ:GQ + KV].reshape(2, L, HEAD_SIZE)
        value = raw[:, GQ + KV:].reshape(2, L, HEAD_SIZE).astype(BF)
        query_normed, query_inverse = norm_parts(query_raw, query_gain)
        key_normed, key_inverse = norm_parts(key_raw, key_gain)
        queries = rotate(query_normed, qcos, qsin).astype(BF)
        keys = rotate(key_normed, cos, sin).astype(BF)
        scores = ein("sqhd,skd->shqk", queries, keys) * score_scale
        scores = jnp.where(allowed[:, None], scores, -1e30)
        top = jnp.max(scores, axis=-1, keepdims=True)
        ex = jnp.exp(scores - top)
        probs = ex / jnp.sum(ex, axis=-1, keepdims=True)
        probs_low = probs.astype(BF)
        attended = ein("shqk,skd->sqhd", probs_low, value).reshape(2 * L, GQ).astype(BF)
        part = mm(attended, O).astype(BF).reshape(2, 2, T, D)
        attn_sum, G = column_sum(n_expert, part, 1), G[0]
    middle = tokens.astype(F32) + attn_sum.astype(F32)

    normed_ffn, inverse_ffn = norm_parts(middle, ffn_gain)
    second_in = normed_ffn.astype(BF)
    logits = mm(second_in, router_weight)
    ids = jnp.arange(E, dtype=jnp.int32)
    chosen = jnp.any(routes[:, :, None] == ids[None, None, :], axis=1)
    masked = jnp.where(chosen, logits, -jnp.inf)
    best = jnp.max(masked, axis=-1, keepdims=True)
    ew = jnp.where(chosen, jnp.exp(logits - best), 0.0)
    weights = ew / jnp.sum(ew, axis=-1, keepdims=True)
    marked = jnp.where(chosen, weights, -1.0).T
    if small_plane:
        back_sum, out_part, dots_in, rows, g_rows, act_w, gate_up = experts_fused(
            second_in, marked, G, w_gate, w_up, w_down, capacity, 3)
        flat = lambda v: v.reshape(EXP_DEV, -1, v.shape[-1])
        Fh = act_w.shape[-1]
        rows = flat(rows)
        down_grad = ein("emf,emd->efd", flat(act_w), flat(g_rows))
        gate_grad = ein("emd,emf->edf", rows, flat(gate_up[..., :Fh]))
        up_grad = ein("emd,emf->edf", rows, flat(gate_up[..., Fh:]))
    else:
        back_sum, out_sum, dots_in, gate_grad, up_grad, down_grad = experts_wide(
            n_expert, second_in, marked, G, w_gate, w_up, w_down, capacity)
    back_sum = back_sum.astype(F32)

    grad_result = cotangent.astype(F32)
    grad_weights = jnp.sum(dots_in[:, :EXP_DEV].reshape(n_expert, 2, EXP_DEV, T), axis=1).reshape(E, T).T
    grad_chosen = weights * (grad_weights - jnp.sum(weights * grad_weights, axis=-1, keepdims=True))
    grad_logits = jnp.where(chosen, grad_chosen, 0.0).astype(BF)
    router_grad = mm(second_in.T, grad_logits)
    grad_second = mm(grad_logits, router_weight.T) + back_sum
    grad_middle_norm, ffn_terms = norm_back(middle, inverse_ffn, ffn_gain, grad_second)
    ffn_gain_grad = jnp.sum(ffn_terms, axis=0)
    grad_middle = grad_result + grad_middle_norm

    if small_plane:
        out_sum, grad_first, raw_grad, out_grad, attn_gain_grad, query_gain_grad, key_gain_grad = attention_backward(
            n_expert, out_part, grad_middle.astype(BF), X.reshape(2 * L, D), first_in, raw, queries, keys, value, attended, W, O,
            attn_gain[None], query_gain[None], key_gain[None], cos2, sin2, allowed.astype(F32), 6)
        attn_gain_grad, query_gain_grad, key_gain_grad = attn_gain_grad[0], query_gain_grad[0], key_gain_grad[0]
    else:
        GA = column_gather(n_expert, grad_middle.astype(BF), 6)
        GA = GA.reshape(2 * L, D)
        out_grad = mm(attended.T, GA)
        grad_attended = ein("td,fd->tf", GA, O).astype(BF).reshape(2, L, GROUP, HEAD_SIZE)
        grad_probs = ein("sqhd,skd->shqk", grad_attended, value)
        grad_scores = (probs * (grad_probs - jnp.sum(probs * grad_probs, axis=-1, keepdims=True))).astype(BF)
        grad_queries = ein("shqk,skd->sqhd", grad_scores, keys) * score_scale
        grad_keys = ein("shqk,sqhd->skd", grad_scores, queries) * score_scale
        grad_values = ein("shqk,sqhd->skd", probs_low, grad_attended)
        grad_query_raw, query_terms = norm_back(query_raw, query_inverse, query_gain, rotate_back(grad_queries, qcos, qsin))
        grad_key_raw, key_terms = norm_back(key_raw, key_inverse, key_gain, rotate_back(grad_keys, cos, sin))
        grad_raw = jnp.concatenate(
            [grad_query_raw.reshape(2 * L, GQ).astype(BF), grad_key_raw.reshape(2 * L, KV).astype(BF),
             grad_values.reshape(2 * L, KV).astype(BF)], axis=-1)
        query_gain_grad = jnp.sum(query_terms, axis=(0, 1, 2))
        key_gain_grad = jnp.sum(key_terms, axis=(0, 1))
        grad_first = ein("tf,df->td", grad_raw, W)
        raw_grad = mm(first_in.T, grad_raw)
        attn_gain_grad = jnp.sum(grad_first * x * inverse_attn, axis=0)
    block_out = (middle + out_sum.astype(F32)).astype(BF)

    small = jnp.concatenate([
        router_grad.reshape(nd, R * E), attn_gain_grad.reshape(nd, R), ffn_gain_grad.reshape(nd, R),
        query_gain_grad.reshape(nd, Q), key_gain_grad.reshape(nd, Q)], axis=1)
    n_small = small.shape[1]
    small = jnp.pad(small, ((0, 0), (0, -n_small % 1024))).reshape(nd, -1, 128)
    grad_first_sum, raw_sum, out_sum2, small_in = reduce_end(
        n_expert, grad_first.astype(BF).reshape(2, 2, T, D), raw_grad.astype(BF).reshape(Z, plane, 2, R, GQ + 2 * KV),
        out_grad.astype(BF).reshape(plane, 2, HR, D), small, 7)
    small_sum = jnp.sum(small_in, axis=0).reshape(-1)
    router_grad = small_sum[:R * E].reshape(R, E)
    attn_gain_grad = small_sum[R * E:R * E + R]
    ffn_gain_grad = small_sum[R * E + R:R * E + 2 * R]
    query_gain_grad = small_sum[R * E + 2 * R:R * E + 2 * R + Q]
    key_gain_grad = small_sum[R * E + 2 * R + Q:n_small]
    raw_sum = raw_sum.astype(F32)
    query_grad = raw_sum[:, :, :GQ].transpose(1, 0, 2).reshape(R, QUERY_HEADS * HEAD_SIZE)
    key_grad = raw_sum[:, :, GQ:GQ + KV].transpose(1, 0, 2).reshape(R, Z * KV)
    value_grad = raw_sum[:, :, GQ + KV:].transpose(1, 0, 2).reshape(R, Z * KV)

    own = tokens.astype(F32)
    inverse_own = lax.rsqrt(jnp.mean(own * own, axis=-1, keepdims=True) + epsilon)
    grad_in, _ = norm_back(own, inverse_own, attn_gain, grad_first_sum.astype(F32))
    grad_tokens = grad_middle + grad_in
    return (
        block_out, grad_tokens, query_grad, key_grad, value_grad, out_sum2.astype(F32), router_grad,
        attn_gain_grad, ffn_gain_grad, query_gain_grad, key_gain_grad, gate_grad, up_grad, down_grad,
    )


def solution(mesh):
    row = P(("expert", "context"), None)
    vec = P(("expert", "context"))
    hidden = P("expert", None, "context")
    return jax.shard_map(
        functools.partial(local, mesh.shape["expert"]),
        mesh=mesh,
        in_specs=(row, row, P("expert", None), row, row, row, row, row, vec, vec, vec, vec, hidden, hidden,
                  P("expert", "context", None), row),
        out_specs=(row, row, row, row, row, row, row, vec, vec, vec, vec, hidden, hidden, P("expert", "context", None)),
        check_vma=False,
    )
```

```python
import functools
import math

import jax
import jax.numpy as jnp
from jax import lax
from jax.experimental import pallas as pl
from jax.experimental.pallas import tpu as pltpu
from jax.sharding import PartitionSpec as P

MESH_ID = pl.DeviceIdType.MESH
BF = jnp.bfloat16
F32 = jnp.float32


class Net:
    def __init__(self, n_expert):
        side = math.isqrt(n_expert // 4)
        self.dims = (4, side, side)
        self.chips = n_expert

    def enter(self):
        e = lax.axis_index("expert")
        _, A, B = self.dims
        self.e = e
        self.at = (e // (A * B), (e // B) % A, e % B)
        self.c = lax.axis_index("context")
        return self

    def chip(self, at):
        _, A, B = self.dims
        return (at[0] * A + at[1]) * B + at[2]

    def moved(self, axis, to):
        at = list(self.at)
        at[axis] = to
        return tuple(at)

    def near(self, axis):
        n, p = self.dims[axis], self.at[axis]
        if n == 2:
            return [(None, 1 - p)]
        return [(p < n - 1, p + 1), (p > 0, p - 1)]


def when(cond, fn):
    if cond is None:
        fn()
    else:
        pl.when(cond)(fn)


def rcopy(src, dst, ss, rs, dev):
    return pltpu.make_async_remote_copy(
        src_ref=src, dst_ref=dst, send_sem=ss, recv_sem=rs, device_id=dev, device_id_type=MESH_ID
    )


def greet(net, axes, partner=True):
    bar = pltpu.get_barrier_semaphore()
    count = 0
    for axis in axes:
        for cond, to in net.near(axis):
            dev = (net.chip(net.moved(axis, to)), net.c)
            when(cond, lambda dev=dev: pl.semaphore_signal(bar, inc=1, device_id=dev, device_id_type=MESH_ID))
            count = count + (1 if cond is None else jnp.where(cond, 1, 0))
    if partner:
        pl.semaphore_signal(bar, inc=1, device_id=(net.e, 1 - net.c), device_id_type=MESH_ID)
        count = count + 1
    pl.semaphore_wait(bar, count)


def greet_column(net):
    bar = pltpu.get_barrier_semaphore()
    n, z = net.dims[0], net.at[0]
    for k in range(1, n):
        dev = (net.chip(net.moved(0, (z + k) % n)), net.c)
        pl.semaphore_signal(bar, inc=1, device_id=dev, device_id_type=MESH_ID)
    count = n - 1
    for axis in (1, 2):
        for cond, to in net.near(axis):
            dev = (net.chip(net.moved(axis, to)), net.c)
            when(cond, lambda dev=dev: pl.semaphore_signal(bar, inc=1, device_id=dev, device_id_type=MESH_ID))
            count = count + (1 if cond is None else jnp.where(cond, 1, 0))
    pl.semaphore_signal(bar, inc=1, device_id=(net.e, 1 - net.c), device_id_type=MESH_ID)
    pl.semaphore_wait(bar, count + 1)


def greet_all(net):
    bar = pltpu.get_barrier_semaphore()
    total = net.chips * 2
    me = net.e * 2 + net.c

    def body(k, _):
        t = (me + k) % total
        pl.semaphore_signal(bar, inc=1, device_id=(t // 2, t % 2), device_id_type=MESH_ID)
        return 0

    lax.fori_loop(1, total, body, 0)
    pl.semaphore_wait(bar, total - 1)


def interleave(*gens, steps=None):
    left = [(g, steps[i] if steps else 1) for i, g in enumerate(gens)]
    while left:
        for item in list(left):
            try:
                for _ in range(item[1]):
                    next(item[0])
            except StopIteration:
                left.remove(item)


def ag_piece(net, order, block, rs, ss, done, partner=True):
    def send(cond, at, kind, dev):
        ch = net.chip(at)
        mk = lambda: rcopy(block(ch, net.c), block(ch, net.c), ss(ch, kind), rs(ch, net.c), dev)
        when(cond, lambda: mk().start())
        return lambda: when(cond, lambda: mk().wait_send())

    def spread(at, stage):
        outs = []
        for i in range(stage, len(order)):
            axis = order[i]
            for k, (cond, to) in enumerate(net.near(axis)):
                outs.append(send(cond, at, 2 * i + k, (net.chip(net.moved(axis, to)), net.c)))
        if partner:
            outs.append(send(None, at, 6, (net.e, 1 - net.c)))
        return outs

    done.extend(spread(net.at, 0))
    yield
    known = [(None, net.at)]

    for i, axis in enumerate(order):
        n, p = net.dims[axis], net.at[axis]
        fresh = []
        if n == 2:
            steps = [(None, 1 - p, None)]
        else:
            steps = []
            for k in range(1, n):
                steps.append((p - k >= 0, p - k, 0))
                steps.append((p + k <= n - 1, p + k, 1))
        for cond, o, way in steps:
            for kcond, kat in known:
                at = list(kat)
                at[axis] = o
                at = tuple(at)
                both = cond if kcond is None else (kcond if cond is None else jnp.logical_and(cond, kcond))

                def onward(at, way, i, axis):
                    outs = []
                    if way is not None:
                        cond2, to = net.near(axis)[way]
                        outs.append((cond2, 2 * i + way, (net.chip(net.moved(axis, to)), net.c)))
                    for j in range(i + 1, len(order)):
                        for k, (c2, to) in enumerate(net.near(order[j])):
                            outs.append((c2, 2 * j + k, (net.chip(net.moved(order[j], to)), net.c)))
                    if partner:
                        outs.append((None, 6, (net.e, 1 - net.c)))
                    return outs

                def arrive(at=at, way=way, i=i, axis=axis):
                    ch = net.chip(at)
                    rcopy(block(ch, net.c), block(ch, net.c), ss(ch, 0), rs(ch, net.c), (net.e, net.c)).wait_recv()
                    for c2, kind, dev in onward(at, way, i, axis):
                        send(c2, at, kind, dev)

                when(both, arrive)

                def drain(at=at, way=way, i=i, axis=axis, both=both):
                    def inner():
                        ch = net.chip(at)
                        for c2, kind, dev in onward(at, way, i, axis):
                            when(c2, lambda kind=kind, dev=dev: rcopy(
                                block(ch, net.c), block(ch, net.c), ss(ch, kind), rs(ch, net.c), dev).wait_send())
                    when(both, inner)

                done.append(drain)
                fresh.append((both, at))
                yield
        known = known + fresh
    if partner:
        for kcond, kat in known:
            def theirs(kat=kat):
                ch = net.chip(kat)
                rcopy(block(ch, 1 - net.c), block(ch, 1 - net.c), ss(ch, 0), rs(ch, 1 - net.c), (net.e, net.c)).wait_recv()
            done.append(lambda kcond=kcond, theirs=theirs: when(kcond, theirs))


def add_into(dst, src, rows):
    step = 16 if rows % 16 == 0 else 8

    def body(i, _):
        r = pl.ds(pl.multiple_of(i * step, step), step)
        dst[r, :] = (dst[r, :].astype(F32) + src[r, :].astype(F32)).astype(dst.dtype)
        return 0

    lax.fori_loop(0, rows // step, body, 0)


def rs_piece(net, order, mine, acc, bufs, key, rs, ss, rows, done, partner=True):
    def all_combos(axes_left):
        out = [()]
        for ax in axes_left:
            out = [o + (v,) for o in out for v in range(net.dims[ax])]
        return out

    def p_send(at):
        ch = net.chip(at)
        mk = lambda: rcopy(mine(ch, 1 - net.c), acc(ch), ss(0, ch), rs(0, ch), (net.e, 1 - net.c))
        mk().start()
        done.append(lambda: mk().wait_send())

    def p_recv(at):
        ch = net.chip(at)
        rcopy(acc(ch), acc(ch), ss(0, ch), rs(0, ch), (net.e, net.c)).wait_recv()
        add_into(acc(ch), mine(ch, net.c), rows)

    stages = []
    for i, axis in enumerate(order):
        left = order[i + 1:]
        combos = all_combos(left)
        stages.append((i, axis, left, combos))

    def targets_of(i, axis, left, combo, t):
        at = list(net.at)
        at[axis] = t
        for ax, v in zip(left, combo):
            at[ax] = v
        return tuple(at)

    for i, axis, left, combos in stages:
        n, p = net.dims[axis], net.at[axis]
        for combo in combos:
            for d in range(1, n):
                t = (p + d) % n
                p_send(targets_of(i, axis, left, combo, t))
        yield
    p_send(net.at)
    yield

    for i, axis, left, combos in stages:
        n, p = net.dims[axis], net.at[axis]
        nxt = lambda to, axis=axis: (net.chip(net.moved(axis, to)), net.c)

        def gather_prev(at):
            p_recv(at)
            for i2, axis2, left2, _ in stages[:i]:
                land(i2, axis2, left2, at)

        def land(i2, axis2, left2, at):
            n2, p2 = net.dims[axis2], net.at[axis2]
            ch = net.chip(at)

            def take(way):
                k = key(i2, way, at)
                rcopy(bufs(i2, k), bufs(i2, k), ss(i2 + 1, k), rs(i2 + 1, k), (net.e, net.c)).wait_recv()
                add_into(acc(ch), bufs(i2, k), rows)

            if n2 == 2:
                take(0)
            else:
                when(p2 > 0, lambda: take(0))
                when(p2 < n2 - 1, lambda: take(1))

        for combo in combos:
            if n == 2:
                at = targets_of(i, axis, left, combo, 1 - p)
                gather_prev(at)
                ch = net.chip(at)
                k = key(i, 0, at)
                mk = lambda ch=ch, k=k, i=i: rcopy(acc(ch), bufs(i, k), ss(i + 1, k), rs(i + 1, k), nxt(1 - p))
                mk().start()
                done.append(lambda mk=mk: mk().wait_send())
                yield
            else:
                for s in range(n - 1):
                    for way in (0, 1):
                        t = n - 1 - s if way == 0 else s
                        cond = (p < t) if way == 0 else (p > t)
                        to = p + 1 if way == 0 else p - 1
                        inner_cond = (p > 0) if way == 0 else (p < n - 1)
                        at = targets_of(i, axis, left, combo, t)
                        ch, k = net.chip(at), key(i, way, at)
                        mk = lambda ch=ch, k=k, i=i, to=to: rcopy(acc(ch), bufs(i, k), ss(i + 1, k), rs(i + 1, k), nxt(to))

                        def step(at=at, ch=ch, k=k, i=i, inner_cond=inner_cond, mk=mk):
                            gather_prev(at)

                            def relay():
                                rcopy(bufs(i, k), bufs(i, k), ss(i + 1, k), rs(i + 1, k), (net.e, net.c)).wait_recv()
                                add_into(acc(ch), bufs(i, k), rows)

                            pl.when(inner_cond)(relay)
                            mk().start()

                        pl.when(cond)(step)
                        done.append(lambda cond=cond, mk=mk: pl.when(cond)(lambda: mk().wait_send()))
                        yield
    at = net.at
    p_recv(at)
    for i2, axis2, left2, _ in stages:
        n2, p2 = net.dims[axis2], net.at[axis2]
        ch = net.chip(at)

        def take(way, i2=i2):
            k = key(i2, way, at)
            rcopy(bufs(i2, k), bufs(i2, k), ss(i2 + 1, k), rs(i2 + 1, k), (net.e, net.c)).wait_recv()
            add_into(acc(ch), bufs(i2, k), rows)

        if n2 == 2:
            take(0)
        else:
            when(p2 > 0, lambda: take(0))
            when(p2 < n2 - 1, lambda: take(1))
        yield


def rs_keys(net, order):
    def size(i):
        left = order[i + 1:]
        m = 1
        for ax in left:
            m *= net.dims[ax]
        n = net.dims[order[i]]
        return m if n == 2 else 2 * n * m

    def key(i, way, at):
        left = order[i + 1:]
        k = 0
        for ax in left:
            k = k * net.dims[ax] + at[ax]
        n = net.dims[order[i]]
        if n == 2:
            return k
        return (k * n + at[order[i]]) * 2 + way

    return key, [size(i) for i in range(len(order))]


def params(cid, vmem=None):
    return pltpu.CompilerParams(collective_id=cid, has_side_effects=True, vmem_limit_bytes=vmem)


ANY = pl.BlockSpec(memory_space=pl.ANY)
VM = pl.BlockSpec(memory_space=pltpu.VMEM)
DMA = pltpu.SemaphoreType.DMA

ORDER_A = (0, 1, 2)
ORDER_B = (0, 2, 1)


def reduce_scatter_all(n_expert, t, cid):
    _, _, rows, cols = t.shape
    half = rows // 2
    net0 = Net(n_expert)
    orders = ((2, 1, 0), (1, 2, 0))
    keys = [rs_keys(net0, o) for o in orders]
    sizes = keys[0][1]
    ns = max([n_expert] + sizes)

    def kernel(t_ref, o_ref, acc, b0, b1, b2, rsem, ssem):
        net = Net(n_expert).enter()
        greet(net, (0, 1, 2))
        done, gens = [], []
        bb = (b0, b1, b2)
        for i, order in enumerate(orders):
            key = keys[i][0]
            r = pl.ds(i * half, half)
            gens.append(rs_piece(
                net, order,
                lambda ch, co, r=r: t_ref.at[ch, co, r],
                lambda ch, r=r: acc.at[ch, r],
                lambda st, k, r=r: bb[st].at[k, r],
                key,
                lambda st, k, i=i: rsem.at[i, st, k],
                lambda st, k, i=i: ssem.at[i, st, k], half, done))
        interleave(*gens)
        o_ref[...] = acc[net.e]
        for f in done:
            f()

    return pl.pallas_call(
        kernel, out_shape=jax.ShapeDtypeStruct((rows, cols), BF),
        in_specs=[VM], out_specs=VM,
        scratch_shapes=[pltpu.VMEM((n_expert, rows, cols), BF)]
        + [pltpu.VMEM((s, rows, cols), BF) for s in sizes]
        + [DMA((2, 4, ns)), DMA((2, 4, ns))],
        compiler_params=params(cid, 60 << 20), name="reduce_all",
    )(t)


def local_copy(src, dst, sem, done):
    cp = lambda: pltpu.make_async_copy(src, dst, sem)
    cp().start()
    done.append(lambda: cp().wait())


def col_ag(net, src, dst, rs, ss, done):
    z, c = net.at[0], net.c
    n = net.dims[0]
    own = z // 2 == c
    s0 = z % 2

    def zdev(to):
        return (net.chip(net.moved(0, to)), c)

    def hop(cond, s, h, way, to, source=None):
        mk = lambda: rcopy(dst(s, h) if source is None else source, dst(s, h), ss(way, s, h), rs(s, h), zdev(to))
        when(cond, lambda: mk().start())
        return lambda: when(cond, lambda: mk().wait_send())

    def arrived(s, h):
        rcopy(dst(s, h), dst(s, h), ss(0, s, h), rs(s, h), (net.e, c)).wait_recv()

    across = lambda: rcopy(src, dst(s0, c), ss(2, 0, 0), rs(s0, c), (net.e, 1 - c))
    keep = lambda: pltpu.make_async_copy(src, dst(s0, c), ss(2, 0, 1))

    def begin():
        keep().start()
        hop(z < n - 1, s0, c, 0, z + 1, src)
        hop(z > 0, s0, c, 1, z - 1, src)

    pl.when(own)(begin)
    pl.when(jnp.logical_not(own))(lambda: across().start())
    yield

    def second():
        arrived(s0, 1 - c)
        hop(z < n - 1, s0, 1 - c, 0, z + 1)
        hop(z > 0, s0, 1 - c, 1, z - 1)

    pl.when(own)(second)
    yield

    def end():
        keep().wait()
        for h in (c, 1 - c):
            source = src if h is c else None
            when(z < n - 1, lambda h=h, source=source: rcopy(
                src if source is not None else dst(s0, h), dst(s0, h), ss(0, s0, h), rs(s0, h), zdev(z + 1)).wait_send())
            when(z > 0, lambda h=h, source=source: rcopy(
                src if source is not None else dst(s0, h), dst(s0, h), ss(1, s0, h), rs(s0, h), zdev(z - 1)).wait_send())

    done.append(lambda: pl.when(own)(end))
    done.append(lambda: pl.when(jnp.logical_not(own))(lambda: across().wait_send()))

    for k in range(1, n):
        for way in (0, 1):
            o = z - k if way == 0 else z + k
            inside = o >= 0 if way == 0 else o <= n - 1
            cond = jnp.logical_and(inside, o // 2 == c)
            more = z < n - 1 if way == 0 else z > 0
            to = z + 1 if way == 0 else z - 1

            def step(o=o, way=way, more=more, to=to):
                for h in (0, 1):
                    arrived(o % 2, h)
                    hop(more, o % 2, h, way, to)

            def finish(o=o, way=way, more=more, to=to):
                for h in (0, 1):
                    when(more, lambda h=h: rcopy(
                        dst(o % 2, h), dst(o % 2, h), ss(way, o % 2, h), rs(o % 2, h), zdev(to)).wait_send())

            pl.when(cond)(step)
            done.append(lambda cond=cond, finish=finish: pl.when(cond)(finish))
            yield


def col_rs(net, part, out, acc, buf, fin, rs, ss, rows, done):
    z, c = net.at[0], net.c
    n = net.dims[0]

    def zdev(to):
        return (net.chip(net.moved(0, to)), c)

    def msg(way, s, h, to):
        return rcopy(acc(way, s, h), buf(way, s, h), ss(way, s, h), rs(way, s, h), zdev(to))

    def arrived(way, s, h):
        rcopy(buf(way, s, h), buf(way, s, h), ss(way, s, h), rs(way, s, h), (net.e, c)).wait_recv()

    for k in range(n - 1):
        for way in (0, 1):
            t = n - 1 - k if way == 0 else k
            s = t % 2
            cond = jnp.logical_and(z < t if way == 0 else z > t, t // 2 == c)
            inner = z > 0 if way == 0 else z < n - 1
            to = z + 1 if way == 0 else z - 1
            for h in (0, 1):
                def step(way=way, s=s, h=h, inner=inner, to=to):
                    def relay():
                        arrived(way, s, h)
                        sum_to(acc(way, s, h), [part(s, h), buf(way, s, h)], rows)

                    pl.when(inner)(relay)
                    pl.when(jnp.logical_not(inner))(lambda: sum_to(acc(way, s, h), [part(s, h)], rows))
                    msg(way, s, h, to).start()

                pl.when(cond)(step)
                done.append(lambda cond=cond, way=way, s=s, h=h, to=to: pl.when(cond)(lambda: msg(way, s, h, to).wait_send()))
                yield

    own = z // 2 == c
    s0 = z % 2
    cross = lambda: rcopy(fin(0), fin(1), ss(2, 0, 0), rs(2, 0, 0), (net.e, 1 - c))

    def last(h, to_ref):
        low, high = z > 0, z < n - 1
        pl.when(low)(lambda: arrived(0, s0, h))
        pl.when(high)(lambda: arrived(1, s0, h))
        mid = jnp.logical_and(low, high)
        pl.when(mid)(lambda: sum_to(to_ref, [part(s0, h), buf(0, s0, h), buf(1, s0, h)], rows))
        pl.when(jnp.logical_not(low))(lambda: sum_to(to_ref, [part(s0, h), buf(1, s0, h)], rows))
        pl.when(jnp.logical_not(high))(lambda: sum_to(to_ref, [part(s0, h), buf(0, s0, h)], rows))

    def final():
        last(1 - c, fin(0))
        cross().start()
        last(c, out)

    pl.when(own)(final)
    done.append(lambda: pl.when(own)(lambda: cross().wait_send()))

    def take():
        cross().wait_recv()
        sum_to(out, [fin(1)], rows)

    yield
    pl.when(jnp.logical_not(own))(take)


def sum_to(dst, srcs, rows):
    step = 16

    def body(i, _):
        r = pl.ds(pl.multiple_of(i * step, step), step)
        v = srcs[0][r, :]
        if len(srcs) > 1:
            v = v.astype(F32)
            for s in srcs[1:]:
                v = v + s[r, :].astype(F32)
        dst[r, :] = v.astype(BF)
        return 0

    lax.fori_loop(0, rows // step, body, 0)


def to_all(net, src, dst, rs, ss, done):
    total = net.chips * 2
    me = net.e * 2 + net.c

    def put(k, _):
        t = (me + k) % total
        rcopy(src(t), dst(me), ss(k), rs(me), (t // 2, t % 2)).start()
        return 0

    lax.fori_loop(1, total, put, 0)
    yield

    def take(k, _):
        t = (me + k) % total
        rcopy(src(t), dst(me), ss(k), rs(me), (t // 2, t % 2)).wait_send()
        rcopy(dst(t), dst(t), ss(k), rs(t), (net.e, net.c)).wait_recv()
        return 0

    done.append(lambda: lax.fori_loop(1, total, take, 0))


def gather_start(n_expert, tokens, wqkv, w_out, aux, cot, cid):
    T, D = tokens.shape
    Z, R, C = wqkv.shape
    HR = w_out.shape[0]
    AR, AW = aux.shape
    plane = n_expert // Z
    nd = 2 * n_expert

    with_g = cot is not None

    def kernel(*refs):
        k = 5 if with_g else 4
        t_ref, w_ref, o_ref, a_ref = refs[:4]
        g_ref, G = (refs[4], refs[2 * k - 1]) if with_g else (None, None)
        X, W, O, A = refs[k:k + 4]
        xr, xs, wr, ws, war, was, oar, oas, ar, as_, gr, gs, loc = refs[2 * k:]
        net = Net(n_expert).enter()
        z, p, c = net.at[0], net.e % plane, net.c
        me = net.e * 2 + c
        done = []
        local_copy(w_ref.at[z], W.at[z, p, c], loc.at[0], [])
        local_copy(o_ref, O.at[p, c], loc.at[1], [])
        local_copy(a_ref, A.at[me], loc.at[2], [])
        if with_g:
            local_copy(g_ref, G.at[net.e, c], loc.at[3], [])
        greet_column(net)

        def wgen():
            for k in range(1, Z):
                j = (z + k) % Z
                mk = lambda j=j, k=k: rcopy(w_ref.at[j], W.at[z, p, c], ws.at[k], wr.at[z], (j * plane + p, c))
                mk().start()
                done.append(lambda mk=mk: mk().wait_send())
            yield
            pltpu.make_async_copy(w_ref.at[z], W.at[z, p, c], loc.at[0]).wait()
            for k in range(1, Z):
                o = (z + k) % Z
                rcopy(W.at[o, p, c], W.at[o, p, c], ws.at[k], wr.at[o], (net.e, c)).wait_recv()
            gens = []
            for i, order in enumerate(((1, 2), (2, 1))):
                r = pl.ds(i * (Z // 2), Z // 2)
                gens.append(ag_piece(
                    net, order, lambda ch, co, r=r: W.at[r, ch % plane, co],
                    lambda ch, co, i=i: war.at[i, ch % plane, co], lambda ch, kind, i=i: was.at[i, ch % plane, kind], done))
            while gens:
                for g in list(gens):
                    try:
                        next(g)
                        yield
                    except StopIteration:
                        gens.remove(g)

        def agen():
            pltpu.make_async_copy(a_ref, A.at[me], loc.at[2]).wait()
            yield from ag_piece(
                net, ORDER_A, lambda ch, co: A.at[ch * 2 + co], lambda ch, co: ar.at[ch, co], lambda ch, kind: as_.at[ch, kind], done)

        def ogen(i, order):
            if i == 0:
                pltpu.make_async_copy(o_ref, O.at[p, c], loc.at[1]).wait()
            r = pl.ds(i * (HR // 2), HR // 2)
            yield from ag_piece(
                net, order, lambda ch, co: O.at[ch % plane, co, r],
                lambda ch, co: oar.at[i, ch % plane, co], lambda ch, kind: oas.at[i, ch % plane, kind], done)

        def ggen(i, order):
            if i == 0:
                pltpu.make_async_copy(g_ref, G.at[net.e, c], loc.at[3]).wait()
            r = pl.ds(i * (T // 2), T // 2)
            yield from ag_piece(
                net, order, lambda ch, co: G.at[ch, co, r],
                lambda ch, co: gr.at[i, ch, co], lambda ch, kind: gs.at[i, ch, kind], done)

        interleave(
            wgen(),
            agen(),
            col_ag(net, t_ref, lambda s, h: X.at[s, h], lambda s, h: xr.at[s, h], lambda w, s, h: xs.at[w, s, h], done),
            ogen(0, (1, 2)), ogen(1, (2, 1)), *([ggen(0, ORDER_A), ggen(1, ORDER_B)] if with_g else []))
        for f in done:
            f()

    S = jax.ShapeDtypeStruct
    return pl.pallas_call(
        kernel,
        out_shape=(S((2, 2, T, D), BF), S((Z, plane, 2, R, C), BF), S((plane, 2, HR, D), BF), S((nd, AR, AW), BF))
        + ((S((n_expert, 2, T, D), BF),) if with_g else ()),
        in_specs=[VM] * (5 if with_g else 4), out_specs=(ANY,) * (5 if with_g else 4),
        scratch_shapes=[DMA((2, 2)), DMA((3, 2, 2)), DMA((Z,)), DMA((Z,)), DMA((2, plane, 2)), DMA((2, plane, 7)),
                        DMA((2, plane, 2)), DMA((2, plane, 7)), DMA((n_expert, 2)), DMA((n_expert, 7)),
                        DMA((2, n_expert, 2)), DMA((2, n_expert, 7)), DMA((4,))],
        compiler_params=params(cid), name="gather_start",
    )(tokens, wqkv, w_out, aux, *((cot,) if with_g else ()))


def column_sum(n_expert, part, cid):
    _, _, T, D = part.shape

    def kernel(p_ref, o_ref, acc, buf, fin, rsem, ssem):
        net = Net(n_expert).enter()
        greet(net, (0,))
        done = []
        interleave(col_rs(
            net, lambda s, h: p_ref.at[s, h], o_ref, lambda w, s, h: acc.at[w, s, h], lambda w, s, h: buf.at[w, s, h],
            lambda i: fin.at[i], lambda w, s, h: rsem.at[w, s, h], lambda w, s, h: ssem.at[w, s, h], T, done))
        for f in done:
            f()

    return pl.pallas_call(
        kernel, out_shape=jax.ShapeDtypeStruct((T, D), BF), in_specs=[VM], out_specs=VM,
        scratch_shapes=[pltpu.VMEM((2, 2, 2, T, D), BF), pltpu.VMEM((2, 2, 2, T, D), BF), pltpu.VMEM((2, T, D), BF),
                        DMA((3, 2, 2)), DMA((3, 2, 2))],
        compiler_params=params(cid, 40 << 20), name="column_sum",
    )(part)


def column_gather(n_expert, x, cid):
    T, D = x.shape

    def kernel(x_ref, X, rsem, ssem):
        net = Net(n_expert).enter()
        greet(net, (0,))
        done = []
        interleave(col_ag(net, x_ref, lambda s, h: X.at[s, h], lambda s, h: rsem.at[s, h], lambda w, s, h: ssem.at[w, s, h], done))
        for f in done:
            f()

    return pl.pallas_call(
        kernel, out_shape=jax.ShapeDtypeStruct((2, 2, T, D), BF), in_specs=[VM], out_specs=ANY,
        scratch_shapes=[DMA((2, 2)), DMA((3, 2, 2))],
        compiler_params=params(cid), name="column_gather",
    )(x)


def gather_all(n_expert, x, aux, cid):
    rows, cols = x.shape
    half = rows // 2
    nd = 2 * n_expert

    def kernel(x_ref, a_ref, o_ref, A, rsem, ssem, ar, as_, lsem):
        net = Net(n_expert).enter()
        me = net.e * 2 + net.c
        done = []
        local_copy(x_ref, o_ref.at[net.e, net.c], lsem.at[0], [])
        local_copy(a_ref, A.at[me], lsem.at[1], done)
        greet_all(net)
        pltpu.make_async_copy(x_ref, o_ref.at[net.e, net.c], lsem.at[0]).wait()
        gens = [to_all(net, lambda t: a_ref, lambda s: A.at[s], lambda s: ar.at[s], lambda k: as_.at[k], done)]
        for i, order in enumerate((ORDER_A, ORDER_B)):
            gens.append(ag_piece(
                net, order,
                lambda ch, co, i=i: o_ref.at[ch, co, pl.ds(i * half, half)],
                lambda ch, co, i=i: rsem.at[i, ch, co],
                lambda ch, kind, i=i: ssem.at[i, ch, kind], done))
        interleave(*gens)
        for f in done:
            f()

    return pl.pallas_call(
        kernel,
        out_shape=(jax.ShapeDtypeStruct((n_expert, 2, rows, cols), x.dtype), jax.ShapeDtypeStruct((nd,) + aux.shape, aux.dtype)),
        in_specs=[VM, VM], out_specs=(ANY, ANY),
        scratch_shapes=[DMA((2, n_expert, 2)), DMA((2, n_expert, 7)), DMA((nd,)), DMA((nd,)), DMA((2,))],
        compiler_params=params(cid), name="gather_all",
    )(x, aux)


def exchange(n_expert, x, cid):
    nd = 2 * n_expert

    def kernel(x_ref, o_ref, ar, as_, lsem):
        net = Net(n_expert).enter()
        me = net.e * 2 + net.c
        done = []
        local_copy(x_ref.at[me], o_ref.at[me], lsem.at[0], done)
        greet_all(net)
        interleave(to_all(net, lambda t: x_ref.at[t], lambda s: o_ref.at[s], lambda s: ar.at[s], lambda k: as_.at[k], done))
        for f in done:
            f()

    return pl.pallas_call(
        kernel, out_shape=jax.ShapeDtypeStruct(x.shape, x.dtype), in_specs=[VM], out_specs=VM,
        scratch_shapes=[DMA((nd,)), DMA((nd,)), DMA((2,))],
        compiler_params=params(cid), name="exchange",
    )(x)


def reduce_end(n_expert, part, dw, do, small, cid):
    _, _, T, D = part.shape
    Z, plane, _, R, C = dw.shape
    HR = do.shape[2]
    nd = 2 * n_expert
    net0 = Net(n_expert)
    orders = ((2, 1), (1, 2))
    keys = [rs_keys(net0, o) for o in orders]
    sizes = keys[0][1]
    ns = max([plane] + sizes)
    hr = HR // 2

    def kernel(p_ref, dw_ref, do_ref, s_ref, x_out, w_out, o_out, s_out,
               acc, buf, fin, wacc, wb0, wb1, oacc, ob0, ob1, wsh,
               xr, xs, wr, ws, our, ous, sr, s_s, zr, zs, loc):
        net = Net(n_expert).enter()
        z, p, c = net.at[0], net.e % plane, net.c
        me = net.e * 2 + c
        done = []
        own = lambda: pltpu.make_async_copy(s_ref.at[me], s_out.at[me], loc)
        own().start()
        done.append(lambda: own().wait())
        greet_all(net)

        def wgen(q):
            i = q // (Z // 2)
            key = keys[i][0]
            bb = (wb0, wb1)
            yield from rs_piece(
                net, orders[i], lambda ch, co: dw_ref.at[q, ch % plane, co], lambda ch: wacc.at[q, ch % plane],
                lambda st, k: bb[st].at[q, k], key, lambda st, k: wr.at[q, st, k if st else k % plane],
                lambda st, k: ws.at[q, st, k if st else k % plane], R, done)
            mk = lambda: rcopy(wacc.at[q, p], wsh.at[z], zs.at[q], zr.at[z], (q * plane + p, c))
            pl.when(z != q)(lambda: mk().start())
            done.append(lambda: pl.when(z != q)(lambda: mk().wait_send()))
            pl.when(z == q)(lambda: sum_to(w_out.at[q], [wacc.at[q, p]], R))

        def ogen(i):
            key = keys[i][0]
            bb = (ob0, ob1)
            r = pl.ds(i * hr, hr)
            yield from rs_piece(
                net, orders[i], lambda ch, co: do_ref.at[ch % plane, co, r], lambda ch: oacc.at[ch % plane, r],
                lambda st, k: bb[st].at[k, r], key, lambda st, k: our.at[i, st, k if st else k % plane],
                lambda st, k: ous.at[i, st, k if st else k % plane], hr, done)

        interleave(
            *[wgen(q) for q in range(Z)],
            ogen(0), ogen(1),
            col_rs(net, lambda s, h: p_ref.at[s, h], x_out, lambda w, s, h: acc.at[w, s, h], lambda w, s, h: buf.at[w, s, h],
                   lambda i: fin.at[i], lambda w, s, h: xr.at[w, s, h], lambda w, s, h: xs.at[w, s, h], T, done),
            to_all(net, lambda t: s_ref.at[t], lambda s: s_out.at[s], lambda s: sr.at[s], lambda k: s_s.at[k], done))
        o_out[...] = oacc[p]
        for k in range(1, Z):
            o = (z + k) % Z
            rcopy(wsh.at[o], wsh.at[o], zs.at[0], zr.at[o], (net.e, c)).wait_recv()
            sum_to(w_out.at[o], [wsh.at[o]], R)
        for f in done:
            f()

    S = jax.ShapeDtypeStruct
    V = pltpu.VMEM
    return pl.pallas_call(
        kernel, out_shape=(S((T, D), BF), S((Z, R, C), BF), S((HR, D), BF), S(small.shape, small.dtype)),
        in_specs=[VM] * 4, out_specs=(VM,) * 4,
        scratch_shapes=[V((2, 2, 2, T, D), BF), V((2, 2, 2, T, D), BF), V((2, T, D), BF),
                        V((Z, plane, R, C), BF), V((Z, sizes[0], R, C), BF), V((Z, sizes[1], R, C), BF),
                        V((plane, HR, D), BF), V((sizes[0], HR, D), BF), V((sizes[1], HR, D), BF), V((Z, R, C), BF),
                        DMA((3, 2, 2)), DMA((3, 2, 2)), DMA((Z, 3, ns)), DMA((Z, 3, ns)), DMA((2, 3, ns)), DMA((2, 3, ns)),
                        DMA((nd,)), DMA((nd,)), DMA((Z,)), DMA((Z,)), DMA],
        compiler_params=params(cid, 60 << 20), name="reduce_end",
    )(part, dw, do, small)


def slot_plane(z, i):
    near = jnp.where(z < 2, z, 3 - z)
    t = jnp.where(jnp.logical_and(near == 1, i < 2), 1 - i, i)
    return jnp.where(z < 2, t, 3 - t)


class Gather22:
    def __init__(self, net, N, T, rsem, ssem, A=None):
        self.net, self.N, self.T, self.rsem, self.ssem, self.A = net, N, T, rsem, ssem, A
        self.axes = ((1, 2), (2, 1), (1, 2))
        self.pieces = (0, 1) if A is None else (2, 0, 1)

    def blk(self, piece, chip, core):
        if piece == 2:
            return self.A.at[chip * 2 + core]
        h = self.T // 2
        return self.N.at[chip, pl.ds(pl.multiple_of(core * self.T + piece * h, h), h)]

    def copy(self, piece, at, kind, dev):
        n = self.net
        ch = n.chip(at)
        b = self.blk(piece, ch, n.c)
        return rcopy(b, b, self.ssem.at[piece, ch, kind], self.rsem.at[piece, ch, n.c], dev)

    def wait(self, piece, at, core):
        n = self.net
        ch = n.chip(at)
        b = self.blk(piece, ch, core)
        rcopy(b, b, self.ssem.at[piece, ch, 0], self.rsem.at[piece, ch, core], (n.e, n.c)).wait_recv()

    def dev(self, axis, to=None):
        n = self.net
        return (n.chip(n.moved(axis, 1 - n.at[axis] if to is None else to)), n.c)

    def level(self, piece, zt, two, three):
        n = self.net
        at = [zt, n.at[1], n.at[2]]
        u, v = self.axes[piece]
        if two:
            at[u] = 1 - at[u]
        if three:
            at[v] = 1 - at[v]
        return tuple(at)

    def outs(self, piece, zt, two, three):
        u, v = self.axes[piece]
        at = self.level(piece, zt, two, three)
        r = []
        if not two and not three:
            r.append((2, self.dev(u)))
        if not three:
            r.append((3, self.dev(v)))
        r.append((4, (self.net.e, 1 - self.net.c)))
        return at, r

    def push(self, piece, zt, two, three):
        at, r = self.outs(piece, zt, two, three)
        for kind, dev in r:
            self.copy(piece, at, kind, dev).start()

    def begin(self):
        z = self.net.at[0]
        for piece in self.pieces:
            pl.when(z < 3)(lambda piece=piece: self.copy(piece, self.net.at, 0, self.dev(0, z + 1)).start())
            pl.when(z > 0)(lambda piece=piece: self.copy(piece, self.net.at, 1, self.dev(0, z - 1)).start())
            self.push(piece, z, False, False)

    def onward(self, zt):
        z = self.net.at[0]
        to = jnp.where(zt < z, z + 1, z - 1)
        return to, jnp.logical_and(to >= 0, to <= 3)

    def from_z(self, zt):
        to, more = self.onward(zt)
        for piece in self.pieces:
            at = self.level(piece, zt, False, False)
            self.wait(piece, at, self.net.c)
            pl.when(more)(lambda piece=piece, at=at: self.copy(piece, at, 0, self.dev(0, to)).start())
            self.push(piece, zt, False, False)

    def from_two(self, zt):
        for piece in self.pieces:
            self.wait(piece, self.level(piece, zt, True, False), self.net.c)
            self.push(piece, zt, True, False)

    def from_three(self, zt):
        for two in (False, True):
            for piece in self.pieces:
                self.wait(piece, self.level(piece, zt, two, True), self.net.c)
                self.push(piece, zt, two, True)

    def from_partner(self, zt):
        for piece in self.pieces:
            for a in (0, 1):
                for b in (0, 1):
                    self.wait(piece, (zt, a, b), 1 - self.net.c)

    def drain(self, i):
        z = self.net.at[0]
        zt = slot_plane(z, i)
        to, more = self.onward(zt)
        for piece in self.pieces:
            def own(piece=piece):
                pl.when(z < 3)(lambda: self.copy(piece, self.net.at, 0, self.dev(0, z + 1)).wait_send())
                pl.when(z > 0)(lambda: self.copy(piece, self.net.at, 1, self.dev(0, z - 1)).wait_send())

            pl.when(i == 0)(own)
            at0 = self.level(piece, zt, False, False)
            pl.when(jnp.logical_and(i > 0, more))(
                lambda piece=piece, at0=at0: self.copy(piece, at0, 0, self.dev(0, to)).wait_send())
            for two in (False, True):
                for three in (False, True):
                    at, r = self.outs(piece, zt, two, three)
                    for kind, dev in r:
                        self.copy(piece, at, kind, dev).wait_send()


def add_rows(dst, srcs, rows):
    step = 32

    def body(i, _):
        r = pl.ds(pl.multiple_of(i * step, step), step)
        v = dst[r, :].astype(F32)
        for s in srcs:
            v = v + s[r, :].astype(F32)
        dst[r, :] = v.astype(BF)
        return 0

    lax.fori_loop(0, rows // step, body, 0)


class Reduce22:
    def __init__(self, net, T, acc, buf1, buf2, zbuf, sems):
        self.net, self.T = net, T
        self.acc, self.buf1, self.buf2, self.zbuf = acc, buf1, buf2, zbuf
        (self.r0, self.s0, self.r1, self.s1, self.r2, self.s2, self.r3, self.s3) = sems
        self.first = (2, 1)
        self.second = (1, 2)

    @staticmethod
    def scratch(T, D):
        V = pltpu.VMEM
        return [V((16, T, D), BF), V((4, 2, T, D), BF), V((4, T, D), BF), V((2, 4, T, D), BF),
                DMA((16,)), DMA((16,)), DMA((2, 4, 2)), DMA((2, 4, 2)), DMA((2, 4)), DMA((2, 4)), DMA((2, 2, 4)), DMA((2, 2, 4))]

    def half(self, piece):
        h = self.T // 2
        return pl.ds(piece * h, h)

    def ring(self):
        n = self.net
        a, b = n.at[1], n.at[2]
        return [(1 - a, 1 - b), (a, 1 - b), (1 - a, b), (a, b)]

    def p_copy(self, Tb, zt, ab):
        n = self.net
        p = ab[0] * 2 + ab[1]
        ch = zt * 4 + p
        src = Tb.at[p, pl.ds(pl.multiple_of((1 - n.c) * self.T, self.T), self.T)]
        return rcopy(src, self.acc.at[ch], self.s0.at[ch], self.r0.at[ch], (n.e, 1 - n.c))

    def p_send(self, Tb, zt):
        for ab in self.ring():
            self.p_copy(Tb, zt, ab).start()

    def p_wait_send(self, Tb, zt):
        for ab in self.ring():
            self.p_copy(Tb, zt, ab).wait_send()

    def p_take(self, Tb, zt, ab):
        n = self.net
        p = ab[0] * 2 + ab[1]
        self.p_copy(Tb, zt, ab).wait_recv()
        add_rows(self.acc.at[zt * 4 + p], [Tb.at[p, pl.ds(pl.multiple_of(n.c * self.T, self.T), self.T)]], self.T)

    def one(self, piece, zt, idx):
        n = self.net
        ax = self.first[piece]
        at = [zt, n.at[1], n.at[2]]
        at[ax] = 1 - at[ax]
        at[self.second[piece]] = idx
        src = self.acc.at[n.chip(at), self.half(piece)]
        dst = self.buf1.at[zt, idx, self.half(piece)]
        return rcopy(src, dst, self.s1.at[piece, zt, idx], self.r1.at[piece, zt, idx], (n.chip(n.moved(ax, 1 - n.at[ax])), n.c))

    def two(self, piece, zt):
        n = self.net
        ax = self.second[piece]
        at = [zt, n.at[1], n.at[2]]
        at[ax] = 1 - at[ax]
        src = self.acc.at[n.chip(at), self.half(piece)]
        return rcopy(src, self.buf2.at[zt, self.half(piece)], self.s2.at[piece, zt], self.r2.at[piece, zt],
                     (n.chip(n.moved(ax, 1 - n.at[ax])), n.c))

    def three(self, piece, zt):
        n = self.net
        z = n.at[0]
        up = zt > z
        d = jnp.where(up, 0, 1)
        to = jnp.where(up, z + 1, z - 1)
        src = self.acc.at[n.chip((zt, n.at[1], n.at[2])), self.half(piece)]
        return rcopy(src, self.zbuf.at[d, zt, self.half(piece)], self.s3.at[piece, d, zt], self.r3.at[piece, d, zt],
                     (n.chip(n.moved(0, to)), n.c))

    def stage0(self, Tb, zt):
        n = self.net
        order = self.ring()
        self.p_take(Tb, zt, order[0])
        self.one(0, zt, 1 - n.at[1]).start()
        self.one(1, zt, 1 - n.at[2]).start()
        self.p_take(Tb, zt, order[1])
        self.one(0, zt, n.at[1]).start()
        self.p_take(Tb, zt, order[2])
        self.one(1, zt, n.at[2]).start()
        self.p_take(Tb, zt, order[3])

    def stage1(self, zt):
        n = self.net
        for part in (0, 1):
            for piece in (0, 1):
                own = n.at[self.second[piece]]
                idx = 1 - own if part == 0 else own
                at = [zt, n.at[1], n.at[2]]
                at[self.second[piece]] = idx
                self.one(piece, zt, idx).wait_recv()
                add_rows(self.acc.at[n.chip(at), self.half(piece)], [self.buf1.at[zt, idx, self.half(piece)]], self.T // 2)
                if part == 0:
                    self.two(piece, zt).start()

    def stage2(self, zt):
        n = self.net
        z = n.at[0]
        feeds = jnp.where(zt > z, z > 0, z < 3)
        for piece in (0, 1):
            self.two(piece, zt).wait_recv()
            add_rows(self.acc.at[n.chip((zt, n.at[1], n.at[2])), self.half(piece)], [self.buf2.at[zt, self.half(piece)]], self.T // 2)
            pl.when(jnp.logical_and(zt != z, jnp.logical_not(feeds)))(lambda piece=piece: self.three(piece, zt).start())

    def relay(self, zt):
        n = self.net
        z = n.at[0]
        d = jnp.where(zt > z, 0, 1)
        feeds = jnp.where(zt > z, z > 0, z < 3)

        def go():
            for piece in (0, 1):
                self.three(piece, zt).wait_recv()
                add_rows(self.acc.at[n.chip((zt, n.at[1], n.at[2])), self.half(piece)],
                         [self.zbuf.at[d, zt, self.half(piece)]], self.T // 2)
                self.three(piece, zt).start()

        pl.when(jnp.logical_and(zt != z, feeds))(go)

    def arrive(self, piece, d):
        n = self.net
        z = n.at[0]
        dst = self.zbuf.at[d, z, self.half(piece)]
        rcopy(dst, dst, self.s3.at[piece, d, z], self.r3.at[piece, d, z], (n.e, n.c)).wait_recv()
        add_rows(self.acc.at[n.e, self.half(piece)], [dst], self.T // 2)

    def last(self, out):
        z = self.net.at[0]
        for piece in (0, 1):
            pl.when(z > 0)(lambda piece=piece: self.arrive(piece, 0))
            pl.when(z < 3)(lambda piece=piece: self.arrive(piece, 1))
        out[...] = self.acc[self.net.e]

    def drain(self, zt):
        n = self.net
        for piece in (0, 1):
            for idx in (0, 1):
                self.one(piece, zt, idx).wait_send()
            self.two(piece, zt).wait_send()
            pl.when(zt != n.at[0])(lambda piece=piece: self.three(piece, zt).wait_send())


NT = (((1,), (1,)), ((), ()))
TN = (((0,), (0,)), ((), ()))


def experts_fused(x, marked, G, w_gate, w_up, w_down, cap, cid):
    T, D = x.shape
    E = marked.shape[0]
    X2, _, Fh = w_gate.shape
    chips = G.shape[0]
    nd = 2 * chips
    S2 = 2 * cap
    M = 4 * S2
    CW = 512
    PR = 64
    SW = 1024

    def kernel(x_ref, a_ref, g_ref, wg_ref, wu_ref, wd_ref, o_sum, o_part, o_dots, o_rows, o_grows, o_act, o_ggu, N,
               A, wgu, wdn, Nst, Gst, H, pk, pkt, sw, rowsb, growsb, h1, h2, actw, ggu, yb, To, Tb, dsend,
               acc, b1, b2, zb, r0, s0, r1, s1, r2, s2, r3, s3, xr, xs, dr, ds_, lsem):
        net = Net(chips).enter()
        z, c, e = net.at[0], net.c, net.e
        me = e * 2 + c
        copies = [(wg_ref.at[i], wgu.at[i, :, pl.ds(0, Fh)]) for i in range(2)]
        copies += [(wu_ref.at[i], wgu.at[i, :, pl.ds(Fh, Fh)]) for i in range(2)]
        copies += [(wd_ref, wdn)]
        loads = [lambda s=s, d=d, i=i: pltpu.make_async_copy(s, d, lsem.at[i]) for i, (s, d) in enumerate(copies)]
        own = lambda: pltpu.make_async_copy(x_ref, N.at[e, pl.ds(pl.multiple_of(c * T, T), T)], lsem.at[6])
        own().start()
        acopy = lambda: pltpu.make_async_copy(a_ref, A.at[me], lsem.at[7])
        acopy().start()
        greet_all(net)
        own().wait()
        acopy().wait()
        ag = Gather22(net, N, T, xr, xs, A)
        rs = Reduce22(net, T, acc, b1, b2, zb, (r0, s0, r1, s1, r2, s2, r3, s3))
        ag.begin()
        for f in loads:
            f().start()
        lane = lax.broadcasted_iota(jnp.int32, (256, 256), 1)
        sub = lax.broadcasted_iota(jnp.int32, (256, 256), 0)
        U = jnp.where(jnp.logical_and(sub < lane, sub // 128 == lane // 128), 1.0, 0.0).astype(BF)
        eye = jnp.where(sub == lane, 1.0, 0.0).astype(BF)
        place = ((lax.broadcasted_iota(jnp.int32, (8, 256), 1) // 128) * cap).astype(F32)
        ag.from_z(slot_plane(z, 1))
        ag.from_two(z)
        for f in loads:
            f().wait()

        def dots_to(t, act):
            pl.when(t != me)(lambda: act(rcopy(dsend.at[t], o_dots.at[me], ds_.at[t], dr.at[me], (t // 2, t % 2))))

        saves = lambda i: [
            (rowsb, o_rows.at[:, i], 8), (growsb, o_grows.at[:, i], 9), (actw, o_act.at[:, i], 10), (ggu, o_ggu.at[:, i], 11)]

        def body(i, _):
            zt = slot_plane(z, i)
            zn = slot_plane(z, i + 1)
            zp = slot_plane(z, i - 1)
            pltpu.make_async_copy(g_ref.at[pl.ds(zt * 4, 4)], Gst, lsem.at[13]).start()
            ag.from_three(zt)
            ag.from_partner(zt)
            cpn = pltpu.make_async_copy(N.at[pl.ds(zt * 4, 4)], Nst, lsem.at[12])
            cpn.start()
            for ch in range(4):
                for ei in range(2):
                    for co in range(2):
                        H[2 * ch + ei:2 * ch + ei + 1, co * 128:(co + 1) * 128] = A[(zt * 4 + ch) * 2 + co, pl.ds(2 * e + ei, 1), :]
            h = H[...]
            here = jnp.where(h >= 0.0, 1.0, 0.0)
            slot = jnp.dot(here.astype(BF), U, preferred_element_type=F32) + place
            slot = jnp.where(here > 0.0, slot, -1.0)
            row_id = lax.broadcasted_iota(jnp.int32, (S2, 256), 0).astype(F32)
            for ch in range(4):
                for ei in range(2):
                    q = 2 * ch + ei
                    hit = row_id == slot[q:q + 1, :]
                    pk[ch, ei * S2:(ei + 1) * S2, :] = jnp.where(hit, 1.0, 0.0).astype(BF)
                    wcol = jnp.sum(jnp.where(hit, h[q:q + 1, :], 0.0), axis=1, keepdims=True)
                    sw[ei, ch * S2:(ch + 1) * S2, :] = jnp.broadcast_to(wcol, (S2, 128))
                pkt[ch] = lax.dot_general(eye, pk[ch], NT, preferred_element_type=F32).astype(BF)

            def before():
                for src, dst, s in saves(i):
                    pltpu.make_async_copy(src, dst, lsem.at[s]).wait()

            pl.when(i > 0)(before)
            cpn.wait()
            pltpu.make_async_copy(g_ref.at[pl.ds(zt * 4, 4)], Gst, lsem.at[13]).wait()

            def picks(k, _):
                ch, j = k // 2, k % 2
                cols = pl.ds(pl.multiple_of(j * (D // 2), D // 2), D // 2)
                at = pl.ds(pl.multiple_of(ch * S2, S2), S2)
                for st, dst in ((Nst, rowsb), (Gst, growsb)):
                    r = jnp.dot(pk[ch], st[ch, :, cols], preferred_element_type=F32).astype(BF)
                    dst[0, at, cols] = r[:S2]
                    dst[1, at, cols] = r[S2:]
                return 0

            lax.fori_loop(0, 8, picks, 0)
            pltpu.make_async_copy(rowsb, o_rows.at[:, i], lsem.at[8]).start()
            pltpu.make_async_copy(growsb, o_grows.at[:, i], lsem.at[9]).start()
            pl.when(i < 2)(lambda: ag.from_z(slot_plane(z, i + 2)))
            pl.when(i > 0)(lambda: rs.stage1(zp))

            for ei in range(2):
                h1[...] = jnp.dot(rowsb[ei], wgu[ei], preferred_element_type=F32)
                h2[...] = lax.dot_general(growsb[ei], wdn[ei], NT, preferred_element_type=F32)

                def point(k, _):
                    r = pl.ds(pl.multiple_of(k * PR, PR), PR)
                    gate, up, ga = h1[r, :Fh], h1[r, Fh:], h2[r, :]
                    w = sw[ei, r, 0:1]
                    sig = 1.0 / (1.0 + jnp.exp(-gate))
                    silu = gate * sig
                    act = silu * up
                    actw[ei, r, :] = (w * act).astype(BF)
                    sw[ei, r, :] = jnp.broadcast_to(jnp.sum(act * ga, axis=1, keepdims=True), (PR, 128))
                    gact = w * ga
                    ggu[ei, r, :Fh] = (gact * up * (sig + silu * (1.0 - sig))).astype(BF)
                    ggu[ei, r, Fh:] = (gact * silu).astype(BF)
                    return 0

                lax.fori_loop(0, M // PR, point, 0)
                for ch in range(4):
                    dcol = sw[ei, ch * S2:(ch + 1) * S2, 0:1]
                    dd = jnp.sum(pk[ch, ei * S2:(ei + 1) * S2, :].astype(F32) * dcol, axis=0, keepdims=True)
                    for co in range(2):
                        dsend[(zt * 4 + ch) * 2 + co, ei:ei + 1, :] = dd[:, co * 128:(co + 1) * 128]
                if ei == 0:
                    pl.when(i < 3)(lambda: ag.from_two(zn))
            for k in range(8):
                dots_to(zt * 8 + k, lambda cp: cp.start())
            pltpu.make_async_copy(actw, o_act.at[:, i], lsem.at[10]).start()
            pltpu.make_async_copy(ggu, o_ggu.at[:, i], lsem.at[11]).start()
            pl.when(i > 0)(lambda: rs.stage2(zp))

            def back(j, _):
                rws = pl.ds(pl.multiple_of(j * CW, CW), CW)
                for ei in range(2):
                    r = lax.dot_general(ggu[ei], wgu[ei, rws, :], NT, preferred_element_type=F32).astype(BF)
                    for ch in range(4):
                        yb[ch, ei * S2:(ei + 1) * S2, rws] = r[ch * S2:(ch + 1) * S2]
                return 0

            lax.fori_loop(0, D // CW, back, 0)
            for ab in rs.ring():
                ch = ab[0] * 2 + ab[1]

                def spread_back(j, _, ch=ch):
                    cols = pl.ds(pl.multiple_of(j * SW, SW), SW)
                    Tb[ch, :, cols] = jnp.dot(pkt[ch], yb[ch, :, cols], preferred_element_type=F32).astype(BF)
                    return 0

                lax.fori_loop(0, D // SW, spread_back, 0)
                rs.p_copy(Tb, zt, ab).start()

            def down(j, _):
                cols = pl.ds(pl.multiple_of(j * CW, CW), CW)
                for ei in range(2):
                    r = jnp.dot(actw[ei], wdn[ei, :, cols], preferred_element_type=F32).astype(BF)
                    for ch in range(4):
                        yb[ch, ei * S2:(ei + 1) * S2, cols] = r[ch * S2:(ch + 1) * S2]
                return 0

            lax.fori_loop(0, D // CW, down, 0)
            rs.stage0(Tb, zt)
            rs.p_wait_send(Tb, zt)
            for ch in range(4):
                cp = lambda ch=ch: pltpu.make_async_copy(To.at[ch % 2], o_part.at[zt * 4 + ch], lsem.at[14 + ch % 2])
                if ch >= 2:
                    cp().wait()

                def spread(j, _, ch=ch):
                    cols = pl.ds(pl.multiple_of(j * SW, SW), SW)
                    To[ch % 2, :, cols] = jnp.dot(pkt[ch], yb[ch, :, cols], preferred_element_type=F32).astype(BF)
                    return 0

                lax.fori_loop(0, D // SW, spread, 0)
                cp().start()
            for ch in (2, 3):
                pltpu.make_async_copy(To.at[ch % 2], o_part.at[zt * 4 + ch], lsem.at[14 + ch % 2]).wait()
            return 0

        lax.fori_loop(0, 4, body, 0)
        z3 = slot_plane(z, 3)
        own_dots = pltpu.make_async_copy(dsend.at[me], o_dots.at[me], lsem.at[5])
        own_dots.start()
        rs.stage1(z3)
        rs.relay(slot_plane(z, 2))
        rs.stage2(z3)
        rs.relay(z3)
        rs.relay(slot_plane(z, 1))
        rs.last(o_sum)
        own_dots.wait()

        def dots_from(k, _):
            t = (me + k) % nd
            rcopy(o_dots.at[t], o_dots.at[t], ds_.at[t], dr.at[t], (e, c)).wait_recv()
            dots_to(t, lambda cp: cp.wait_send())
            return 0

        lax.fori_loop(1, nd, dots_from, 0)
        for src, dst, s in saves(3):
            pltpu.make_async_copy(src, dst, lsem.at[s]).wait()

        def finish(i, _):
            ag.drain(i)
            rs.drain(slot_plane(z, i))
            return 0

        lax.fori_loop(0, 4, finish, 0)

    S = jax.ShapeDtypeStruct
    V = pltpu.VMEM
    return pl.pallas_call(
        kernel,
        out_shape=(S((T, D), BF), S((chips, 2 * T, D), BF), S((nd, 8, 128), F32), S((2, 4, M, D), BF), S((2, 4, M, D), BF),
                   S((2, 4, M, Fh), BF), S((2, 4, M, 2 * Fh), BF), S((chips, 2 * T, D), BF)),
        in_specs=[VM, VM, ANY, ANY, ANY, ANY], out_specs=(VM, ANY, VM, ANY, ANY, ANY, ANY, ANY),
        scratch_shapes=[
            V((nd, E, T), F32), V((2, D, 2 * Fh), BF), V((2, Fh, D), BF), V((4, 2 * T, D), BF), V((4, 2 * T, D), BF),
            V((8, 2 * T), F32), V((4, 2 * S2, 2 * T), BF), V((4, 2 * T, 2 * S2), BF), V((2, M, 128), F32), V((2, M, D), BF), V((2, M, D), BF),
            V((M, 2 * Fh), F32), V((M, Fh), F32), V((2, M, Fh), BF), V((2, M, 2 * Fh), BF), V((4, 2 * S2, D), BF),
            V((2, 2 * T, D), BF), V((4, 2 * T, D), BF), V((nd, 8, 128), F32)]
        + Reduce22.scratch(T, D)
        + [DMA((3, chips, 2)), DMA((3, chips, 5)), DMA((nd,)), DMA((nd,)), DMA((16,))],
        compiler_params=params(cid, 64 << 20), name="experts",
    )(x, marked, G, w_gate, w_up, w_down)[:7]


def head_rotated(v, gain, cos, sin):
    inv = lax.rsqrt(jnp.mean(v * v, axis=-1, keepdims=True) + epsilon)
    n = v * inv * gain
    return n * cos + pltpu.roll(n, HEAD_SIZE // 2, 1) * sin, inv


def head_back(v, gain, cos, sin, grad):
    inv = lax.rsqrt(jnp.mean(v * v, axis=-1, keepdims=True) + epsilon)
    g = grad * cos - pltpu.roll(grad, HEAD_SIZE // 2, 1) * sin
    s = g * gain
    return inv * (s - v * (inv * inv * jnp.mean(s * v, axis=-1, keepdims=True))), g * v * inv


def softmax_rows(q, k, allowed):
    s = lax.dot_general(q, k, NT, preferred_element_type=F32) * (HEAD_SIZE ** -0.5)
    s = jnp.where(allowed > 0.0, s, -1e30)
    ex = jnp.exp(s - jnp.max(s, axis=-1, keepdims=True))
    return ex * (1.0 / jnp.sum(ex, axis=-1, keepdims=True))


def attention_forward(n_expert, X, W, O, gain, gq, gk, cos, sin, allowed, cot, cid):
    T, D = cot.shape
    L = 2 * T
    rows = 2 * L
    GQ = O.shape[0]
    heads = GQ // HEAD_SIZE
    C = W.shape[1]
    HS = HEAD_SIZE

    def kernel(X_ref, W_ref, O_ref, gain_ref, gq_ref, gk_ref, cos_ref, sin_ref, ok_ref, x_ref,
               o_ref, N, first, raw, qs, ks, vs, att, part, acc, buf, fin, rsem, ssem, xr, xs, lsem):
        net = Net(n_expert).enter()
        z, e, c = net.at[0], net.e, net.c
        own = lambda: pltpu.make_async_copy(x_ref, N.at[e, pl.ds(pl.multiple_of(c * T, T), T)], lsem)
        own().start()
        greet(net, (0, 1, 2))
        own().wait()
        ag = Gather22(net, N, T, xr, xs)
        done = []

        def gather():
            ag.begin()
            yield
            for i in range(4):
                if i < 3:
                    ag.from_z(slot_plane(z, i + 1))
                    yield
                ag.from_two(slot_plane(z, i))
                yield
                if i:
                    ag.from_three(slot_plane(z, i - 1))
                    yield
            ag.from_three(slot_plane(z, 3))
            for i in range(4):
                ag.from_partner(slot_plane(z, i))

        def compute():
            def norm(i, _):
                r = pl.ds(pl.multiple_of(i * 32, 32), 32)
                x = X_ref[r, :].astype(F32)
                inv = lax.rsqrt(jnp.mean(x * x, axis=-1, keepdims=True) + epsilon)
                first[r, :] = (x * inv * gain_ref[...]).astype(BF)
                return 0

            lax.fori_loop(0, rows // 32, norm, 0)

            def project(j, _):
                cols = pl.ds(pl.multiple_of(j * 256, 256), 256)
                raw[:, cols] = jnp.dot(first[...], W_ref[:, cols], preferred_element_type=F32)
                return 0

            lax.fori_loop(0, 2, project, 0)
            yield
            lax.fori_loop(2, C // 256, project, 0)
            yield
            for s in range(2):
                r = slice(s * L, (s + 1) * L)
                k, _ = head_rotated(raw[r, GQ:GQ + HS], gk_ref[...], cos_ref[...], sin_ref[...])
                ks[r, :] = k.astype(BF)
                vs[r, :] = raw[r, GQ + HS:].astype(BF)
            for s in range(2):
                r = pl.ds(s * L, L)

                def one_head(h, _):
                    cols = pl.ds(pl.multiple_of(h * HS, HS), HS)
                    q, _ = head_rotated(raw[r, cols], gq_ref[...], cos_ref[...], sin_ref[...])
                    q = q.astype(BF)
                    qs[r, cols] = q
                    p = softmax_rows(q, ks[r, :], ok_ref[s]).astype(BF)
                    att[r, cols] = jnp.dot(p, vs[r, :], preferred_element_type=F32).astype(BF)
                    return 0

                for g in range(2):
                    lax.fori_loop(g * heads // 2, (g + 1) * heads // 2, one_head, 0)
                    yield

            def project_out(j, _):
                cols = pl.ds(pl.multiple_of(j * 512, 512), 512)
                part[:, cols] = jnp.dot(att[...], O_ref[:, cols], preferred_element_type=F32).astype(BF)
                return 0

            lax.fori_loop(0, D // 512, project_out, 0)
            yield
            yield from col_rs(
                net, lambda s, h: part.at[pl.ds(s * L + h * T, T)], o_ref, lambda w, s, h: acc.at[w, s, h],
                lambda w, s, h: buf.at[w, s, h], lambda i: fin.at[i], lambda w, s, h: rsem.at[w, s, h],
                lambda w, s, h: ssem.at[w, s, h], T, done)

        interleave(gather(), compute(), steps=(1, 3))
        for f in done:
            f()

        def finish(i, _):
            ag.drain(i)
            return 0

        lax.fori_loop(0, 4, finish, 0)

    S = jax.ShapeDtypeStruct
    V = pltpu.VMEM
    return pl.pallas_call(
        kernel,
        out_shape=(S((T, D), BF), S((n_expert, 2 * T, D), BF), S((rows, D), BF), S((rows, C), F32), S((rows, GQ), BF),
                   S((rows, HS), BF), S((rows, HS), BF), S((rows, GQ), BF)),
        in_specs=[VM] * 10, out_specs=(VM, ANY, VM, VM, VM, VM, VM, VM),
        scratch_shapes=[V((rows, D), BF), V((2, 2, 2, T, D), BF), V((2, 2, 2, T, D), BF), V((2, T, D), BF),
                        DMA((3, 2, 2)), DMA((3, 2, 2)), DMA((2, n_expert, 2)), DMA((2, n_expert, 5)), DMA],
        compiler_params=params(cid, 60 << 20), name="attention_forward",
    )(X, W, O, gain, gq, gk, cos, sin, allowed, cot)


def attention_backward(n_expert, out_part, gx, X, first, raw, qs, ks, vs, att, W, O, gain, gq, gk, cos, sin, allowed, cid):
    T, D = gx.shape
    L = 2 * T
    rows = 2 * L
    GQ = O.shape[0]
    heads = GQ // HEAD_SIZE
    C = W.shape[1]
    HS = HEAD_SIZE
    scale = HS ** -0.5

    def kernel(p_ref, gx_ref, X_ref, first, raw, qs, ks, vs, att, W_ref, O_ref, gain_ref, gq_ref, gk_ref, cos_ref, sin_ref, ok_ref,
               o_ref, dX, dW, dO, ga_out, gq_out, gk_out,
               GA, gatt, graw, dk, dv, invc, Tb, acc, b1, b2, zb, r0, s0, r1, s1, r2, s2, r3, s3, xr, xs, lsem):
        net = Net(n_expert).enter()
        z = net.at[0]
        far = lambda i: slot_plane(z, 3 - i)
        load = lambda i: pltpu.make_async_copy(p_ref.at[pl.ds(far(i) * 4, 4)], Tb, lsem)
        load(0).start()
        greet(net, (0, 1, 2))
        rs = Reduce22(net, T, acc, b1, b2, zb, (r0, s0, r1, s1, r2, s2, r3, s3))
        lane = lax.broadcasted_iota(jnp.int32, (256, 256), 1)
        sub = lax.broadcasted_iota(jnp.int32, (256, 256), 0)
        eye = jnp.where(sub == lane, 1.0, 0.0).astype(BF)

        def flip(v):
            return lax.dot_general(eye[:v.shape[1], :v.shape[1]], v, NT, preferred_element_type=F32).astype(BF)

        def reduce():
            for i in range(4):
                load(i).wait()
                rs.p_send(Tb, far(i))
                yield
                rs.stage0(Tb, far(i))
                rs.p_wait_send(Tb, far(i))
                if i < 3:
                    load(i + 1).start()
                yield
                if i:
                    rs.stage1(far(i - 1))
                    yield
                if i > 1:
                    rs.stage2(far(i - 2))
                    yield
            rs.stage1(far(3))
            yield
            rs.stage2(far(2))
            yield
            for i in (0, 1, 2):
                rs.relay(far(i))
                yield
            rs.stage2(far(3))
            yield
            rs.last(o_ref)

        def compute():
            done = []
            place = lambda s, h: GA.at[pl.ds(pl.multiple_of(s * L + h * T, T), T)]
            yield from col_ag(net, gx_ref, place, lambda s, h: xr.at[s, h], lambda w, s, h: xs.at[w, s, h], done)
            for f in done:
                f()

            def grad_att(j, _):
                cols = pl.ds(pl.multiple_of(j * 256, 256), 256)
                gatt[:, cols] = lax.dot_general(GA[...], O_ref[cols, :], NT, preferred_element_type=F32).astype(BF)
                return 0

            lax.fori_loop(0, GQ // 256, grad_att, 0)
            yield
            gq_out[...] = jnp.zeros_like(gq_out)
            gk_out[...] = jnp.zeros_like(gk_out)

            def inverse(i, _):
                r = pl.ds(pl.multiple_of(i * 32, 32), 32)
                x = X_ref[r, :].astype(F32)
                inv = lax.rsqrt(jnp.mean(x * x, axis=-1, keepdims=True) + epsilon)
                invc[r, :] = jnp.broadcast_to(inv, (32, 128))
                return 0

            lax.fori_loop(0, rows // 32, inverse, 0)
            for s in range(2):
                r = pl.ds(s * L, L)
                dk[...] = jnp.zeros_like(dk)
                dv[...] = jnp.zeros_like(dv)

                def one_head(h, _):
                    cols = pl.ds(pl.multiple_of(h * HS, HS), HS)
                    q, k, v, g = qs[r, cols], ks[r, :], vs[r, :], gatt[r, cols]
                    p = softmax_rows(q, k, ok_ref[s])
                    dp = lax.dot_general(g, v, NT, preferred_element_type=F32)
                    ds = (p * (dp - jnp.sum(p * dp, axis=-1, keepdims=True))).astype(BF)
                    dv[...] += jnp.dot(flip(p.astype(BF)), g, preferred_element_type=F32)
                    dk[...] += jnp.dot(flip(ds), q, preferred_element_type=F32)
                    dq = jnp.dot(ds, k, preferred_element_type=F32) * scale
                    gr, terms = head_back(raw[r, cols], gq_ref[...], cos_ref[...], sin_ref[...], dq)
                    graw[r, cols] = gr.astype(BF)
                    gq_out[...] += jnp.sum(terms, axis=0, keepdims=True)
                    return 0

                for g in range(2):
                    lax.fori_loop(g * heads // 2, (g + 1) * heads // 2, one_head, 0)
                    yield
                gr, terms = head_back(raw[r, GQ:GQ + HS], gk_ref[...], cos_ref[...], sin_ref[...], dk[...] * scale)
                graw[r, GQ:GQ + HS] = gr.astype(BF)
                gk_out[...] += jnp.sum(terms, axis=0, keepdims=True)
                graw[r, GQ + HS:] = dv[...].astype(BF)

            def grad_o(h, _):
                cols = pl.ds(pl.multiple_of(h * HS, HS), HS)
                aT = flip(att[:, cols])
                for j in range(2):
                    w = slice(j * (D // 2), (j + 1) * (D // 2))
                    dO[cols, w] = jnp.dot(aT, GA[:, w], preferred_element_type=F32).astype(BF)
                return 0

            lax.fori_loop(0, heads, grad_o, 0)
            yield

            def grad_x(j, _):
                cols = pl.ds(pl.multiple_of(j * 256, 256), 256)
                dx = lax.dot_general(graw[...], W_ref[cols, :], NT, preferred_element_type=F32)
                dX[:, cols] = dx.astype(BF)
                ga_out[:, cols] = jnp.sum(dx * X_ref[:, cols].astype(F32) * invc[:, 0:1], axis=0, keepdims=True)
                return 0

            for g in range(2):
                lax.fori_loop(g * D // 512, (g + 1) * D // 512, grad_x, 0)
                yield

            def grad_w(j, _):
                cols = pl.ds(pl.multiple_of(j * 256, 256), 256)
                dW[cols, :] = jnp.dot(flip(first[:, cols]), graw[...], preferred_element_type=F32).astype(BF)
                return 0

            for g in range(2):
                lax.fori_loop(g * D // 512, (g + 1) * D // 512, grad_w, 0)
                yield

        interleave(reduce(), compute())

        def finish(i, _):
            rs.drain(slot_plane(z, i))
            return 0

        lax.fori_loop(0, 4, finish, 0)

    S = jax.ShapeDtypeStruct
    V = pltpu.VMEM
    return pl.pallas_call(
        kernel,
        out_shape=(S((T, D), BF), S((rows, D), BF), S((D, C), BF), S((GQ, D), BF), S((1, D), F32), S((1, HS), F32), S((1, HS), F32)),
        in_specs=[ANY] + [VM] * 16, out_specs=(VM,) * 7,
        scratch_shapes=[V((rows, D), BF), V((rows, GQ), BF), V((rows, C), BF), V((L, HS), F32), V((L, HS), F32), V((rows, 128), F32),
                        V((4, 2 * T, D), BF)] + Reduce22.scratch(T, D) + [DMA((2, 2)), DMA((3, 2, 2)), DMA],
        compiler_params=params(cid, 64 << 20), name="attention_backward",
    )(out_part, gx, X, first, raw, qs, ks, vs, att, W, O, gain, gq, gk, cos, sin, allowed)


MODEL_WIDTH = 2048
QUERY_HEADS = 32
KEY_VALUE_HEADS = 4
HEAD_SIZE = 128
GROUP = QUERY_HEADS // KEY_VALUE_HEADS
TOP = 8
EXP_DEV = 2

epsilon = 1e-06
rope_base = 1000000.0


def norm_parts(values_in, gain_vec):
    inverse = lax.rsqrt(jnp.mean(values_in * values_in, axis=-1, keepdims=True) + epsilon)
    return (values_in * inverse * gain_vec, inverse)


def norm_back(values_in, inverse, gain_vec, grad_out):
    scaled = grad_out * gain_vec
    grad_in = inverse * (
        scaled
        - values_in * inverse * inverse * jnp.mean(scaled * values_in, axis=-1, keepdims=True)
    )
    return (grad_in, grad_out * values_in * inverse)


def rope_tables(positions):
    exponent = jnp.arange(HEAD_SIZE // 2).astype(F32) * (2.0 / HEAD_SIZE)
    frequency = jnp.exp(-math.log(rope_base) * exponent)
    angles = positions.astype(F32)[:, None] * frequency[None, :]
    return (jnp.cos(angles), jnp.sin(angles))


def rotate(v, cos, sin):
    half = v.shape[-1] // 2
    a, b = v[..., :half], v[..., half:]
    return jnp.concatenate([a * cos - b * sin, b * cos + a * sin], axis=-1)


def rotate_back(v, cos, sin):
    half = v.shape[-1] // 2
    a, b = v[..., :half], v[..., half:]
    return jnp.concatenate([a * cos + b * sin, b * cos - a * sin], axis=-1)


def mm(a, b):
    return jnp.dot(a, b, preferred_element_type=F32)


def ein(spec, *args):
    return jnp.einsum(spec, *args, preferred_element_type=F32)


def experts_wide(n_expert, second_in, marked, G, w_gate, w_up, w_down, capacity):
    T, D = second_in.shape
    nd = 2 * n_expert
    e = lax.axis_index("expert")
    N, M = gather_all(n_expert, second_in, marked, 2)

    mine = lax.dynamic_slice(M, (0, EXP_DEV * e, 0), (nd, EXP_DEV, T))
    here = mine >= 0.0
    rank = jnp.cumsum(here.astype(jnp.int32), axis=-1) - 1
    slots = jnp.arange(capacity, dtype=jnp.int32)
    pick = here[:, :, None, :] & (rank[:, :, None, :] == slots[None, None, :, None])
    slot_weight = jnp.sum(jnp.where(pick, mine[:, :, None, :], 0.0), axis=-1).transpose(1, 0, 2)[..., None]
    pick = pick.astype(BF)
    N = N.reshape(nd, T, D)
    G = G.reshape(nd, T, D)
    rows = ein("sect,std->escd", pick, N).astype(BF)
    g_rows = ein("sect,std->escd", pick, G)
    flat = lambda v: v.reshape(EXP_DEV, nd * capacity, v.shape[-1])
    deep = lambda v: v.reshape(EXP_DEV, nd, capacity, v.shape[-1])
    rows = flat(rows)
    grad_rows = flat((slot_weight * g_rows).astype(BF))
    gate_value = ein("emd,edf->emf", rows, w_gate)
    up_value = ein("emd,edf->emf", rows, w_up)
    sig = jax.nn.sigmoid(gate_value)
    act = (gate_value * sig * up_value).astype(BF)
    expert_part = deep(ein("emf,efd->emd", act, w_down))
    dots = jnp.sum(g_rows * expert_part, axis=-1)
    out_part = ein("sect,escd->std", pick, (slot_weight * expert_part).astype(BF)).astype(BF)
    dots = ein("sect,esc->set", pick.astype(F32), dots)
    grad_act = ein("emd,efd->emf", grad_rows, w_down)
    grad_gate_v = (grad_act * up_value * sig * (1.0 + gate_value * (1.0 - sig))).astype(BF)
    grad_up_v = (grad_act * gate_value * sig).astype(BF)
    down_grad = ein("emf,emd->efd", act, grad_rows)
    gate_grad = ein("emd,emf->edf", rows, grad_gate_v)
    up_grad = ein("emd,emf->edf", rows, grad_up_v)
    back_rows = ein("emf,edf->emd", grad_gate_v, w_gate) + ein("emf,edf->emd", grad_up_v, w_up)
    back_part = ein("sect,escd->std", pick, deep(back_rows.astype(BF))).astype(BF)

    dots_out = jnp.pad(dots, ((0, 0), (0, 8 - EXP_DEV), (0, 0)))
    dots_in = exchange(n_expert, dots_out, 3)
    parts = max(1, n_expert // 16)
    cols = D // parts

    def summed(v, cid):
        v = v.reshape(n_expert, 2, T, D)
        part = lambda i: reduce_scatter_all(n_expert, lax.dynamic_slice_in_dim(v, i * cols, cols, axis=3), cid)
        return lax.map(part, jnp.arange(parts)).transpose(1, 0, 2).reshape(T, D)

    back_sum, out_sum = summed(back_part, 4), summed(out_part, 5)
    return back_sum, out_sum, dots_in, gate_grad, up_grad, down_grad


def local(
    n_expert, tokens, routes, documents, w_query, key_projection, value_projection, w_out, w_router,
    gain_attn, gain_ffn, gain_query, gain_key, w_gate, w_up, w_down, cotangent,
):
    Z = KEY_VALUE_HEADS
    plane = n_expert // Z
    nd = 2 * n_expert
    T, D = tokens.shape
    R, HR, E = w_query.shape[0], w_out.shape[0], w_router.shape[1]
    Q = gain_query.shape[0]
    KV = HEAD_SIZE
    GQ = GROUP * HEAD_SIZE
    e, c = lax.axis_index("expert"), lax.axis_index("context")
    z, p = e // plane, e % plane
    capacity = T * TOP * 5 // (4 * E)
    score_scale = HEAD_SIZE ** (-0.5)

    wqkv = jnp.concatenate(
        [w_query.reshape(R, Z, GQ), key_projection.reshape(R, Z, KV), value_projection.reshape(R, Z, KV)], axis=-1
    ).transpose(1, 0, 2)
    width = -(-(E + 4) // 128) * 128
    pad = lambda v: jnp.pad(v, (0, R - v.shape[0]))[:, None]
    head = jnp.concatenate(
        [w_router, gain_attn[:, None], gain_ffn[:, None], pad(gain_query), pad(gain_key), jnp.zeros((R, width - E - 4), BF)], axis=1
    )
    docs_own = lax.dynamic_slice_in_dim(documents[0], c * T, T).astype(BF)[None]
    docs_own = jnp.pad(docs_own, ((0, 15), (0, width - T)))
    aux = jnp.concatenate([head, docs_own], axis=0)
    small_plane = plane == 4
    X, W, O, A, *G = gather_start(n_expert, tokens, wqkv, w_out, aux, None if small_plane else cotangent, 0)
    W = W.reshape(D, GQ + 2 * KV)
    O = O.reshape(GQ, D)
    table = A[:, :R].reshape(D, width)
    router_weight = table[:, :E]
    attn_gain = table[:, E].astype(F32)
    ffn_gain = table[:, E + 1].astype(F32)
    query_gain = A[:, :Q, E + 2].reshape(HEAD_SIZE).astype(F32)
    key_gain = A[:, :Q, E + 3].reshape(HEAD_SIZE).astype(F32)
    docs = A[:, R, :T].reshape(Z, plane, 2 * T)
    docs = lax.dynamic_slice(docs, (2 * c, p, 0), (2, 1, 2 * T)).reshape(2, 2 * T)

    L = 2 * T
    places = jnp.arange(L, dtype=jnp.int32)
    cos, sin = rope_tables(places)
    qcos, qsin = cos[:, None, :], sin[:, None, :]
    allowed = (places[:, None] >= places[None, :])[None] & (docs[:, :, None] == docs[:, None, :])
    if small_plane:
        cos2 = jnp.concatenate([cos, cos], axis=1)
        sin2 = jnp.concatenate([-sin, sin], axis=1)
        attn_sum, G, first_in, raw, queries, keys, value, attended = attention_forward(
            n_expert, X.reshape(2 * L, D), W, O, attn_gain[None], query_gain[None], key_gain[None], cos2, sin2,
            allowed.astype(F32), cotangent, 1)
    else:
        x = X.reshape(2 * L, D).astype(F32)
        normed, inverse_attn = norm_parts(x, attn_gain)
        first_in = normed.astype(BF)
        raw = mm(first_in, W)
        query_raw = raw[:, :GQ].reshape(2, L, GROUP, HEAD_SIZE)
        key_raw = raw[:, GQ:GQ + KV].reshape(2, L, HEAD_SIZE)
        value = raw[:, GQ + KV:].reshape(2, L, HEAD_SIZE).astype(BF)
        query_normed, query_inverse = norm_parts(query_raw, query_gain)
        key_normed, key_inverse = norm_parts(key_raw, key_gain)
        queries = rotate(query_normed, qcos, qsin).astype(BF)
        keys = rotate(key_normed, cos, sin).astype(BF)
        scores = ein("sqhd,skd->shqk", queries, keys) * score_scale
        scores = jnp.where(allowed[:, None], scores, -1e30)
        top = jnp.max(scores, axis=-1, keepdims=True)
        ex = jnp.exp(scores - top)
        probs = ex / jnp.sum(ex, axis=-1, keepdims=True)
        probs_low = probs.astype(BF)
        attended = ein("shqk,skd->sqhd", probs_low, value).reshape(2 * L, GQ).astype(BF)
        part = mm(attended, O).astype(BF).reshape(2, 2, T, D)
        attn_sum, G = column_sum(n_expert, part, 1), G[0]
    middle = tokens.astype(F32) + attn_sum.astype(F32)

    normed_ffn, inverse_ffn = norm_parts(middle, ffn_gain)
    second_in = normed_ffn.astype(BF)
    logits = mm(second_in, router_weight)
    ids = jnp.arange(E, dtype=jnp.int32)
    chosen = jnp.any(routes[:, :, None] == ids[None, None, :], axis=1)
    masked = jnp.where(chosen, logits, -jnp.inf)
    best = jnp.max(masked, axis=-1, keepdims=True)
    ew = jnp.where(chosen, jnp.exp(logits - best), 0.0)
    weights = ew / jnp.sum(ew, axis=-1, keepdims=True)
    marked = jnp.where(chosen, weights, -1.0).T
    if small_plane:
        back_sum, out_part, dots_in, rows, g_rows, act_w, gate_up = experts_fused(
            second_in, marked, G, w_gate, w_up, w_down, capacity, 3)
        flat = lambda v: v.reshape(EXP_DEV, -1, v.shape[-1])
        Fh = act_w.shape[-1]
        rows = flat(rows)
        down_grad = ein("emf,emd->efd", flat(act_w), flat(g_rows))
        gate_grad = ein("emd,emf->edf", rows, flat(gate_up[..., :Fh]))
        up_grad = ein("emd,emf->edf", rows, flat(gate_up[..., Fh:]))
    else:
        back_sum, out_sum, dots_in, gate_grad, up_grad, down_grad = experts_wide(
            n_expert, second_in, marked, G, w_gate, w_up, w_down, capacity)
    back_sum = back_sum.astype(F32)

    grad_result = cotangent.astype(F32)
    grad_weights = jnp.sum(dots_in[:, :EXP_DEV].reshape(n_expert, 2, EXP_DEV, T), axis=1).reshape(E, T).T
    grad_chosen = weights * (grad_weights - jnp.sum(weights * grad_weights, axis=-1, keepdims=True))
    grad_logits = jnp.where(chosen, grad_chosen, 0.0).astype(BF)
    router_grad = mm(second_in.T, grad_logits)
    grad_second = mm(grad_logits, router_weight.T) + back_sum
    grad_middle_norm, ffn_terms = norm_back(middle, inverse_ffn, ffn_gain, grad_second)
    ffn_gain_grad = jnp.sum(ffn_terms, axis=0)
    grad_middle = grad_result + grad_middle_norm

    if small_plane:
        out_sum, grad_first, raw_grad, out_grad, attn_gain_grad, query_gain_grad, key_gain_grad = attention_backward(
            n_expert, out_part, grad_middle.astype(BF), X.reshape(2 * L, D), first_in, raw, queries, keys, value, attended, W, O,
            attn_gain[None], query_gain[None], key_gain[None], cos2, sin2, allowed.astype(F32), 6)
        attn_gain_grad, query_gain_grad, key_gain_grad = attn_gain_grad[0], query_gain_grad[0], key_gain_grad[0]
    else:
        GA = column_gather(n_expert, grad_middle.astype(BF), 6)
        GA = GA.reshape(2 * L, D)
        out_grad = mm(attended.T, GA)
        grad_attended = ein("td,fd->tf", GA, O).astype(BF).reshape(2, L, GROUP, HEAD_SIZE)
        grad_probs = ein("sqhd,skd->shqk", grad_attended, value)
        grad_scores = (probs * (grad_probs - jnp.sum(probs * grad_probs, axis=-1, keepdims=True))).astype(BF)
        grad_queries = ein("shqk,skd->sqhd", grad_scores, keys) * score_scale
        grad_keys = ein("shqk,sqhd->skd", grad_scores, queries) * score_scale
        grad_values = ein("shqk,sqhd->skd", probs_low, grad_attended)
        grad_query_raw, query_terms = norm_back(query_raw, query_inverse, query_gain, rotate_back(grad_queries, qcos, qsin))
        grad_key_raw, key_terms = norm_back(key_raw, key_inverse, key_gain, rotate_back(grad_keys, cos, sin))
        grad_raw = jnp.concatenate(
            [grad_query_raw.reshape(2 * L, GQ).astype(BF), grad_key_raw.reshape(2 * L, KV).astype(BF),
             grad_values.reshape(2 * L, KV).astype(BF)], axis=-1)
        query_gain_grad = jnp.sum(query_terms, axis=(0, 1, 2))
        key_gain_grad = jnp.sum(key_terms, axis=(0, 1))
        grad_first = ein("tf,df->td", grad_raw, W)
        raw_grad = mm(first_in.T, grad_raw)
        attn_gain_grad = jnp.sum(grad_first * x * inverse_attn, axis=0)
    block_out = (middle + out_sum.astype(F32)).astype(BF)

    small = jnp.concatenate([
        router_grad.reshape(nd, R * E), attn_gain_grad.reshape(nd, R), ffn_gain_grad.reshape(nd, R),
        query_gain_grad.reshape(nd, Q), key_gain_grad.reshape(nd, Q)], axis=1)
    n_small = small.shape[1]
    small = jnp.pad(small, ((0, 0), (0, -n_small % 2048))).reshape(nd, -1, 128).astype(BF)
    grad_first_sum, raw_sum, out_sum2, small_in = reduce_end(
        n_expert, grad_first.astype(BF).reshape(2, 2, T, D), raw_grad.astype(BF).reshape(Z, plane, 2, R, GQ + 2 * KV),
        out_grad.astype(BF).reshape(plane, 2, HR, D), small, 7)
    small_sum = jnp.sum(small_in.astype(F32), axis=0).reshape(-1)
    router_grad = small_sum[:R * E].reshape(R, E)
    attn_gain_grad = small_sum[R * E:R * E + R]
    ffn_gain_grad = small_sum[R * E + R:R * E + 2 * R]
    query_gain_grad = small_sum[R * E + 2 * R:R * E + 2 * R + Q]
    key_gain_grad = small_sum[R * E + 2 * R + Q:n_small]
    raw_sum = raw_sum.astype(F32)
    query_grad = raw_sum[:, :, :GQ].transpose(1, 0, 2).reshape(R, QUERY_HEADS * HEAD_SIZE)
    key_grad = raw_sum[:, :, GQ:GQ + KV].transpose(1, 0, 2).reshape(R, Z * KV)
    value_grad = raw_sum[:, :, GQ + KV:].transpose(1, 0, 2).reshape(R, Z * KV)

    own = tokens.astype(F32)
    inverse_own = lax.rsqrt(jnp.mean(own * own, axis=-1, keepdims=True) + epsilon)
    grad_in, _ = norm_back(own, inverse_own, attn_gain, grad_first_sum.astype(F32))
    grad_tokens = grad_middle + grad_in
    return (
        block_out, grad_tokens, query_grad, key_grad, value_grad, out_sum2.astype(F32), router_grad,
        attn_gain_grad, ffn_gain_grad, query_gain_grad, key_gain_grad, gate_grad, up_grad, down_grad,
    )


def solution(mesh):
    row = P(("expert", "context"), None)
    vec = P(("expert", "context"))
    hidden = P("expert", None, "context")
    return jax.shard_map(
        functools.partial(local, mesh.shape["expert"]),
        mesh=mesh,
        in_specs=(row, row, P("expert", None), row, row, row, row, row, vec, vec, vec, vec, hidden, hidden,
                  P("expert", "context", None), row),
        out_specs=(row, row, row, row, row, row, row, vec, vec, vec, vec, hidden, hidden, P("expert", "context", None)),
        check_vma=False,
    )
```
